32 devices in a mesh: ctx: 16 (over z, y, core), head: 2 (over x).
Axes of the slice: x: 2, y: 2, z: 4, core: 2. Of those that a mesh axis runs over, the one named last changes fastest.
Arguments:
- queries: bfloat16 [16, 1024, 2048], P('ctx', None, 'head'), may hold values from -8 to 8
- keys: bfloat16 [16, 1024, 2048], P('ctx', None, 'head'), may hold values from -8 to 8
- values: bfloat16 [16, 1024, 2048], P('ctx', None, 'head'), may hold values from -24 to 24
- w_out: bfloat16 [2048, 4096], P('head'), may hold values from -0.125 to 0.125
Outputs:
- mixed: bfloat16 [16, 1024, 4096], P('ctx', 'head')
The draws below stay inside these ranges and needn't reach their ends.
All inputs are finite; a program needn't handle non-finite values.
Results may differ from the reference program's by a relative error of at most 0.013.
Values may be sent and summed in bfloat16 or wider, within the bound.
A program may use at most 128 MiB of HBM per device.

```python
import jax
import jax.numpy as jnp
from jax import lax

D = 4096
HD = 128
GROUP = 4
STRIDE = 1024
ROWS = 16
FEAT = 2048
N_HEAD = 2


def draw_queries(key, part):
    shape = (ROWS, STRIDE, FEAT)
    base = jax.random.truncated_normal(jax.random.fold_in(key, 11), -4.0, 4.0, shape, jnp.float32)
    return base.astype(jnp.bfloat16)


def draw_keys(key, part):
    shape = (ROWS, STRIDE, FEAT)
    base = jax.random.truncated_normal(jax.random.fold_in(key, 12), -4.0, 4.0, shape, jnp.float32)
    return base.astype(jnp.bfloat16)


def shard_levels(stream_key, shape, cuts, low, largest):
    level, own = 1.0, jax.random.fold_in(stream_key, 6)
    for dim, blocks in cuts:
        draws = jnp.exp(jax.random.uniform(jax.random.fold_in(own, dim), (blocks,), jnp.float32, low / len(cuts), largest / len(cuts)))
        level = level * jnp.repeat(draws, shape[dim] // blocks).reshape([-1 if axis == dim else 1 for axis in range(len(shape))])
    return level


def noise(stream_key, shape, scale, reach, pieces=(), kind=jnp.bfloat16):
    entries = scale * jax.random.normal(stream_key, shape, jnp.float32)
    if pieces:
        entries = entries * shard_levels(stream_key, shape, pieces, -0.22, 0.18)
    return jnp.clip(entries, -reach, reach).astype(kind)


def setup_inputs(seed: int = 0) -> dict:
    key_of = jax.random.split(jax.random.key(seed), 5)
    queries = draw_queries(jax.random.fold_in(key_of[4], 71), 0)
    keys = draw_keys(jax.random.fold_in(key_of[4], 71), 0)
    values = noise(key_of[2], (ROWS, STRIDE, FEAT), 4.0, 24.0, ((0, 16), (2, 2)))
    w_out = noise(key_of[3], (FEAT, D), FEAT ** -0.5, 0.125, ((0, 2),))
    return {"queries": queries, "keys": keys, "values": values, "w_out": w_out}


masked_score = -1e30


def split_kinds(tensor, parity):
    groups = tensor.shape[2] // (2 * GROUP * HD)
    shaped = tensor.reshape((tensor.shape[0], tensor.shape[1], groups, 2, GROUP, HD))
    return shaped[:, :, :, parity].reshape((tensor.shape[0], tensor.shape[1], groups * GROUP, HD))


def normalized(scores):
    top = jnp.max(scores, axis=-1, keepdims=True)
    expo = jnp.exp(scores - top)
    total = jnp.sum(expo, axis=-1, keepdims=True)
    return (expo / total).astype(jnp.bfloat16)


def reference(queries, keys, values, w_out):
    scale = jnp.float32(1.0 / (HD ** 0.5))
    row_q, row_k, row_v = split_kinds(queries, 0), split_kinds(keys, 0), split_kinds(values, 0)
    col_q, col_k, col_v = split_kinds(queries, 1), split_kinds(keys, 1), split_kinds(values, 1)
    length = STRIDE
    causal_row = lax.broadcasted_iota(jnp.int32, (length, length), 1) <= lax.broadcasted_iota(jnp.int32, (length, length), 0)

    def one_row(triple):
        query_row, key_row, value_row = triple
        scores = jnp.einsum("qhd,khd->hqk", query_row.astype(jnp.float32), key_row.astype(jnp.float32)) * scale
        scores = jnp.where(causal_row, scores, masked_score)
        weights = normalized(scores)
        return jnp.einsum("hqk,khd->qhd", weights.astype(jnp.float32), value_row.astype(jnp.float32)).astype(jnp.bfloat16)

    row_out = lax.map(one_row, (row_q, row_k, row_v))
    causal_col = lax.broadcasted_iota(jnp.int32, (ROWS, ROWS), 1) <= lax.broadcasted_iota(jnp.int32, (ROWS, ROWS), 0)
    scores = jnp.einsum("rchd,schd->chrs", col_q.astype(jnp.float32), col_k.astype(jnp.float32)) * scale
    scores = jnp.where(causal_col, scores, masked_score)
    weights = normalized(scores)
    col_out = jnp.einsum("chrs,schd->rchd", weights.astype(jnp.float32), col_v.astype(jnp.float32)).astype(jnp.bfloat16)
    groups = FEAT // (2 * GROUP * HD)
    joined = jnp.stack([row_out.reshape((ROWS, STRIDE, groups, GROUP, HD)), col_out.reshape((ROWS, STRIDE, groups, GROUP, HD))], axis=3)
    flat = joined.reshape((ROWS * STRIDE, FEAT))
    width = FEAT // N_HEAD
    total = jnp.zeros((ROWS * STRIDE, D), jnp.float32)
    for index in range(N_HEAD):
        term = jnp.dot(flat[:, index * width:(index + 1) * width], w_out[index * width:(index + 1) * width], preferred_element_type=jnp.float32)
        total = total + lax.optimization_barrier(term.astype(jnp.bfloat16)).astype(jnp.float32)
    return total.astype(jnp.bfloat16).reshape((ROWS, STRIDE, D))
```

```python
import functools

import jax
import jax.numpy as jnp
from jax import lax
from jax.experimental import pallas as pl
from jax.experimental.pallas import tpu as pltpu
from jax.sharding import PartitionSpec as P

HD = 128
GROUP = 4
MESH = pl.DeviceIdType.MESH
SHARES = 8
STRAIGHT = 2
PARTS = 2
LAYER = 4
CHUNKS = 8
WIDTH = 16
PIECES = 4
AHEAD = 2

masked_score = -1e30


def attend(query, key, value, allowed):
    scores = lax.dot_general(
        query, key, (((1,), (1,)), ((), ())), preferred_element_type=jnp.float32
    ) * jnp.float32(1.0 / HD**0.5)
    scores = jnp.where(allowed, scores, masked_score)
    top = jnp.max(scores, axis=-1, keepdims=True)
    expo = jnp.exp(scores - top)
    total = jnp.sum(expo, axis=-1, keepdims=True)
    mixed = jnp.dot(expo.astype(jnp.bfloat16), value, preferred_element_type=jnp.float32)
    return (mixed / total).astype(jnp.bfloat16)


def weigh(query, key, value, allowed):
    scores = lax.dot_general(
        query, key, (((1,), (1,)), ((), ())), preferred_element_type=jnp.float32
    ) * jnp.float32(1.0 / HD**0.5)
    if allowed is not None:
        scores = jnp.where(allowed, scores, masked_score)
    top = jnp.max(scores, axis=-1, keepdims=True)
    expo = jnp.exp(scores - top)
    total = jnp.sum(expo, axis=-1, keepdims=True)
    mixed = jnp.dot(expo.astype(jnp.bfloat16), value, preferred_element_type=jnp.float32)
    return (mixed / total).astype(jnp.bfloat16), top + jnp.log(total)


def layered(
    n, q_hbm, k_hbm, v_hbm, w_hbm, out_hbm, q_row, k_row, v_row, q_in, k_in, v_in, o_out, p_in,
    stats, stats_in, row_out, joined, summed, w_own, w_other, staged,
    local_sem, lay_send, lay_recv, up_send, up_recv, part_send, part_recv, stat_send, stat_recv,
    back_send, back_recv, w_send, w_recv, row_send, row_recv, out_sem,
):
    me, head = lax.axis_index("ctx"), lax.axis_index("head")
    other = 1 - head
    z, s = lax.div(me, LAYER), lax.rem(me, LAYER)
    core = lax.rem(s, 2)
    sib = s + 1 - 2 * core
    opp = s + 2 - 4 * lax.div(s, 2)
    far = sib + 2 - 4 * lax.div(sib, 2)
    peers = (s, sib, opp, far)
    stride = q_hbm.shape[1]
    block = q_row.shape[1]
    depth = w_own.shape[0]
    half = joined.shape[1]
    cols = stride // LAYER
    cw = cols // CHUNKS
    per = half // cols
    hbm = (q_hbm, k_hbm, v_hbm)
    ins = (q_in, k_in, v_in)
    own_at = (0, LAYER, LAYER)
    back_head = lax.div(s * cols, half)
    back_start = lax.rem(s * cols, half)
    stays = back_head == head
    feats = pl.ds(block, block)

    def remote(src, dst, send, recv, ctx, at):
        return pltpu.make_async_remote_copy(
            src_ref=src, dst_ref=dst, send_sem=send, recv_sem=recv,
            device_id=(ctx, at), device_id_type=MESH,
        )

    def here(slot):
        return z * LAYER + slot

    def lay(t, j, d, source):
        row = peers[d] if source else s
        return remote(
            hbm[t].at[0, pl.ds(peers[d] * cols + j * cw, cw), feats],
            ins[t].at[own_at[t] + row, pl.ds(j * cw, cw)],
            lay_send.at[t * CHUNKS + j, d], lay_recv.at[t * CHUNKS + j, d],
            here(peers[d]), head,
        )

    def up(kind, t, j, d, layer, base):
        if d < 2:
            src, slot, row = hbm[t].at[0, pl.ds(peers[d] * cols + j * cw, cw), feats], peers[d], s
        else:
            src, slot, row = ins[t].at[own_at[t] + peers[d], pl.ds(j * cw, cw)], s, peers[d]
        return remote(
            src, ins[t].at[base + row, pl.ds(j * cw, cw)],
            up_send.at[kind * CHUNKS + j, d], up_recv.at[kind * CHUNKS + j, d],
            layer * LAYER + slot, head,
        )

    def up_arrival(kind, t, j, d, base):
        return remote(
            hbm[t].at[0, pl.ds(0, cw), feats], ins[t].at[base + peers[d], pl.ds(j * cw, cw)],
            up_send.at[kind * CHUNKS + j, d], up_recv.at[kind * CHUNKS + j, d],
            here(sib), head,
        )

    routes = {
        0: ((0, 1, 1, 0), (1, 2, 1, 0)),
        2: ((2, 0, 1, LAYER),),
        3: ((3, 0, 1, 2 * LAYER), (2, 0, 2, LAYER)),
    }

    def direct(layer, j):
        for kind, t, to, base in routes[layer]:
            for d in (0, 1):
                up(kind, t, j, d, to, base).start()

    def relay(layer, j):
        for t in sorted({t for _, t, _, _ in routes[layer]}):
            for d in (2, 3):
                lay(t, j, d, True).wait_recv()
                for kind, t2, to, base in routes[layer]:
                    if t2 == t:
                        up(kind, t, j, d, to, base).start()

    def piece_rows(q, c, k):
        eighth = depth // 16
        rows = eighth // (PIECES // 2)
        start = lax.div(k, PIECES // 2) * (depth // 2)
        start += (q * 2 + c) * eighth + lax.rem(k, PIECES // 2) * rows
        return pl.ds(start, rows)

    def w_copy(source, q, c, k, way, to_ctx, to_head):
        rows = piece_rows(q, c, k)
        index = (q * 2 + c) * PIECES + k
        return remote(
            source.at[rows], w_other.at[rows], w_send.at[way, index], w_recv.at[index], to_ctx, to_head
        )

    even = lax.rem(z + lax.div(s, 2), 2)
    y_next = here(opp)
    z_next = me + LAYER - 2 * LAYER * lax.rem(z, 2)
    z_early = (z == 1) | (z == 2)

    def w_first(q, k):
        return w_copy(w_hbm, 2 * even + q, core, k, 0, me, other)

    def w_side(q, k):
        return w_copy(w_other, 2 * even + q, core, k, 2, y_next if q == 0 else z_next, head)

    def w_beside(q, k):
        return w_copy(w_other, 2 * (1 - even) + q, core, k, 1, here(sib), head)

    def w_here(q, k):
        return w_copy(w_other, 2 * even + q, core, k, 1, here(sib), head)

    def w_in(q, k):
        w_first(q, k).wait_recv()
        w_here(q, k).start()
        if q == 0:
            w_side(q, k).start()
        else:

            @pl.when(z_early)
            def _():
                w_side(q, k).start()

    def w_on(q, k):
        w_copy(w_other, 2 * (1 - even) + q, core, k, 2, me, other).wait_recv()
        w_beside(q, k).start()

    def exchange(ts):
        @pl.loop(0, CHUNKS)
        def _(j):
            for t in ts:
                for d in (2, 3, 1):
                    lay(t, j, d, False).start()

    for layer in routes:

        @pl.when(z == layer)
        def _():
            for j in range(AHEAD):
                direct(layer, j)

    @pl.when(z < 2)
    def _():
        exchange((1, 2))
        exchange((0,))

    @pl.when(z >= 2)
    def _():
        exchange((0,))
        exchange((1, 2))

    @pl.loop(0, PIECES)
    def _(k):
        w_first(0, k).start()
        w_first(1, k).start()

    local = [
        pltpu.make_async_copy(hbm[t].at[0, :, pl.ds(0, block)], (q_row, k_row, v_row)[t], local_sem.at[t])
        for t in range(3)
    ]
    local += [
        pltpu.make_async_copy(
            hbm[t].at[0, pl.ds(s * cols, cols), feats], ins[t].at[own_at[t] + s], local_sem.at[3 + t]
        )
        for t in range(3)
    ]
    local.append(pltpu.make_async_copy(w_hbm, w_own, local_sem.at[6]))
    for copy in local:
        copy.start()
    for copy in local[:6]:
        copy.wait()

    tile = min(256, half)
    row_index = lax.broadcasted_iota(jnp.int32, (tile, stride), 0)
    key_index = lax.broadcasted_iota(jnp.int32, (tile, stride), 1)

    def row_tile(h, start):
        lanes = pl.ds(pl.multiple_of(h * HD, HD), HD)
        end = start + tile
        row_out[pl.ds(start, tile), lanes] = attend(
            q_row[pl.ds(start, tile), lanes],
            k_row[pl.ds(0, end), lanes],
            v_row[pl.ds(0, end), lanes],
            key_index[:, :end] <= row_index[:, :end] + start,
        )

    def spread(sums, size, off):
        lane = lax.broadcasted_iota(jnp.int32, (size, HD), 1)
        row = lax.broadcasted_iota(jnp.int32, (size, HD), 0)
        return jnp.sum(jnp.where(lane == row + off, sums, 0.0), axis=0, keepdims=True)

    def column(line, size, off):
        lane = lax.broadcasted_iota(jnp.int32, (size, HD), 1)
        row = lax.broadcasted_iota(jnp.int32, (size, HD), 0)
        return jnp.sum(jnp.where(lane == row + off, line, 0.0), axis=1, keepdims=True)

    heads = block // HD
    size = LAYER * WIDTH

    def small(q_at, q_rows, k_at, k_rows, c, b, causal, keep):
        start = pl.multiple_of(c * cw + b * WIDTH, WIDTH)
        shape = (q_rows * WIDTH, k_rows * WIDTH)
        r = lax.broadcasted_iota(jnp.int32, shape, 0)
        m = lax.broadcasted_iota(jnp.int32, shape, 1)
        allowed = ((r - m) & (WIDTH - 1)) == 0
        if causal is not None:
            allowed &= m <= r + causal * WIDTH
        for h in range(heads):
            lanes = pl.ds(h * HD, HD)
            q_slice = (pl.ds(q_at, q_rows), pl.ds(start, WIDTH), lanes)
            k_slice = (pl.ds(k_at, k_rows), pl.ds(start, WIDTH), lanes)
            got, sums = weigh(
                q_in[q_slice].reshape(shape[0], HD),
                k_in[k_slice].reshape(shape[1], HD),
                v_in[k_slice].reshape(shape[1], HD),
                allowed,
            )
            o_out[q_slice] = got.reshape(q_rows, WIDTH, HD)
            if keep is not None:
                stats[c * (cw // WIDTH) + b, pl.ds(h, 1)] = spread(sums, shape[0], keep)

    strips = cw // WIDTH

    def partial(kind, slot, j, rows, layer, base):
        return remote(
            o_out.at[pl.ds(rows, LAYER), pl.ds(j * cw, cw)],
            p_in.at[pl.ds(base, LAYER), pl.ds(j * cw, cw)],
            part_send.at[kind, j], part_recv.at[slot, j], layer * LAYER + s, head,
        )

    def partial_stats(kind, slot, j, layer):
        at = pl.ds(j * strips, strips)
        return remote(
            stats.at[at], stats_in.at[slot, at],
            stat_send.at[kind, j], stat_recv.at[slot, j], layer * LAYER + s, head,
        )

    def back(j, d):
        row = peers[d]
        return remote(
            o_out.at[row, pl.ds(j * cw, cw)],
            joined.at[head, pl.ds(back_start + j * cw, cw), feats],
            back_send.at[j, d], back_recv.at[head * per + lax.rem(s, per), j],
            here(row), back_head,
        )

    def back_all(j):
        for d in (2, 3, 1):
            back(j, d).start()

        @pl.when(jnp.logical_not(stays))
        def _():
            back(j, 0).start()

        @pl.when(stays)
        def _():
            joined[head, pl.ds(pl.multiple_of(back_start + j * cw, WIDTH), cw), feats] = o_out[
                s, pl.ds(pl.multiple_of(j * cw, WIDTH), cw)
            ]

    def ext(j):
        for t in (1, 2):
            for d in (1, 2, 3):
                lay(t, j, d, True).wait_recv()
        for kind, t, base in ((0, 1, 0), (1, 2, 0), (2, 0, LAYER), (3, 0, 2 * LAYER)):
            for d in range(4):
                up_arrival(kind, t, j, d, base).wait_recv()
        for b in range(strips):
            small(LAYER, 2 * LAYER, 0, 2 * LAYER, j, b, None, 0)
        for kind, rows, layer in ((0, LAYER, 2), (1, 2 * LAYER, 3)):
            partial(kind, 0, j, rows, layer, 0).start()
            partial_stats(kind, 0, j, layer).start()

    def own(c):
        @pl.when(z == 0)
        def _():
            for t, ds in ((0, (1, 2, 3)), (1, (1,)), (2, (1,))):
                for d in ds:
                    lay(t, c, d, True).wait_recv()
            for b in range(strips):
                small(0, LAYER, LAYER, LAYER, c, b, 0, None)
            back_all(c)

        @pl.when(z == 1)
        def _():
            for d in (1, 2, 3):
                lay(0, c, d, True).wait_recv()
            for b in range(strips):
                small(0, LAYER, 0, 2 * LAYER, c, b, LAYER, None)
            back_all(c)

        @pl.when(z >= 2)
        def _():
            lay(0, c, 1, True).wait_recv()
            for t in (1, 2):
                for d in (1, 2, 3):
                    lay(t, c, d, True).wait_recv()

        @pl.when(z == 2)
        def _():
            for d in range(4):
                up_arrival(2, 0, c, d, LAYER).wait_recv()
            for b in range(strips):
                small(0, 2 * LAYER, LAYER, LAYER, c, b, 0, 0)
            partial(0, 1, c, LAYER, 3, LAYER).start()
            partial_stats(0, 1, c, 3).start()

        @pl.when(z == 3)
        def _():
            for b in range(strips):
                small(0, LAYER, LAYER, LAYER, c, b, 0, size)

    def combine(c):
        def weights(lines):
            top = functools.reduce(jnp.maximum, lines)
            terms = [jnp.exp(line - top) for line in lines]
            total = functools.reduce(jnp.add, terms)
            return [term / total for term in terms]

        def mix(b, lines, off):
            start = pl.multiple_of(c * cw + b * WIDTH, WIDTH)
            shares = weights(lines)
            for h in range(heads):
                lanes = pl.ds(h * HD, HD)
                at = (pl.ds(0, LAYER), pl.ds(start, WIDTH), lanes)
                parts = [o_out[at], p_in[at]]
                if len(lines) == 3:
                    parts.append(p_in[pl.ds(LAYER, LAYER), pl.ds(start, WIDTH), lanes])
                total = 0.0
                for part, share in zip(parts, shares):
                    weight = column(share[h : h + 1], size, off)
                    total += part.reshape(size, HD).astype(jnp.float32) * weight
                o_out[at] = total.astype(jnp.bfloat16).reshape(LAYER, WIDTH, HD)

        def wait(slot):
            partial(0, slot, c, 0, 0, slot * LAYER).wait_recv()
            partial_stats(0, slot, c, 0).wait_recv()

        @pl.when(z == 2)
        def _():
            wait(0)
            for b in range(strips):
                strip = c * strips + b
                mix(b, [stats[strip, :heads], stats_in[0, strip, :heads]], 0)
            back_all(c)

        @pl.when(z == 3)
        def _():
            wait(0)
            wait(1)
            for b in range(strips):
                strip = c * strips + b
                mix(
                    b,
                    [stats[strip, :heads], stats_in[0, strip, :heads], stats_in[1, strip, :heads]],
                    size,
                )
            back_all(c)

    def step_of(h, u):
        j = 2 * h + u
        tiles_of = [start for i, start in enumerate(range(0, stride, tile)) if (i % 4 in (0, 3)) == (u == 0)]
        for start in tiles_of:
            row_tile(h, start)
        for layer in routes:

            @pl.when(z == layer)
            def _():
                relay(layer, j)

                @pl.when(j + AHEAD < CHUNKS)
                def _():
                    direct(layer, j + AHEAD)

        @pl.when(z == 1)
        def _():
            ext(j)

        if u == 0:

            @pl.when(h > 0)
            def _():
                w_in(1, h - 1)

        else:
            w_in(0, h)

        @pl.when(h >= heads // 2)
        def _():
            c = 4 * (h - heads // 2) + 2 * u
            own(c)
            own(c + 1)

    @pl.loop(0, heads)
    def _(h):
        step_of(h, 0)
        step_of(h, 1)

    row_copy = remote(
        row_out.at[pl.ds(pl.multiple_of(other * half, half), half)],
        joined.at[head, :, pl.ds(0, block)], row_send, row_recv, me, other,
    )
    row_copy.start()
    joined[head, :, pl.ds(0, block)] = row_out[pl.ds(pl.multiple_of(head * half, half), half)]

    w_in(1, PIECES - 1)

    @pl.when(jnp.logical_not(z_early))
    def _():
        @pl.loop(0, PIECES)
        def _(k):
            w_side(1, k).start()

    local[6].wait()
    step = 512
    count = staged.shape[1] // step

    def tiles(add):
        @pl.loop(0, count)
        def _(c):
            add(pl.ds(pl.multiple_of(c * step, step), step))

    def own_row_part(lanes):
        summed[:, lanes] = jnp.dot(
            joined[head, :, pl.ds(0, block)],
            w_own[pl.ds(0, block), lanes],
            preferred_element_type=jnp.float32,
        )

    tiles(own_row_part)

    @pl.when(z >= 2)
    def _():
        @pl.loop(0, CHUNKS - 2)
        def _(c):
            combine(c)

    @pl.loop(0, PIECES)
    def _(k):
        w_on(0, k)

    @pl.when(z >= 2)
    def _():
        @pl.loop(CHUNKS - 2, CHUNKS)
        def _(c):
            combine(c)

    @pl.loop(0, PIECES)
    def _(k):
        w_on(1, k)

    def w_from_sibling(first, last):
        @pl.loop(first, last)
        def _(k):
            for q in range(4):
                w_copy(w_other, q, 1 - core, k, 1, here(sib), head).wait_recv()

    w_from_sibling(0, PIECES // 2)
    row_copy.wait_recv()

    def other_row_part(lanes):
        summed[:, lanes] += jnp.dot(
            joined[other, :, pl.ds(0, block)],
            w_other[pl.ds(0, block), lanes],
            preferred_element_type=jnp.float32,
        )

    tiles(other_row_part)

    def back_wait(source_head):
        for slot in range(per):
            mine = (head * per + slot == s) & (head == source_head)

            @pl.when(jnp.logical_not(mine))
            def _():
                @pl.loop(0, CHUNKS)
                def _(j):
                    remote(
                        o_out.at[0, pl.ds(j * cw, cw)],
                        joined.at[source_head, pl.ds(slot * cols + j * cw, cw), feats],
                        back_send.at[j, 0], back_recv.at[source_head * per + slot, j],
                        me, other,
                    ).wait_recv()

    back_wait(head)
    back_wait(other)
    w_from_sibling(PIECES // 2, PIECES)

    def leave(c):
        lanes = pl.ds(pl.multiple_of(c * step, step), step)
        return pltpu.make_async_copy(staged.at[:, lanes], out_hbm.at[:, lanes], out_sem.at[c])

    @pl.loop(0, count)
    def _(c):
        lanes = pl.ds(pl.multiple_of(c * step, step), step)
        total = summed[:, lanes] + jnp.dot(
            joined[head, :, feats], w_own[feats, lanes], preferred_element_type=jnp.float32
        )
        total += jnp.dot(
            joined[other, :, feats], w_other[feats, lanes], preferred_element_type=jnp.float32
        )
        staged[:, lanes] = total.astype(jnp.bfloat16)
        leave(c).start()

    @pl.loop(0, CHUNKS)
    def _(j):
        for t in range(3):
            for d in (1, 2, 3):
                lay(t, j, d, False).wait_send()
        for layer in routes:

            @pl.when(z == layer)
            def _():
                for kind, t, to, base in routes[layer]:
                    for d in range(4):
                        up(kind, t, j, d, to, base).wait_send()

        @pl.when(z == 1)
        def _():
            for kind, rows, layer in ((0, LAYER, 2), (1, 2 * LAYER, 3)):
                partial(kind, 0, j, rows, layer, 0).wait_send()
                partial_stats(kind, 0, j, layer).wait_send()

        @pl.when(z == 2)
        def _():
            partial(0, 1, j, LAYER, 3, LAYER).wait_send()
            partial_stats(0, 1, j, 3).wait_send()

        for d in (1, 2, 3):
            back(j, d).wait_send()

        @pl.when(jnp.logical_not(stays))
        def _():
            back(j, 0).wait_send()

    @pl.loop(0, PIECES)
    def _(k):
        for q in (0, 1):
            w_first(q, k).wait_send()
            w_here(q, k).wait_send()
            w_side(q, k).wait_send()
            w_beside(q, k).wait_send()

    row_copy.wait_send()

    @pl.loop(0, count)
    def _(c):
        leave(c).wait()


def call_layered(n, queries, keys, values, w_out, half):
    _, stride, local_feat = queries.shape
    depth, width = w_out.shape
    block = local_feat // 2
    cols = stride // LAYER
    bf16, f32 = jnp.bfloat16, jnp.float32
    dma = pltpu.SemaphoreType.DMA
    blocks = cols // WIDTH
    return pl.pallas_call(
        functools.partial(layered, n),
        out_shape=jax.ShapeDtypeStruct((half, width), bf16),
        in_specs=[pl.BlockSpec(memory_space=pltpu.HBM)] * 4,
        out_specs=pl.BlockSpec(memory_space=pltpu.HBM),
        scratch_shapes=[pltpu.VMEM((stride, block), bf16)] * 3
        + [
            pltpu.VMEM((3 * LAYER, cols, block), bf16),
            pltpu.VMEM((2 * LAYER, cols, block), bf16),
            pltpu.VMEM((2 * LAYER, cols, block), bf16),
            pltpu.VMEM((3 * LAYER, cols, block), bf16),
            pltpu.VMEM((2 * LAYER, cols, block), bf16),
            pltpu.VMEM((blocks, 8, HD), f32),
            pltpu.VMEM((2, blocks, 8, HD), f32),
            pltpu.VMEM((stride, block), bf16),
            pltpu.VMEM((2, half, local_feat), bf16),
            pltpu.VMEM((half, width), f32),
            pltpu.VMEM((depth, width), bf16),
            pltpu.VMEM((depth, width), bf16),
            pltpu.VMEM((half, width), bf16),
            dma((7,)),
            dma((3 * CHUNKS, LAYER)),
            dma((3 * CHUNKS, LAYER)),
            dma((4 * CHUNKS, LAYER)),
            dma((4 * CHUNKS, LAYER)),
            dma((2, CHUNKS)),
            dma((2, CHUNKS)),
            dma((2, CHUNKS)),
            dma((2, CHUNKS)),
            dma((CHUNKS, LAYER)),
            dma((2 * (half // cols), CHUNKS)),
            dma((3, 8 * PIECES)),
            dma((8 * PIECES,)),
            dma,
            dma,
            dma((width // 512,)),
        ],
        compiler_params=pltpu.CompilerParams(has_side_effects=True, vmem_limit_bytes=60 * 2**20),
    )(queries, keys, values, w_out)


def body(
    n, q_hbm, k_hbm, v_hbm, w_hbm, out_ref, q_row, k_row, v_row, q_col, k_col, v_col,
    col_out, row_out, joined, summed, w_own, w_other, local_sem, in_send, in_recv, back_send, back_recv,
    w_send, w_recv, row_send, row_recv,
):
    me, head = lax.axis_index("ctx"), lax.axis_index("head")
    other = 1 - head
    stride = q_hbm.shape[1]
    block = q_row.shape[1]
    depth = w_own.shape[0]
    half = joined.shape[1]
    cols = stride // n
    share = block // PARTS
    hbm = (q_hbm, k_hbm, v_hbm)
    rows_in = (q_row, k_row, v_row)
    cols_in = (q_col, k_col, v_col)
    back_head = lax.div(me * cols, half)
    member = lax.rem(me, 4)
    sibling = me + 1 - 2 * lax.rem(me, 2)
    beside = me + 2 - 4 * lax.div(member, 2)
    piece = depth // (4 * SHARES)

    def col_copy(t, part, d):
        peer = lax.rem(me + d, n)
        lanes = pl.ds(part * share, share)
        return pltpu.make_async_remote_copy(
            src_ref=hbm[t].at[0, pl.ds(peer * cols, cols), pl.ds(block + part * share, share)],
            dst_ref=cols_in[t].at[me, :, lanes],
            send_sem=in_send.at[t * PARTS + part, d],
            recv_sem=in_recv.at[t * PARTS + part, d],
            device_id=(peer, head),
            device_id_type=MESH,
        )

    def col_arrival(t, part, d):
        source = lax.rem(me + n - d, n)
        lanes = pl.ds(part * share, share)
        return pltpu.make_async_remote_copy(
            src_ref=hbm[t].at[0, pl.ds(0, cols), pl.ds(block + part * share, share)],
            dst_ref=cols_in[t].at[source, :, lanes],
            send_sem=in_send.at[t * PARTS + part, d],
            recv_sem=in_recv.at[t * PARTS + part, d],
            device_id=(source, head),
            device_id_type=MESH,
        )

    def w_copy(source, index, way, to_ctx, to_head):
        rows = pl.ds(index * piece, piece)
        return pltpu.make_async_remote_copy(
            src_ref=source.at[rows],
            dst_ref=w_other.at[rows],
            send_sem=w_send.at[way, index],
            recv_sem=w_recv.at[index],
            device_id=(to_ctx, to_head),
            device_id_type=MESH,
        )

    def index_of(who, s):
        return who * SHARES + s

    member_sibling = lax.rem(sibling, 4)
    member_beside = lax.rem(beside, 4)
    member_far = lax.rem(member + 2, 4) + 1 - 2 * lax.rem(member, 2)

    for part in range(PARTS):

        @pl.loop(1, n)
        def _(d):
            for t in range(3):
                col_copy(t, part, d).start()

    @pl.loop(0, SHARES)
    def _(s):
        w_copy(w_hbm, index_of(member, s), 0, me, other).start()

    @pl.loop(SHARES - STRAIGHT, SHARES)
    def _(s):
        w_copy(w_hbm, index_of(member_beside, s), 0, me, other).start()

    local = [
        pltpu.make_async_copy(hbm[t].at[0, :, pl.ds(0, block)], rows_in[t], local_sem.at[t])
        for t in range(3)
    ]
    local += [
        pltpu.make_async_copy(
            hbm[t].at[0, pl.ds(me * cols, cols), pl.ds(block, block)],
            cols_in[t].at[me],
            local_sem.at[3 + t],
        )
        for t in range(3)
    ]
    local.append(pltpu.make_async_copy(w_hbm, w_own, local_sem.at[6]))
    for copy in local:
        copy.start()
    for copy in local[:3]:
        copy.wait()

    tile = min(256, half)
    row_index = lax.broadcasted_iota(jnp.int32, (tile, stride), 0)
    key_index = lax.broadcasted_iota(jnp.int32, (tile, stride), 1)

    @pl.loop(0, block // HD)
    def _(h):
        lanes = pl.ds(pl.multiple_of(h * HD, HD), HD)
        for start in range(0, stride, tile):
            end = start + tile
            row_out[pl.ds(start, tile), lanes] = attend(
                q_row[pl.ds(start, tile), lanes],
                k_row[pl.ds(0, end), lanes],
                v_row[pl.ds(0, end), lanes],
                key_index[:, :end] <= row_index[:, :end] + start,
            )

    row_copy = pltpu.make_async_remote_copy(
        src_ref=row_out.at[pl.ds(pl.multiple_of(other * half, half), half)],
        dst_ref=joined.at[head, :, pl.ds(0, block)],
        send_sem=row_send,
        recv_sem=row_recv,
        device_id=(me, other),
        device_id_type=MESH,
    )
    row_copy.start()
    joined[head, :, pl.ds(0, block)] = row_out[pl.ds(pl.multiple_of(head * half, half), half)]

    def onward(first, last):
        @pl.loop(first, last)
        def _(s):
            index = index_of(member, s)
            w_copy(w_hbm, index, 0, me, other).wait_recv()

            @pl.when(s < SHARES - STRAIGHT)
            def _():
                w_copy(w_other, index, 1, beside, head).start()

            w_copy(w_other, index, 2, sibling, head).start()

    onward(0, SHARES // 2)

    for copy in local[3:]:
        copy.wait()

    step = 512

    def tiles(add):
        @pl.loop(0, out_ref.shape[1] // step)
        def _(c):
            add(pl.ds(pl.multiple_of(c * step, step), step))

    def own_row_part(lanes):
        summed[:, lanes] = jnp.dot(
            joined[head, :, pl.ds(0, block)],
            w_own[pl.ds(0, block), lanes],
            preferred_element_type=jnp.float32,
        )

    tiles(own_row_part)
    width = min(cols, max(16, 256 // n))
    size = n * width
    r_index = lax.broadcasted_iota(jnp.int32, (size, size), 0)
    s_index = lax.broadcasted_iota(jnp.int32, (size, size), 1)
    allowed = (s_index <= r_index) & (((r_index - s_index) & (width - 1)) == 0)

    slot_here = lax.rem(me, n // 2)
    stays = back_head == head

    def landing(source_head, part, slot):
        return joined.at[
            source_head,
            pl.ds(pl.multiple_of(slot * cols, cols), cols),
            pl.ds(block + part * share, share),
        ]

    def back_copy(part, r):
        return pltpu.make_async_remote_copy(
            src_ref=col_out.at[r, :, pl.ds(part * share, share)],
            dst_ref=landing(head, part, slot_here),
            send_sem=back_send.at[part, r],
            recv_sem=back_recv.at[head * PARTS + part, slot_here],
            device_id=(r, back_head),
            device_id_type=MESH,
        )

    def back_arrival(source_head, part, slot):
        return pltpu.make_async_remote_copy(
            src_ref=col_out.at[0, :, pl.ds(part * share, share)],
            dst_ref=landing(source_head, part, slot),
            send_sem=back_send.at[part, 0],
            recv_sem=back_recv.at[source_head * PARTS + part, slot],
            device_id=(me, other),
            device_id_type=MESH,
        )

    for part in range(PARTS):

        @pl.loop(1, n)
        def _(d):
            for t in range(3):
                col_arrival(t, part, d).wait_recv()

        @pl.loop(part * (share // HD), (part + 1) * (share // HD))
        def _(h):
            lanes = pl.ds(pl.multiple_of(h * HD, HD), HD)
            for start in range(0, cols, width):
                at = (slice(None), pl.ds(start, width), lanes)
                got = attend(*(ref[at].reshape(size, HD) for ref in cols_in), allowed)
                col_out[at] = got.reshape(n, width, HD)

        @pl.loop(1, n)
        def _(d):
            back_copy(part, lax.rem(me + d, n)).start()

        @pl.when(stays)
        def _():
            rows = pl.ds(pl.multiple_of(slot_here * cols, cols), cols)
            joined[head, rows, pl.ds(block + part * share, share)] = col_out[
                me, :, pl.ds(part * share, share)
            ]

        @pl.when(jnp.logical_not(stays))
        def _():
            back_copy(part, me).start()

        if part == 0:
            onward(SHARES // 2, SHARES)

    @pl.loop(0, SHARES)
    def _(s):
        index = index_of(member_beside, s)
        w_copy(w_other, index, 1, beside, head).wait_recv()
        w_copy(w_other, index, 3, sibling, head).start()

    row_copy.wait_recv()

    def back_wait(source_head):
        @pl.loop(0, n // 2)
        def _(slot):
            mine = (head * (n // 2) + slot == me) & (head == source_head)

            @pl.when(jnp.logical_not(mine))
            def _():
                for part in range(PARTS):
                    back_arrival(source_head, part, slot).wait_recv()

    back_wait(head)

    def own_col_part(lanes):
        summed[:, lanes] += jnp.dot(
            joined[head, :, pl.ds(block, block)],
            w_own[pl.ds(block, block), lanes],
            preferred_element_type=jnp.float32,
        )

    tiles(own_col_part)

    @pl.loop(0, SHARES)
    def _(s):
        w_copy(w_other, index_of(member_sibling, s), 2, sibling, head).wait_recv()
        w_copy(w_other, index_of(member_far, s), 3, sibling, head).wait_recv()

    back_wait(other)

    def other_part(lanes):
        total = summed[:, lanes] + jnp.dot(
            joined[other], w_other[:, lanes], preferred_element_type=jnp.float32
        )
        out_ref[:, lanes] = total.astype(jnp.bfloat16)

    tiles(other_part)

    for part in range(PARTS):

        @pl.loop(1, n)
        def _(d):
            for t in range(3):
                col_copy(t, part, d).wait_send()

    @pl.loop(0, SHARES)
    def _(s):
        w_copy(w_hbm, index_of(member, s), 0, me, other).wait_send()
        w_copy(w_other, index_of(member, s), 2, sibling, head).wait_send()
        w_copy(w_other, index_of(member_beside, s), 3, sibling, head).wait_send()

    @pl.loop(0, SHARES - STRAIGHT)
    def _(s):
        w_copy(w_other, index_of(member, s), 1, beside, head).wait_send()

    @pl.loop(SHARES - STRAIGHT, SHARES)
    def _(s):
        w_copy(w_hbm, index_of(member_beside, s), 0, me, other).wait_send()

    row_copy.wait_send()

    for part in range(PARTS):

        @pl.loop(1, n)
        def _(d):
            back_copy(part, lax.rem(me + d, n)).wait_send()

        @pl.when(jnp.logical_not(stays))
        def _():
            back_copy(part, me).wait_send()


def on_device(n, queries, keys, values, w_out):
    _, stride, local_feat = queries.shape
    depth, model_width = w_out.shape
    block = GROUP * HD
    assert queries.shape[0] == 1 and local_feat == 2 * block
    half = stride // lax.axis_size("head")
    cols = stride // n
    if n == LAYER * LAYER and stride % (LAYER * CHUNKS * WIDTH) == 0:
        out = call_layered(n, queries, keys, values, w_out, half)
        return out.reshape((1, half, model_width))
    bf16 = jnp.bfloat16
    dma = pltpu.SemaphoreType.DMA
    out = pl.pallas_call(
        functools.partial(body, n),
        out_shape=jax.ShapeDtypeStruct((half, model_width), bf16),
        in_specs=[pl.BlockSpec(memory_space=pltpu.HBM)] * 4,
        out_specs=pl.BlockSpec(memory_space=pltpu.VMEM),
        scratch_shapes=[pltpu.VMEM((stride, block), bf16)] * 3
        + [pltpu.VMEM((n, cols, block), bf16)] * 4
        + [
            pltpu.VMEM((stride, block), bf16),
            pltpu.VMEM((2, half, local_feat), bf16),
            pltpu.VMEM((half, model_width), jnp.float32),
            pltpu.VMEM((depth, model_width), bf16),
            pltpu.VMEM((depth, model_width), bf16),
            dma((7,)),
            dma((3 * PARTS, n)),
            dma((3 * PARTS, n)),
            dma((PARTS, n)),
            dma((2 * PARTS, n // 2)),
            dma((4, 4 * SHARES)),
            dma((4 * SHARES,)),
            dma,
            dma,
        ],
        compiler_params=pltpu.CompilerParams(has_side_effects=True, vmem_limit_bytes=60 * 2**20),
    )(queries, keys, values, w_out)
    return out.reshape((1, half, model_width))


def solution(mesh):
    return jax.shard_map(
        functools.partial(on_device, mesh.shape["ctx"]),
        mesh=mesh,
        in_specs=(
            P("ctx", None, "head"),
            P("ctx", None, "head"),
            P("ctx", None, "head"),
            P("head", None),
        ),
        out_specs=P("ctx", "head", None),
        check_vma=False,
    )
```

```python
import functools

import jax
import jax.numpy as jnp
from jax import lax
from jax.experimental import pallas as pl
from jax.experimental.pallas import tpu as pltpu
from jax.sharding import PartitionSpec as P

HD = 128
GROUP = 4
MESH = pl.DeviceIdType.MESH
SHARES = 8
STRAIGHT = 2
PARTS = 2
LAYER = 4
CHUNKS = 8
WIDTH = 16
WIDTH_LOG = 4
PIECES = 4
AHEAD = 3

masked_score = -1e30


def attend(query, key, value, allowed):
    scores = lax.dot_general(
        query, key, (((1,), (1,)), ((), ())), preferred_element_type=jnp.float32
    ) * jnp.float32(1.0 / HD**0.5)
    scores = jnp.where(allowed, scores, masked_score)
    top = jnp.max(scores, axis=-1, keepdims=True)
    expo = jnp.exp(scores - top)
    total = jnp.sum(expo, axis=-1, keepdims=True)
    mixed = jnp.dot(expo.astype(jnp.bfloat16), value, preferred_element_type=jnp.float32)
    return (mixed / total).astype(jnp.bfloat16)


def weigh(query, key, value, allowed):
    scores = lax.dot_general(
        query, key, (((1,), (1,)), ((), ())), preferred_element_type=jnp.float32
    ) * jnp.float32(1.0 / HD**0.5)
    if allowed is not None:
        scores = jnp.where(allowed, scores, masked_score)
    top = jnp.max(scores, axis=-1, keepdims=True)
    expo = jnp.exp(scores - top)
    total = jnp.sum(expo, axis=-1, keepdims=True)
    mixed = jnp.dot(expo.astype(jnp.bfloat16), value, preferred_element_type=jnp.float32)
    return (mixed / total).astype(jnp.bfloat16), top + jnp.log(total)


def layered(
    n, q_hbm, k_hbm, v_hbm, w_hbm, out_hbm, q_row, k_row, v_row, q_in, k_in, v_in, o_out, p_in,
    stats, stats_in, row_out, joined, summed, w_own, w_other, staged,
    local_sem, lay_send, lay_recv, up_send, up_recv, part_send, part_recv, stat_send, stat_recv,
    back_send, back_recv, w_send, w_recv, row_send, row_recv, out_sem,
):
    me, head = lax.axis_index("ctx"), lax.axis_index("head")
    other = 1 - head
    z, s = lax.div(me, LAYER), lax.rem(me, LAYER)
    core = lax.rem(s, 2)
    sib = s + 1 - 2 * core
    opp = s + 2 - 4 * lax.div(s, 2)
    far = sib + 2 - 4 * lax.div(sib, 2)
    peers = (s, sib, opp, far)
    stride = q_hbm.shape[1]
    block = q_row.shape[1]
    depth = w_own.shape[0]
    half = joined.shape[1]
    cols = stride // LAYER
    cw = cols // CHUNKS
    per = half // cols
    hbm = (q_hbm, k_hbm, v_hbm)
    ins = (q_in, k_in, v_in)
    own_at = (0, LAYER, LAYER)
    back_head = lax.div(s * cols, half)
    back_start = lax.rem(s * cols, half)
    stays = back_head == head
    feats = pl.ds(block, block)

    def remote(src, dst, send, recv, ctx, at):
        return pltpu.make_async_remote_copy(
            src_ref=src, dst_ref=dst, send_sem=send, recv_sem=recv,
            device_id=(ctx, at), device_id_type=MESH,
        )

    def here(slot):
        return z * LAYER + slot

    def lay(t, j, d, source):
        row = peers[d] if source else s
        return remote(
            hbm[t].at[0, pl.ds(peers[d] * cols + j * cw, cw), feats],
            ins[t].at[own_at[t] + row, pl.ds(j * cw, cw)],
            lay_send.at[t * CHUNKS + j, d], lay_recv.at[t * CHUNKS + j, d],
            here(peers[d]), head,
        )

    def up(kind, t, j, d, layer, base):
        if d < 2:
            src, slot, row = hbm[t].at[0, pl.ds(peers[d] * cols + j * cw, cw), feats], peers[d], s
        else:
            src, slot, row = ins[t].at[own_at[t] + peers[d], pl.ds(j * cw, cw)], s, peers[d]
        return remote(
            src, ins[t].at[base + row, pl.ds(j * cw, cw)],
            up_send.at[kind * CHUNKS + j, d], up_recv.at[kind * CHUNKS + j, d],
            layer * LAYER + slot, head,
        )

    def up_arrival(kind, t, j, d, base):
        return remote(
            hbm[t].at[0, pl.ds(0, cw), feats], ins[t].at[base + peers[d], pl.ds(j * cw, cw)],
            up_send.at[kind * CHUNKS + j, d], up_recv.at[kind * CHUNKS + j, d],
            here(sib), head,
        )

    routes = {
        0: ((0, 1, 1, 0), (1, 2, 1, 0)),
        2: ((2, 0, 1, LAYER),),
        3: ((3, 0, 1, 2 * LAYER), (2, 0, 2, LAYER)),
    }

    def direct(layer, j):
        for kind, t, to, base in routes[layer]:
            for d in (0, 1):
                up(kind, t, j, d, to, base).start()

    def relay(layer, j):
        for t in sorted({t for _, t, _, _ in routes[layer]}):
            for d in (2, 3):
                lay(t, j, d, True).wait_recv()
                for kind, t2, to, base in routes[layer]:
                    if t2 == t:
                        up(kind, t, j, d, to, base).start()

    def piece_rows(q, c, k):
        eighth = depth // 16
        rows = eighth // (PIECES // 2)
        start = lax.div(k, PIECES // 2) * (depth // 2)
        start += (q * 2 + c) * eighth + lax.rem(k, PIECES // 2) * rows
        return pl.ds(start, rows)

    def w_copy(source, q, c, k, way, to_ctx, to_head):
        rows = piece_rows(q, c, k)
        index = (q * 2 + c) * PIECES + k
        return remote(
            source.at[rows], w_other.at[rows], w_send.at[way, index], w_recv.at[index], to_ctx, to_head
        )

    even = lax.rem(z + lax.div(s, 2), 2)
    y_next = here(opp)
    z_next = me + LAYER - 2 * LAYER * lax.rem(z, 2)
    z_early = (z == 1) | (z == 2)

    def w_first(q, k):
        return w_copy(w_hbm, 2 * even + q, core, k, 0, me, other)

    def w_side(q, k):
        return w_copy(w_other, 2 * even + q, core, k, 2, y_next if q == 0 else z_next, head)

    def w_beside(q, k):
        return w_copy(w_other, 2 * (1 - even) + q, core, k, 1, here(sib), head)

    def w_here(q, k):
        return w_copy(w_other, 2 * even + q, core, k, 1, here(sib), head)

    def w_in(q, k):
        w_first(q, k).wait_recv()
        w_here(q, k).start()
        if q == 0:
            w_side(q, k).start()
        else:

            @pl.when(z_early)
            def _():
                w_side(q, k).start()

    def w_on(q, k):
        w_copy(w_other, 2 * (1 - even) + q, core, k, 2, me, other).wait_recv()
        w_beside(q, k).start()

    def exchange(ts):
        @pl.loop(0, CHUNKS)
        def _(j):
            for t in ts:
                for d in (2, 3, 1):
                    lay(t, j, d, False).start()

    for layer in routes:

        @pl.when(z == layer)
        def _():
            for j in range(AHEAD):
                direct(layer, j)

    @pl.when(z < 2)
    def _():
        exchange((1, 2))
        exchange((0,))

    @pl.when(z >= 2)
    def _():
        exchange((0,))
        exchange((1, 2))

    @pl.loop(0, PIECES)
    def _(k):
        w_first(0, k).start()
        w_first(1, k).start()

    local = [
        pltpu.make_async_copy(hbm[t].at[0, :, pl.ds(0, block)], (q_row, k_row, v_row)[t], local_sem.at[t])
        for t in range(3)
    ]
    local += [
        pltpu.make_async_copy(
            hbm[t].at[0, pl.ds(s * cols, cols), feats], ins[t].at[own_at[t] + s], local_sem.at[3 + t]
        )
        for t in range(3)
    ]
    local.append(pltpu.make_async_copy(w_hbm, w_own, local_sem.at[6]))
    for copy in local:
        copy.start()
    for copy in local[:6]:
        copy.wait()

    tile = min(256, half)
    row_index = lax.broadcasted_iota(jnp.int32, (tile, stride), 0)
    key_index = lax.broadcasted_iota(jnp.int32, (tile, stride), 1)

    def row_tile(h, start):
        lanes = pl.ds(pl.multiple_of(h * HD, HD), HD)
        end = start + tile
        row_out[pl.ds(start, tile), lanes] = attend(
            q_row[pl.ds(start, tile), lanes],
            k_row[pl.ds(0, end), lanes],
            v_row[pl.ds(0, end), lanes],
            key_index[:, :end] <= row_index[:, :end] + start,
        )

    def spread(sums):
        lane = lax.broadcasted_iota(jnp.int32, (HD, HD), 1)
        row = lax.broadcasted_iota(jnp.int32, (HD, HD), 0)
        return jnp.sum(jnp.where(lane == row, sums, 0.0), axis=0, keepdims=True)

    def column(line, off, period):
        lane = lax.broadcasted_iota(jnp.int32, (size, HD), 1)
        row = lax.broadcasted_iota(jnp.int32, (size, HD), 0)
        at = off + (row & (WIDTH - 1)) + lax.shift_right_logical(row, WIDTH_LOG) * period
        return jnp.sum(jnp.where(lane == at, line, 0.0), axis=1, keepdims=True)

    heads = block // HD
    size = LAYER * WIDTH

    def small(q_at, q_rows, k_at, k_rows, c, b, width, causal, keep):
        start = pl.multiple_of(c * cw + b * width, width)
        shape = (q_rows * width, k_rows * width)
        r = lax.broadcasted_iota(jnp.int32, shape, 0)
        m = lax.broadcasted_iota(jnp.int32, shape, 1)
        allowed = ((r - m) & (width - 1)) == 0
        if causal is not None:
            allowed &= m <= r + causal * width
        for h in range(heads):
            lanes = pl.ds(h * HD, HD)
            q_slice = (pl.ds(q_at, q_rows), pl.ds(start, width), lanes)
            k_slice = (pl.ds(k_at, k_rows), pl.ds(start, width), lanes)
            got, sums = weigh(
                q_in[q_slice].reshape(shape[0], HD),
                k_in[k_slice].reshape(shape[1], HD),
                v_in[k_slice].reshape(shape[1], HD),
                allowed,
            )
            o_out[q_slice] = got.reshape(q_rows, width, HD)
            if keep:
                stats[c * strips + b, pl.ds(h, 1)] = spread(sums)

    strips = cw // WIDTH

    def partial(kind, slot, j, rows, layer, base):
        return remote(
            o_out.at[pl.ds(rows, LAYER), pl.ds(j * cw, cw)],
            p_in.at[pl.ds(base, LAYER), pl.ds(j * cw, cw)],
            part_send.at[kind, j], part_recv.at[slot, j], layer * LAYER + s, head,
        )

    def partial_stats(kind, slot, j, layer):
        at = pl.ds(j * strips, strips)
        return remote(
            stats.at[at], stats_in.at[slot, at],
            stat_send.at[kind, j], stat_recv.at[slot, j], layer * LAYER + s, head,
        )

    def back(j, d):
        row = peers[d]
        return remote(
            o_out.at[row, pl.ds(j * cw, cw)],
            joined.at[head, pl.ds(back_start + j * cw, cw), feats],
            back_send.at[j, d], back_recv.at[head * per + lax.rem(s, per), j],
            here(row), back_head,
        )

    def back_all(j):
        for d in (2, 3, 1):
            back(j, d).start()

        @pl.when(jnp.logical_not(stays))
        def _():
            back(j, 0).start()

        @pl.when(stays)
        def _():
            joined[head, pl.ds(pl.multiple_of(back_start + j * cw, WIDTH), cw), feats] = o_out[
                s, pl.ds(pl.multiple_of(j * cw, WIDTH), cw)
            ]

    def ext(j):
        for t in (1, 2):
            for d in (1, 2, 3):
                lay(t, j, d, True).wait_recv()
        for kind, t, base in ((0, 1, 0), (1, 2, 0), (2, 0, LAYER), (3, 0, 2 * LAYER)):
            for d in range(4):
                up_arrival(kind, t, j, d, base).wait_recv()
        for b in range(strips):
            small(LAYER, 2 * LAYER, 0, 2 * LAYER, j, b, WIDTH, None, True)
        for kind, rows, layer in ((0, LAYER, 2), (1, 2 * LAYER, 3)):
            partial(kind, 0, j, rows, layer, 0).start()
            partial_stats(kind, 0, j, layer).start()

    def own(c):
        @pl.when(z == 0)
        def _():
            for t, ds in ((0, (1, 2, 3)), (1, (1,)), (2, (1,))):
                for d in ds:
                    lay(t, c, d, True).wait_recv()
            small(0, LAYER, LAYER, LAYER, c, 0, cw, 0, False)
            back_all(c)

        @pl.when(z == 1)
        def _():
            for d in (1, 2, 3):
                lay(0, c, d, True).wait_recv()
            small(0, LAYER, 0, 2 * LAYER, c, 0, cw, LAYER, False)
            back_all(c)

        @pl.when(z >= 2)
        def _():
            lay(0, c, 1, True).wait_recv()
            for t in (1, 2):
                for d in (1, 2, 3):
                    lay(t, c, d, True).wait_recv()

        @pl.when(z == 2)
        def _():
            for d in range(4):
                up_arrival(2, 0, c, d, LAYER).wait_recv()
            for b in range(strips):
                small(0, 2 * LAYER, LAYER, LAYER, c, b, WIDTH, 0, True)
            partial(0, 1, c, LAYER, 3, LAYER).start()
            partial_stats(0, 1, c, 3).start()

        @pl.when(z == 3)
        def _():
            small(0, LAYER, LAYER, LAYER, c, 0, cw, 0, True)

    def combine(c):
        def mix(b, parts):
            start = pl.multiple_of(c * cw + b * WIDTH, WIDTH)
            rows = pl.ds(start, WIDTH)
            for h in range(heads):
                lanes = pl.ds(h * HD, HD)
                lines = [column(ref[strip, pl.ds(h, 1)], off, period) for _, _, ref, strip, off, period in parts]
                top = functools.reduce(jnp.maximum, lines)
                terms = [jnp.exp(line - top) for line in lines]
                total = functools.reduce(jnp.add, terms)
                got = 0.0
                for (source, base, *_), term in zip(parts, terms):
                    value = source[pl.ds(base, LAYER), rows, lanes].reshape(size, HD)
                    got += value.astype(jnp.float32) * (term / total)
                o_out[pl.ds(0, LAYER), rows, lanes] = got.astype(jnp.bfloat16).reshape(LAYER, WIDTH, HD)

        def wait(slot):
            partial(0, slot, c, 0, 0, slot * LAYER).wait_recv()
            partial_stats(0, slot, c, 0).wait_recv()

        @pl.when(z == 2)
        def _():
            wait(0)
            for b in range(strips):
                strip = c * strips + b
                mix(
                    b,
                    [
                        (o_out, 0, stats, strip, 0, WIDTH),
                        (p_in, 0, stats_in.at[0], strip, 0, WIDTH),
                    ],
                )
            back_all(c)

        @pl.when(z == 3)
        def _():
            wait(0)
            wait(1)
            for b in range(strips):
                strip = c * strips + b
                mix(
                    b,
                    [
                        (o_out, 0, stats, c * strips, b * WIDTH, cw),
                        (p_in, 0, stats_in.at[0], strip, size, WIDTH),
                        (p_in, LAYER, stats_in.at[1], strip, size, WIDTH),
                    ],
                )
            back_all(c)

    row_copy = remote(
        row_out.at[pl.ds(pl.multiple_of(other * half, half), half)],
        joined.at[head, :, pl.ds(0, block)], row_send, row_recv, me, other,
    )
    step = 512
    count = staged.shape[1] // step

    def tiles(add):
        @pl.loop(0, count)
        def _(c):
            add(pl.ds(pl.multiple_of(c * step, step), step))

    def own_row_part(lanes):
        summed[:, lanes] = jnp.dot(
            joined[head, :, pl.ds(0, block)],
            w_own[pl.ds(0, block), lanes],
            preferred_element_type=jnp.float32,
        )

    @pl.loop(0, CHUNKS)
    def _(j):
        @pl.when(j < 2)
        def _():
            @pl.loop(j * (heads // 2), (j + 1) * (heads // 2))
            def _(h):
                for start in range(0, stride, tile):
                    row_tile(h, start)

        @pl.when(j == 1)
        def _():
            row_copy.start()
            joined[head, :, pl.ds(0, block)] = row_out[pl.ds(pl.multiple_of(head * half, half), half)]

        for layer in routes:

            @pl.when(z == layer)
            def _():
                relay(layer, j)

                @pl.when(j + AHEAD < CHUNKS)
                def _():
                    direct(layer, j + AHEAD)

        @pl.when(z == 1)
        def _():
            ext(j)

        @pl.when(j == 2)
        def _():
            local[6].wait()
            tiles(own_row_part)

        @pl.when((j > 0) & (lax.rem(j, 2) == 1))
        def _():
            w_in(0, lax.div(j, 2))

        @pl.when((j > 0) & (lax.rem(j, 2) == 0))
        def _():
            w_in(1, lax.div(j, 2) - 1)

        @pl.when(j >= CHUNKS // 2)
        def _():
            c = 2 * j - CHUNKS
            own(c)
            own(c + 1)

            @pl.when(z >= 2)
            def _():
                combine(j - CHUNKS // 2)

    w_in(1, PIECES - 1)

    @pl.when(jnp.logical_not(z_early))
    def _():
        @pl.loop(0, PIECES)
        def _(k):
            w_side(1, k).start()

    @pl.when(z >= 2)
    def _():
        @pl.loop(CHUNKS // 2, CHUNKS - 2)
        def _(c):
            combine(c)

    @pl.loop(0, PIECES)
    def _(k):
        w_on(0, k)

    @pl.when(z >= 2)
    def _():
        @pl.loop(CHUNKS - 2, CHUNKS)
        def _(c):
            combine(c)

    @pl.loop(0, PIECES // 2)
    def _(k):
        w_on(1, k)

    def w_from_sibling(qs, first, last):
        @pl.loop(first, last)
        def _(k):
            for q in qs:
                w_copy(w_other, q, 1 - core, k, 1, here(sib), head).wait_recv()

    w_from_sibling((0, 1, 2, 3), 0, PIECES // 2)
    row_copy.wait_recv()

    def other_row_part(lanes):
        summed[:, lanes] += jnp.dot(
            joined[other, :, pl.ds(0, block)],
            w_other[pl.ds(0, block), lanes],
            preferred_element_type=jnp.float32,
        )

    tiles(other_row_part)

    def back_wait(source_head):
        for slot in range(per):
            mine = (head * per + slot == s) & (head == source_head)

            @pl.when(jnp.logical_not(mine))
            def _():
                @pl.loop(0, CHUNKS)
                def _(j):
                    remote(
                        o_out.at[0, pl.ds(j * cw, cw)],
                        joined.at[source_head, pl.ds(slot * cols + j * cw, cw), feats],
                        back_send.at[j, 0], back_recv.at[source_head * per + slot, j],
                        me, other,
                    ).wait_recv()

    back_wait(head)
    back_wait(other)
    w_from_sibling((2 * even, 2 * even + 1), PIECES // 2, PIECES)
    quarter = block // 2
    early = pl.ds(pl.multiple_of(block + even * quarter, quarter), quarter)
    late = pl.ds(pl.multiple_of(block + (1 - even) * quarter, quarter), quarter)

    def col_part(lanes):
        total = summed[:, lanes] + jnp.dot(
            joined[head, :, feats], w_own[feats, lanes], preferred_element_type=jnp.float32
        )
        summed[:, lanes] = total + jnp.dot(
            joined[other, :, early], w_other[early, lanes], preferred_element_type=jnp.float32
        )

    tiles(col_part)

    @pl.loop(PIECES // 2, PIECES)
    def _(k):
        w_on(1, k)

    w_from_sibling((2 - 2 * even, 3 - 2 * even), PIECES // 2, PIECES)

    def leave(c):
        lanes = pl.ds(pl.multiple_of(c * step, step), step)
        return pltpu.make_async_copy(staged.at[:, lanes], out_hbm.at[:, lanes], out_sem.at[c])

    @pl.loop(0, count)
    def _(c):
        lanes = pl.ds(pl.multiple_of(c * step, step), step)
        total = summed[:, lanes] + jnp.dot(
            joined[other, :, late], w_other[late, lanes], preferred_element_type=jnp.float32
        )
        staged[:, lanes] = total.astype(jnp.bfloat16)
        leave(c).start()

    @pl.loop(0, CHUNKS)
    def _(j):
        for t in range(3):
            for d in (1, 2, 3):
                lay(t, j, d, False).wait_send()
        for layer in routes:

            @pl.when(z == layer)
            def _():
                for kind, t, to, base in routes[layer]:
                    for d in range(4):
                        up(kind, t, j, d, to, base).wait_send()

        @pl.when(z == 1)
        def _():
            for kind, rows, layer in ((0, LAYER, 2), (1, 2 * LAYER, 3)):
                partial(kind, 0, j, rows, layer, 0).wait_send()
                partial_stats(kind, 0, j, layer).wait_send()

        @pl.when(z == 2)
        def _():
            partial(0, 1, j, LAYER, 3, LAYER).wait_send()
            partial_stats(0, 1, j, 3).wait_send()

        for d in (1, 2, 3):
            back(j, d).wait_send()

        @pl.when(jnp.logical_not(stays))
        def _():
            back(j, 0).wait_send()

    @pl.loop(0, PIECES)
    def _(k):
        for q in (0, 1):
            w_first(q, k).wait_send()
            w_here(q, k).wait_send()
            w_side(q, k).wait_send()
            w_beside(q, k).wait_send()

    row_copy.wait_send()

    @pl.loop(0, count)
    def _(c):
        leave(c).wait()


def call_layered(n, queries, keys, values, w_out, half):
    _, stride, local_feat = queries.shape
    depth, width = w_out.shape
    block = local_feat // 2
    cols = stride // LAYER
    bf16, f32 = jnp.bfloat16, jnp.float32
    dma = pltpu.SemaphoreType.DMA
    blocks = cols // WIDTH
    return pl.pallas_call(
        functools.partial(layered, n),
        out_shape=jax.ShapeDtypeStruct((half, width), bf16),
        in_specs=[pl.BlockSpec(memory_space=pltpu.HBM)] * 4,
        out_specs=pl.BlockSpec(memory_space=pltpu.HBM),
        scratch_shapes=[pltpu.VMEM((stride, block), bf16)] * 3
        + [
            pltpu.VMEM((3 * LAYER, cols, block), bf16),
            pltpu.VMEM((2 * LAYER, cols, block), bf16),
            pltpu.VMEM((2 * LAYER, cols, block), bf16),
            pltpu.VMEM((3 * LAYER, cols, block), bf16),
            pltpu.VMEM((2 * LAYER, cols, block), bf16),
            pltpu.VMEM((blocks, 8, HD), f32),
            pltpu.VMEM((2, blocks, 8, HD), f32),
            pltpu.VMEM((stride, block), bf16),
            pltpu.VMEM((2, half, local_feat), bf16),
            pltpu.VMEM((half, width), f32),
            pltpu.VMEM((depth, width), bf16),
            pltpu.VMEM((depth, width), bf16),
            pltpu.VMEM((half, width), bf16),
            dma((7,)),
            dma((3 * CHUNKS, LAYER)),
            dma((3 * CHUNKS, LAYER)),
            dma((4 * CHUNKS, LAYER)),
            dma((4 * CHUNKS, LAYER)),
            dma((2, CHUNKS)),
            dma((2, CHUNKS)),
            dma((2, CHUNKS)),
            dma((2, CHUNKS)),
            dma((CHUNKS, LAYER)),
            dma((2 * (half // cols), CHUNKS)),
            dma((3, 8 * PIECES)),
            dma((8 * PIECES,)),
            dma,
            dma,
            dma((width // 512,)),
        ],
        compiler_params=pltpu.CompilerParams(has_side_effects=True, vmem_limit_bytes=60 * 2**20),
    )(queries, keys, values, w_out)


def body(
    n, q_hbm, k_hbm, v_hbm, w_hbm, out_ref, q_row, k_row, v_row, q_col, k_col, v_col,
    col_out, row_out, joined, summed, w_own, w_other, local_sem, in_send, in_recv, back_send, back_recv,
    w_send, w_recv, row_send, row_recv,
):
    me, head = lax.axis_index("ctx"), lax.axis_index("head")
    other = 1 - head
    stride = q_hbm.shape[1]
    block = q_row.shape[1]
    depth = w_own.shape[0]
    half = joined.shape[1]
    cols = stride // n
    share = block // PARTS
    hbm = (q_hbm, k_hbm, v_hbm)
    rows_in = (q_row, k_row, v_row)
    cols_in = (q_col, k_col, v_col)
    back_head = lax.div(me * cols, half)
    member = lax.rem(me, 4)
    sibling = me + 1 - 2 * lax.rem(me, 2)
    beside = me + 2 - 4 * lax.div(member, 2)
    piece = depth // (4 * SHARES)

    def col_copy(t, part, d):
        peer = lax.rem(me + d, n)
        lanes = pl.ds(part * share, share)
        return pltpu.make_async_remote_copy(
            src_ref=hbm[t].at[0, pl.ds(peer * cols, cols), pl.ds(block + part * share, share)],
            dst_ref=cols_in[t].at[me, :, lanes],
            send_sem=in_send.at[t * PARTS + part, d],
            recv_sem=in_recv.at[t * PARTS + part, d],
            device_id=(peer, head),
            device_id_type=MESH,
        )

    def col_arrival(t, part, d):
        source = lax.rem(me + n - d, n)
        lanes = pl.ds(part * share, share)
        return pltpu.make_async_remote_copy(
            src_ref=hbm[t].at[0, pl.ds(0, cols), pl.ds(block + part * share, share)],
            dst_ref=cols_in[t].at[source, :, lanes],
            send_sem=in_send.at[t * PARTS + part, d],
            recv_sem=in_recv.at[t * PARTS + part, d],
            device_id=(source, head),
            device_id_type=MESH,
        )

    def w_copy(source, index, way, to_ctx, to_head):
        rows = pl.ds(index * piece, piece)
        return pltpu.make_async_remote_copy(
            src_ref=source.at[rows],
            dst_ref=w_other.at[rows],
            send_sem=w_send.at[way, index],
            recv_sem=w_recv.at[index],
            device_id=(to_ctx, to_head),
            device_id_type=MESH,
        )

    def index_of(who, s):
        return who * SHARES + s

    member_sibling = lax.rem(sibling, 4)
    member_beside = lax.rem(beside, 4)
    member_far = lax.rem(member + 2, 4) + 1 - 2 * lax.rem(member, 2)

    for part in range(PARTS):

        @pl.loop(1, n)
        def _(d):
            for t in range(3):
                col_copy(t, part, d).start()

    @pl.loop(0, SHARES)
    def _(s):
        w_copy(w_hbm, index_of(member, s), 0, me, other).start()

    @pl.loop(SHARES - STRAIGHT, SHARES)
    def _(s):
        w_copy(w_hbm, index_of(member_beside, s), 0, me, other).start()

    local = [
        pltpu.make_async_copy(hbm[t].at[0, :, pl.ds(0, block)], rows_in[t], local_sem.at[t])
        for t in range(3)
    ]
    local += [
        pltpu.make_async_copy(
            hbm[t].at[0, pl.ds(me * cols, cols), pl.ds(block, block)],
            cols_in[t].at[me],
            local_sem.at[3 + t],
        )
        for t in range(3)
    ]
    local.append(pltpu.make_async_copy(w_hbm, w_own, local_sem.at[6]))
    for copy in local:
        copy.start()
    for copy in local[:3]:
        copy.wait()

    tile = min(256, half)
    row_index = lax.broadcasted_iota(jnp.int32, (tile, stride), 0)
    key_index = lax.broadcasted_iota(jnp.int32, (tile, stride), 1)

    @pl.loop(0, block // HD)
    def _(h):
        lanes = pl.ds(pl.multiple_of(h * HD, HD), HD)
        for start in range(0, stride, tile):
            end = start + tile
            row_out[pl.ds(start, tile), lanes] = attend(
                q_row[pl.ds(start, tile), lanes],
                k_row[pl.ds(0, end), lanes],
                v_row[pl.ds(0, end), lanes],
                key_index[:, :end] <= row_index[:, :end] + start,
            )

    row_copy = pltpu.make_async_remote_copy(
        src_ref=row_out.at[pl.ds(pl.multiple_of(other * half, half), half)],
        dst_ref=joined.at[head, :, pl.ds(0, block)],
        send_sem=row_send,
        recv_sem=row_recv,
        device_id=(me, other),
        device_id_type=MESH,
    )
    row_copy.start()
    joined[head, :, pl.ds(0, block)] = row_out[pl.ds(pl.multiple_of(head * half, half), half)]

    def onward(first, last):
        @pl.loop(first, last)
        def _(s):
            index = index_of(member, s)
            w_copy(w_hbm, index, 0, me, other).wait_recv()

            @pl.when(s < SHARES - STRAIGHT)
            def _():
                w_copy(w_other, index, 1, beside, head).start()

            w_copy(w_other, index, 2, sibling, head).start()

    onward(0, SHARES // 2)

    for copy in local[3:]:
        copy.wait()

    step = 512

    def tiles(add):
        @pl.loop(0, out_ref.shape[1] // step)
        def _(c):
            add(pl.ds(pl.multiple_of(c * step, step), step))

    def own_row_part(lanes):
        summed[:, lanes] = jnp.dot(
            joined[head, :, pl.ds(0, block)],
            w_own[pl.ds(0, block), lanes],
            preferred_element_type=jnp.float32,
        )

    tiles(own_row_part)
    width = min(cols, max(16, 256 // n))
    size = n * width
    r_index = lax.broadcasted_iota(jnp.int32, (size, size), 0)
    s_index = lax.broadcasted_iota(jnp.int32, (size, size), 1)
    allowed = (s_index <= r_index) & (((r_index - s_index) & (width - 1)) == 0)

    slot_here = lax.rem(me, n // 2)
    stays = back_head == head

    def landing(source_head, part, slot):
        return joined.at[
            source_head,
            pl.ds(pl.multiple_of(slot * cols, cols), cols),
            pl.ds(block + part * share, share),
        ]

    def back_copy(part, r):
        return pltpu.make_async_remote_copy(
            src_ref=col_out.at[r, :, pl.ds(part * share, share)],
            dst_ref=landing(head, part, slot_here),
            send_sem=back_send.at[part, r],
            recv_sem=back_recv.at[head * PARTS + part, slot_here],
            device_id=(r, back_head),
            device_id_type=MESH,
        )

    def back_arrival(source_head, part, slot):
        return pltpu.make_async_remote_copy(
            src_ref=col_out.at[0, :, pl.ds(part * share, share)],
            dst_ref=landing(source_head, part, slot),
            send_sem=back_send.at[part, 0],
            recv_sem=back_recv.at[source_head * PARTS + part, slot],
            device_id=(me, other),
            device_id_type=MESH,
        )

    for part in range(PARTS):

        @pl.loop(1, n)
        def _(d):
            for t in range(3):
                col_arrival(t, part, d).wait_recv()

        @pl.loop(part * (share // HD), (part + 1) * (share // HD))
        def _(h):
            lanes = pl.ds(pl.multiple_of(h * HD, HD), HD)
            for start in range(0, cols, width):
                at = (slice(None), pl.ds(start, width), lanes)
                got = attend(*(ref[at].reshape(size, HD) for ref in cols_in), allowed)
                col_out[at] = got.reshape(n, width, HD)

        @pl.loop(1, n)
        def _(d):
            back_copy(part, lax.rem(me + d, n)).start()

        @pl.when(stays)
        def _():
            rows = pl.ds(pl.multiple_of(slot_here * cols, cols), cols)
            joined[head, rows, pl.ds(block + part * share, share)] = col_out[
                me, :, pl.ds(part * share, share)
            ]

        @pl.when(jnp.logical_not(stays))
        def _():
            back_copy(part, me).start()

        if part == 0:
            onward(SHARES // 2, SHARES)

    @pl.loop(0, SHARES)
    def _(s):
        index = index_of(member_beside, s)
        w_copy(w_other, index, 1, beside, head).wait_recv()
        w_copy(w_other, index, 3, sibling, head).start()

    row_copy.wait_recv()

    def back_wait(source_head):
        @pl.loop(0, n // 2)
        def _(slot):
            mine = (head * (n // 2) + slot == me) & (head == source_head)

            @pl.when(jnp.logical_not(mine))
            def _():
                for part in range(PARTS):
                    back_arrival(source_head, part, slot).wait_recv()

    back_wait(head)

    def own_col_part(lanes):
        summed[:, lanes] += jnp.dot(
            joined[head, :, pl.ds(block, block)],
            w_own[pl.ds(block, block), lanes],
            preferred_element_type=jnp.float32,
        )

    tiles(own_col_part)

    @pl.loop(0, SHARES)
    def _(s):
        w_copy(w_other, index_of(member_sibling, s), 2, sibling, head).wait_recv()
        w_copy(w_other, index_of(member_far, s), 3, sibling, head).wait_recv()

    back_wait(other)

    def other_part(lanes):
        total = summed[:, lanes] + jnp.dot(
            joined[other], w_other[:, lanes], preferred_element_type=jnp.float32
        )
        out_ref[:, lanes] = total.astype(jnp.bfloat16)

    tiles(other_part)

    for part in range(PARTS):

        @pl.loop(1, n)
        def _(d):
            for t in range(3):
                col_copy(t, part, d).wait_send()

    @pl.loop(0, SHARES)
    def _(s):
        w_copy(w_hbm, index_of(member, s), 0, me, other).wait_send()
        w_copy(w_other, index_of(member, s), 2, sibling, head).wait_send()
        w_copy(w_other, index_of(member_beside, s), 3, sibling, head).wait_send()

    @pl.loop(0, SHARES - STRAIGHT)
    def _(s):
        w_copy(w_other, index_of(member, s), 1, beside, head).wait_send()

    @pl.loop(SHARES - STRAIGHT, SHARES)
    def _(s):
        w_copy(w_hbm, index_of(member_beside, s), 0, me, other).wait_send()

    row_copy.wait_send()

    for part in range(PARTS):

        @pl.loop(1, n)
        def _(d):
            back_copy(part, lax.rem(me + d, n)).wait_send()

        @pl.when(jnp.logical_not(stays))
        def _():
            back_copy(part, me).wait_send()


def on_device(n, queries, keys, values, w_out):
    _, stride, local_feat = queries.shape
    depth, model_width = w_out.shape
    block = GROUP * HD
    assert queries.shape[0] == 1 and local_feat == 2 * block
    half = stride // lax.axis_size("head")
    cols = stride // n
    if n == LAYER * LAYER and stride % (LAYER * CHUNKS * WIDTH) == 0:
        out = call_layered(n, queries, keys, values, w_out, half)
        return out.reshape((1, half, model_width))
    bf16 = jnp.bfloat16
    dma = pltpu.SemaphoreType.DMA
    out = pl.pallas_call(
        functools.partial(body, n),
        out_shape=jax.ShapeDtypeStruct((half, model_width), bf16),
        in_specs=[pl.BlockSpec(memory_space=pltpu.HBM)] * 4,
        out_specs=pl.BlockSpec(memory_space=pltpu.VMEM),
        scratch_shapes=[pltpu.VMEM((stride, block), bf16)] * 3
        + [pltpu.VMEM((n, cols, block), bf16)] * 4
        + [
            pltpu.VMEM((stride, block), bf16),
            pltpu.VMEM((2, half, local_feat), bf16),
            pltpu.VMEM((half, model_width), jnp.float32),
            pltpu.VMEM((depth, model_width), bf16),
            pltpu.VMEM((depth, model_width), bf16),
            dma((7,)),
            dma((3 * PARTS, n)),
            dma((3 * PARTS, n)),
            dma((PARTS, n)),
            dma((2 * PARTS, n // 2)),
            dma((4, 4 * SHARES)),
            dma((4 * SHARES,)),
            dma,
            dma,
        ],
        compiler_params=pltpu.CompilerParams(has_side_effects=True, vmem_limit_bytes=60 * 2**20),
    )(queries, keys, values, w_out)
    return out.reshape((1, half, model_width))


def solution(mesh):
    return jax.shard_map(
        functools.partial(on_device, mesh.shape["ctx"]),
        mesh=mesh,
        in_specs=(
            P("ctx", None, "head"),
            P("ctx", None, "head"),
            P("ctx", None, "head"),
            P("head", None),
        ),
        out_specs=P("ctx", "head", None),
        check_vma=False,
    )
```

```python
import functools

import jax
import jax.numpy as jnp
from jax import lax
from jax.experimental import pallas as pl
from jax.experimental.pallas import tpu as pltpu
from jax.sharding import PartitionSpec as P

HD = 128
GROUP = 4
MESH = pl.DeviceIdType.MESH
SHARES = 8
STRAIGHT = 2
PARTS = 2
LAYER = 4
CHUNKS = 8
WIDTH = 16
WIDTH_LOG = 4
PIECES = 4
AHEAD = 3

masked_score = -1e30


def attend(query, key, value, allowed):
    scores = lax.dot_general(
        query, key, (((1,), (1,)), ((), ())), preferred_element_type=jnp.float32
    ) * jnp.float32(1.0 / HD**0.5)
    scores = jnp.where(allowed, scores, masked_score)
    top = jnp.max(scores, axis=-1, keepdims=True)
    expo = jnp.exp(scores - top)
    total = jnp.sum(expo, axis=-1, keepdims=True)
    mixed = jnp.dot(expo.astype(jnp.bfloat16), value, preferred_element_type=jnp.float32)
    return (mixed / total).astype(jnp.bfloat16)


def weigh(queries, keys, values, allowed):
    scores = [
        lax.dot_general(q, k, (((1,), (1,)), ((), ())), preferred_element_type=jnp.float32)
        for q, k in zip(queries, keys)
    ]
    scores = [jnp.where(allowed, s * jnp.float32(1.0 / HD**0.5), masked_score) for s in scores]
    tops = [jnp.max(s, axis=-1, keepdims=True) for s in scores]
    expos = [jnp.exp(s - top) for s, top in zip(scores, tops)]
    totals = [jnp.sum(e, axis=-1, keepdims=True) for e in expos]
    mixed = [
        jnp.dot(e.astype(jnp.bfloat16), v, preferred_element_type=jnp.float32)
        for e, v in zip(expos, values)
    ]
    return [
        ((m / total).astype(jnp.bfloat16), top + jnp.log(total))
        for m, total, top in zip(mixed, totals, tops)
    ]


def layered(
    n, q_hbm, k_hbm, v_hbm, w_hbm, out_hbm, q_row, k_row, v_row, q_in, k_in, v_in, o_out, p_in,
    stats, stats_in, row_out, joined, summed, w_own, w_other, staged,
    local_sem, chunk_sem, lay_send, lay_recv, up_send, up_recv, part_send, part_recv,
    back_send, back_recv, w_send, w_recv, row_send, row_recv, out_sem,
):
    me, head = lax.axis_index("ctx"), lax.axis_index("head")
    other = 1 - head
    z, s = lax.div(me, LAYER), lax.rem(me, LAYER)
    core = lax.rem(s, 2)
    sib = s + 1 - 2 * core
    opp = s + 2 - 4 * lax.div(s, 2)
    far = sib + 2 - 4 * lax.div(sib, 2)
    peers = (s, sib, opp, far)
    stride = q_hbm.shape[1]
    block = q_row.shape[1]
    depth = w_own.shape[0]
    half = joined.shape[1]
    cols = stride // LAYER
    cw = cols // CHUNKS
    hbm = (q_hbm, k_hbm, v_hbm)
    ins = (q_in, k_in, v_in)
    own_at = (0, LAYER, LAYER)
    feats = pl.ds(block, block)

    def place(j, slot):
        return slot * (cols // 2) + lax.div(j, 2) * cw

    def chunk_of(j, slot):
        return pl.ds(pl.multiple_of(lax.rem(j, 2) * half + place(j, slot), cw), cw)

    def remote(src, dst, send, recv, ctx, at):
        return pltpu.make_async_remote_copy(
            src_ref=src, dst_ref=dst, send_sem=send, recv_sem=recv,
            device_id=(ctx, at), device_id_type=MESH,
        )

    def here(slot):
        return z * LAYER + slot

    def lay(t, j, d, source):
        row = peers[d] if source else s
        return remote(
            hbm[t].at[0, chunk_of(j, peers[d]), feats],
            ins[t].at[own_at[t] + row, pl.ds(j * cw, cw)],
            lay_send.at[t * CHUNKS + j, d], lay_recv.at[t * CHUNKS + j, d],
            here(peers[d]), head,
        )

    def up(kind, t, j, d, layer, base):
        if d < 2:
            src, slot, row = hbm[t].at[0, chunk_of(j, peers[d]), feats], peers[d], s
        else:
            src, slot, row = ins[t].at[own_at[t] + peers[d], pl.ds(j * cw, cw)], s, peers[d]
        return remote(
            src, ins[t].at[base + row, pl.ds(j * cw, cw)],
            up_send.at[kind * CHUNKS + j, d], up_recv.at[kind * CHUNKS + j, d],
            layer * LAYER + slot, head,
        )

    def up_arrival(kind, t, j, d, base):
        return remote(
            hbm[t].at[0, pl.ds(0, cw), feats], ins[t].at[base + peers[d], pl.ds(j * cw, cw)],
            up_send.at[kind * CHUNKS + j, d], up_recv.at[kind * CHUNKS + j, d],
            here(sib), head,
        )

    routes = {
        0: ((0, 1, 1, 0), (1, 2, 1, 0)),
        2: ((2, 0, 1, LAYER),),
        3: ((2, 0, 2, LAYER),),
    }

    def onward(j):
        at = pl.ds(j * cw, cw)
        return remote(
            q_in.at[pl.ds(LAYER, LAYER), at], q_in.at[pl.ds(2 * LAYER, LAYER), at],
            up_send.at[3 * CHUNKS + j, 0], up_recv.at[3 * CHUNKS + j, 0], LAYER + s, head,
        )

    def pass_on(j):
        for d in range(4):
            up_arrival(2, 0, j, d, LAYER).wait_recv()
        onward(j).start()

    def direct(layer, j):
        for kind, t, to, base in routes[layer]:
            for d in (0, 1):
                up(kind, t, j, d, to, base).start()

    def relay(layer, j):
        for t in sorted({t for _, t, _, _ in routes[layer]}):
            for d in (2, 3):
                lay(t, j, d, True).wait_recv()
                for kind, t2, to, base in routes[layer]:
                    if t2 == t:
                        up(kind, t, j, d, to, base).start()

    def piece_rows(q, c, k):
        eighth = depth // 16
        rows = eighth // (PIECES // 2)
        start = lax.div(k, PIECES // 2) * (depth // 2)
        start += (q * 2 + c) * eighth + lax.rem(k, PIECES // 2) * rows
        return pl.ds(start, rows)

    def w_copy(source, q, c, k, way, to_ctx, to_head):
        rows = piece_rows(q, c, k)
        index = (q * 2 + c) * PIECES + k
        return remote(
            source.at[rows], w_other.at[rows], w_send.at[way, index], w_recv.at[index], to_ctx, to_head
        )

    even = lax.rem(z + lax.div(s, 2), 2)
    y_next = here(opp)
    z_next = me + LAYER - 2 * LAYER * lax.rem(z, 2)
    z_early = (z == 1) | (z == 2)

    def w_first(q, k):
        return w_copy(w_hbm, 2 * even + q, core, k, 0, me, other)

    def w_side(q, k):
        return w_copy(w_other, 2 * even + q, core, k, 2, y_next if q == 0 else z_next, head)

    def w_beside(q, k):
        return w_copy(w_other, 2 * (1 - even) + q, core, k, 1, here(sib), head)

    def w_here(q, k):
        return w_copy(w_other, 2 * even + q, core, k, 1, here(sib), head)

    def w_in(q, k):
        w_first(q, k).wait_recv()
        w_here(q, k).start()
        if q == 0:
            w_side(q, k).start()
        else:

            @pl.when(z_early | (k > 0))
            def _():
                w_side(q, k).start()

    def w_on(q, k):
        w_copy(w_other, 2 * (1 - even) + q, core, k, 2, me, other).wait_recv()
        w_beside(q, k).start()

    def exchange(ts):
        @pl.loop(0, CHUNKS)
        def _(j):
            for t in ts:
                for d in (2, 3, 1):
                    lay(t, j, d, False).start()

    for layer in routes:

        @pl.when(z == layer)
        def _():
            for j in range(AHEAD):
                direct(layer, j)

    @pl.when(z < 2)
    def _():
        exchange((1, 2))
        exchange((0,))

    @pl.when(z >= 2)
    def _():
        exchange((0,))
        exchange((1, 2))

    @pl.loop(0, PIECES)
    def _(k):
        w_first(0, k).start()
        w_first(1, k).start()

    local = [
        pltpu.make_async_copy(hbm[t].at[0, :, pl.ds(0, block)], (q_row, k_row, v_row)[t], local_sem.at[t])
        for t in range(3)
    ]
    local += [
        pltpu.make_async_copy(
            hbm[t].at[0, chunk_of(j, s), feats],
            ins[t].at[own_at[t] + s, pl.ds(j * cw, cw)],
            chunk_sem.at[t, j],
        )
        for t in range(3)
        for j in range(CHUNKS)
    ]
    local.append(pltpu.make_async_copy(w_hbm, w_own, local_sem.at[3]))
    for copy in local:
        copy.start()
    for copy in local[:-1]:
        copy.wait()

    tile = min(256, half)
    row_index = lax.broadcasted_iota(jnp.int32, (tile, stride), 0)
    key_index = lax.broadcasted_iota(jnp.int32, (tile, stride), 1)

    def row_tile(h, start):
        lanes = pl.ds(pl.multiple_of(h * HD, HD), HD)
        end = start + tile
        row_out[pl.ds(start, tile), lanes] = attend(
            q_row[pl.ds(start, tile), lanes],
            k_row[pl.ds(0, end), lanes],
            v_row[pl.ds(0, end), lanes],
            key_index[:, :end] <= row_index[:, :end] + start,
        )

    def spread(sums):
        lane = lax.broadcasted_iota(jnp.int32, (HD, HD), 1)
        row = lax.broadcasted_iota(jnp.int32, (HD, HD), 0)
        return jnp.sum(jnp.where(lane == row, sums, 0.0), axis=0, keepdims=True)

    def laid(sums, off):
        lane = lax.broadcasted_iota(jnp.int32, (size, HD), 1)
        row = lax.broadcasted_iota(jnp.int32, (size, HD), 0)
        return jnp.sum(jnp.where(lane == row + off, sums, 0.0), axis=0, keepdims=True)

    def column(line, off, period):
        lane = lax.broadcasted_iota(jnp.int32, (size, HD), 1)
        row = lax.broadcasted_iota(jnp.int32, (size, HD), 0)
        at = off + (row & (WIDTH - 1)) + lax.shift_right_logical(row, WIDTH_LOG) * period
        return jnp.sum(jnp.where(lane == at, line, 0.0), axis=1, keepdims=True)

    heads = block // HD
    size = LAYER * WIDTH

    def small(q_at, q_rows, k_at, k_rows, c, b, width, causal, keep):
        start = pl.multiple_of(c * cw + b * width, width)
        shape = (q_rows * width, k_rows * width)
        r = lax.broadcasted_iota(jnp.int32, shape, 0)
        m = lax.broadcasted_iota(jnp.int32, shape, 1)
        allowed = ((r - m) & (width - 1)) == 0
        if causal is not None:
            allowed &= m <= r + causal * width
        slices = []
        for h in range(heads):
            lanes = pl.ds(h * HD, HD)
            slices.append(
                (
                    (pl.ds(q_at, q_rows), pl.ds(start, width), lanes),
                    (pl.ds(k_at, k_rows), pl.ds(start, width), lanes),
                )
            )
        found = weigh(
            [q_in[at].reshape(shape[0], HD) for at, _ in slices],
            [k_in[at].reshape(shape[1], HD) for _, at in slices],
            [v_in[at].reshape(shape[1], HD) for _, at in slices],
            allowed,
        )
        for h, (got, sums) in enumerate(found):
            o_out[slices[h][0]] = got.reshape(q_rows, width, HD)
            if keep:
                stats[c * strips + b, pl.ds(h, 1)] = spread(sums)

    strips = cw // WIDTH

    def partial(j, rows, layer):
        return remote(
            o_out.at[pl.ds(LAYER, rows), pl.ds(j * cw, cw)], p_in.at[pl.ds(0, rows), pl.ds(j * cw, cw)],
            part_send.at[0, j], part_recv.at[0, j], layer * LAYER + s, head,
        )

    def partial_stats(j, layer):
        at = pl.ds(j * strips, strips)
        return remote(
            stats.at[at], stats_in.at[at], part_send.at[1, j], part_recv.at[1, j], layer * LAYER + s, head
        )

    def back(j, d):
        return remote(
            o_out.at[peers[d], pl.ds(j * cw, cw)],
            joined.at[head, pl.ds(place(j, s), cw), feats],
            back_send.at[j, d], back_recv.at[head * LAYER + s, lax.div(j, 2)],
            here(peers[d]), lax.rem(j, 2),
        )

    def stays(j):
        return lax.rem(j, 2) == head

    def back_all(j):
        for d in (2, 3, 1):
            back(j, d).start()

        @pl.when(jnp.logical_not(stays(j)))
        def _():
            back(j, 0).start()

        @pl.when(stays(j))
        def _():
            joined[head, pl.ds(pl.multiple_of(place(j, s), cw), cw), feats] = o_out[
                s, pl.ds(pl.multiple_of(j * cw, cw), cw)
            ]

    def ext(j):
        for t in (1, 2):
            for d in (1, 2, 3):
                lay(t, j, d, True).wait_recv()
        for kind, t, base in ((0, 1, 0), (1, 2, 0), (2, 0, LAYER)):
            for d in range(4):
                up_arrival(kind, t, j, d, base).wait_recv()
        onward(j).wait_recv()
        for b in range(strips):
            small(LAYER, 2 * LAYER, 0, 2 * LAYER, j, b, WIDTH, None, True)
        partial(j, 2 * LAYER, 2).start()
        partial_stats(j, 2).start()

    def own(c):
        @pl.when(z == 0)
        def _():
            for t, ds in ((0, (1, 2, 3)), (1, (1,)), (2, (1,))):
                for d in ds:
                    lay(t, c, d, True).wait_recv()
            small(0, LAYER, LAYER, LAYER, c, 0, cw, 0, False)
            back_all(c)

        @pl.when(z == 1)
        def _():
            for d in (1, 2, 3):
                lay(0, c, d, True).wait_recv()
            small(0, LAYER, 0, 2 * LAYER, c, 0, cw, LAYER, False)
            back_all(c)

        @pl.when(z >= 2)
        def _():
            lay(0, c, 1, True).wait_recv()
            for t in (1, 2):
                for d in (1, 2, 3):
                    lay(t, c, d, True).wait_recv()

        @pl.when(z == 2)
        def _():
            for b in range(strips):
                small(0, 2 * LAYER, LAYER, LAYER, c, b, WIDTH, 0, True)

        @pl.when(z == 3)
        def _():
            small(0, LAYER, LAYER, LAYER, c, 0, cw, 0, True)

    def combine(c):
        def mix(b, base, parts, keep):
            start = pl.multiple_of(c * cw + b * WIDTH, WIDTH)
            rows = pl.ds(start, WIDTH)
            strip = c * strips + b
            for h in range(heads):
                lanes = pl.ds(h * HD, HD)
                lines = [column(ref[at, pl.ds(row + h, 1)], off, period) for _, _, ref, at, row, off, period in parts]
                top = functools.reduce(jnp.maximum, lines)
                terms = [jnp.exp(line - top) for line in lines]
                total = functools.reduce(jnp.add, terms)
                got = 0.0
                for (source, first, *_), term in zip(parts, terms):
                    value = source[pl.ds(first, LAYER), rows, lanes].reshape(size, HD)
                    got += value.astype(jnp.float32) * (term / total)
                o_out[pl.ds(base, LAYER), rows, lanes] = got.astype(jnp.bfloat16).reshape(LAYER, WIDTH, HD)
                if keep:
                    stats[strip, pl.ds(heads + h, 1)] = laid(top + jnp.log(total), size)

        @pl.when(z == 2)
        def _():
            partial(c, 2 * LAYER, 2).wait_recv()
            partial_stats(c, 2).wait_recv()
            for first in (LAYER, 0):
                off = size if first else 0
                for b in range(strips):
                    strip = c * strips + b
                    mix(
                        b,
                        first,
                        [
                            (o_out, first, stats, strip, 0, off, WIDTH),
                            (p_in, first, stats_in, strip, 0, off, WIDTH),
                        ],
                        first > 0,
                    )
                if first:
                    partial(c, LAYER, 3).start()
                    partial_stats(c, 3).start()

        @pl.when(z == 3)
        def _():
            partial(c, LAYER, 3).wait_recv()
            partial_stats(c, 3).wait_recv()
            for b in range(strips):
                strip = c * strips + b
                mix(
                    b,
                    0,
                    [
                        (o_out, 0, stats, c * strips, 0, b * WIDTH, cw),
                        (p_in, 0, stats_in, strip, heads, size, WIDTH),
                    ],
                    False,
                )

        back_all(c)

    row_copy = remote(
        row_out.at[pl.ds(pl.multiple_of(other * half, half), half)],
        joined.at[head, :, pl.ds(0, block)], row_send, row_recv, me, other,
    )
    step = 512
    count = staged.shape[1] // step

    def tiles(add):
        @pl.loop(0, count)
        def _(c):
            add(pl.ds(pl.multiple_of(c * step, step), step))

    def own_row_part(lanes):
        summed[:, lanes] = jnp.dot(
            joined[head, :, pl.ds(0, block)],
            w_own[pl.ds(0, block), lanes],
            preferred_element_type=jnp.float32,
        )

    @pl.loop(0, CHUNKS)
    def _(j):
        @pl.when(j < 2)
        def _():
            @pl.loop(j * (heads // 2), (j + 1) * (heads // 2))
            def _(h):
                for start in range(0, stride, tile):
                    row_tile(h, start)

        @pl.when(j == 1)
        def _():
            row_copy.start()
            joined[head, :, pl.ds(0, block)] = row_out[pl.ds(pl.multiple_of(head * half, half), half)]

        for layer in routes:

            @pl.when((z == layer) & (j < CHUNKS // 2))
            def _():
                @pl.loop(2 * j, 2 * j + 2)
                def _(c):
                    relay(layer, c)
                    if layer == 2:
                        pass_on(c)

                    @pl.when(c + AHEAD < CHUNKS)
                    def _():
                        direct(layer, c + AHEAD)

        @pl.when(z == 1)
        def _():
            ext(j)

        @pl.when(j == 2)
        def _():
            local[-1].wait()
            tiles(own_row_part)

        @pl.when(jnp.logical_not(z_early) & (j == CHUNKS // 2))
        def _():
            w_side(1, 0).start()

        @pl.when((j > 0) & (lax.rem(j, 2) == 1))
        def _():
            w_in(0, lax.div(j, 2))

        @pl.when((j > 0) & (lax.rem(j, 2) == 0))
        def _():
            w_in(1, lax.div(j, 2) - 1)

        @pl.when(j >= CHUNKS // 2)
        def _():
            c = 2 * j - CHUNKS
            own(c)
            own(c + 1)

            @pl.when((z >= 2) & (j > CHUNKS // 2))
            def _():
                combine(j - CHUNKS // 2 - 1)

    w_in(1, PIECES - 1)

    @pl.when(z >= 2)
    def _():
        @pl.loop(CHUNKS // 2 - 1, CHUNKS - 2)
        def _(c):
            combine(c)

    @pl.loop(0, PIECES)
    def _(k):
        w_on(0, k)

    @pl.when(z >= 2)
    def _():
        @pl.loop(CHUNKS - 2, CHUNKS)
        def _(c):
            combine(c)

    @pl.loop(0, PIECES // 2)
    def _(k):
        w_on(1, k)

    def w_from_sibling(qs, first, last):
        @pl.loop(first, last)
        def _(k):
            for q in qs:
                w_copy(w_other, q, 1 - core, k, 1, here(sib), head).wait_recv()

    w_from_sibling((0, 1, 2, 3), 0, PIECES // 2)
    row_copy.wait_recv()

    def other_row_part(lanes):
        summed[:, lanes] += jnp.dot(
            joined[other, :, pl.ds(0, block)],
            w_other[pl.ds(0, block), lanes],
            preferred_element_type=jnp.float32,
        )

    tiles(other_row_part)

    def back_wait(source_head):
        for slot in range(LAYER):

            @pl.when(jnp.logical_not((slot == s) & (head == source_head)))
            def _():
                @pl.loop(0, CHUNKS // 2)
                def _(i):
                    remote(
                        o_out.at[0, pl.ds(i * cw, cw)],
                        joined.at[source_head, pl.ds(place(2 * i, slot), cw), feats],
                        back_send.at[i, 0], back_recv.at[source_head * LAYER + slot, i],
                        me, other,
                    ).wait_recv()

    back_wait(head)
    back_wait(other)
    w_from_sibling((2 * even, 2 * even + 1), PIECES // 2, PIECES)
    quarter = block // 2
    early = pl.ds(pl.multiple_of(block + even * quarter, quarter), quarter)
    late = pl.ds(pl.multiple_of(block + (1 - even) * quarter, quarter), quarter)

    def col_part(lanes):
        total = summed[:, lanes] + jnp.dot(
            joined[head, :, feats], w_own[feats, lanes], preferred_element_type=jnp.float32
        )
        summed[:, lanes] = total + jnp.dot(
            joined[other, :, early], w_other[early, lanes], preferred_element_type=jnp.float32
        )

    tiles(col_part)

    @pl.loop(PIECES // 2, PIECES)
    def _(k):
        w_on(1, k)

    w_from_sibling((2 - 2 * even, 3 - 2 * even), PIECES // 2, PIECES)

    def leave(c):
        lanes = pl.ds(pl.multiple_of(c * step, step), step)
        return pltpu.make_async_copy(staged.at[:, lanes], out_hbm.at[:, lanes], out_sem.at[c])

    @pl.loop(0, count)
    def _(c):
        lanes = pl.ds(pl.multiple_of(c * step, step), step)
        total = summed[:, lanes] + jnp.dot(
            joined[other, :, late], w_other[late, lanes], preferred_element_type=jnp.float32
        )
        staged[:, lanes] = total.astype(jnp.bfloat16)
        leave(c).start()

    @pl.loop(0, CHUNKS)
    def _(j):
        for t in range(3):
            for d in (1, 2, 3):
                lay(t, j, d, False).wait_send()
        for layer in routes:

            @pl.when(z == layer)
            def _():
                for kind, t, to, base in routes[layer]:
                    for d in range(4):
                        up(kind, t, j, d, to, base).wait_send()

        @pl.when(z == 1)
        def _():
            partial(j, 2 * LAYER, 2).wait_send()
            partial_stats(j, 2).wait_send()

        @pl.when(z == 2)
        def _():
            onward(j).wait_send()
            partial(j, LAYER, 3).wait_send()
            partial_stats(j, 3).wait_send()

        for d in (1, 2, 3):
            back(j, d).wait_send()

        @pl.when(jnp.logical_not(stays(j)))
        def _():
            back(j, 0).wait_send()

    @pl.loop(0, PIECES)
    def _(k):
        for q in (0, 1):
            w_first(q, k).wait_send()
            w_here(q, k).wait_send()
            w_side(q, k).wait_send()
            w_beside(q, k).wait_send()

    row_copy.wait_send()

    @pl.loop(0, count)
    def _(c):
        leave(c).wait()


def call_layered(n, queries, keys, values, w_out, half):
    _, stride, local_feat = queries.shape
    depth, width = w_out.shape
    block = local_feat // 2
    cols = stride // LAYER
    bf16, f32 = jnp.bfloat16, jnp.float32
    dma = pltpu.SemaphoreType.DMA
    blocks = cols // WIDTH
    return pl.pallas_call(
        functools.partial(layered, n),
        out_shape=jax.ShapeDtypeStruct((half, width), bf16),
        in_specs=[pl.BlockSpec(memory_space=pltpu.HBM)] * 4,
        out_specs=pl.BlockSpec(memory_space=pltpu.HBM),
        scratch_shapes=[pltpu.VMEM((stride, block), bf16)] * 3
        + [
            pltpu.VMEM((3 * LAYER, cols, block), bf16),
            pltpu.VMEM((2 * LAYER, cols, block), bf16),
            pltpu.VMEM((2 * LAYER, cols, block), bf16),
            pltpu.VMEM((3 * LAYER, cols, block), bf16),
            pltpu.VMEM((2 * LAYER, cols, block), bf16),
            pltpu.VMEM((blocks, 8, HD), f32),
            pltpu.VMEM((blocks, 8, HD), f32),
            pltpu.VMEM((stride, block), bf16),
            pltpu.VMEM((2, half, local_feat), bf16),
            pltpu.VMEM((half, width), f32),
            pltpu.VMEM((depth, width), bf16),
            pltpu.VMEM((depth, width), bf16),
            pltpu.VMEM((half, width), bf16),
            dma((4,)),
            dma((3, CHUNKS)),
            dma((3 * CHUNKS, LAYER)),
            dma((3 * CHUNKS, LAYER)),
            dma((4 * CHUNKS, LAYER)),
            dma((4 * CHUNKS, LAYER)),
            dma((2, CHUNKS)),
            dma((2, CHUNKS)),
            dma((CHUNKS, LAYER)),
            dma((2 * LAYER, CHUNKS // 2)),
            dma((3, 8 * PIECES)),
            dma((8 * PIECES,)),
            dma,
            dma,
            dma((width // 512,)),
        ],
        compiler_params=pltpu.CompilerParams(has_side_effects=True, vmem_limit_bytes=60 * 2**20),
    )(queries, keys, values, w_out)


def body(
    n, q_hbm, k_hbm, v_hbm, w_hbm, out_ref, q_row, k_row, v_row, q_col, k_col, v_col,
    col_out, row_out, joined, summed, w_own, w_other, local_sem, in_send, in_recv, back_send, back_recv,
    w_send, w_recv, row_send, row_recv,
):
    me, head = lax.axis_index("ctx"), lax.axis_index("head")
    other = 1 - head
    stride = q_hbm.shape[1]
    block = q_row.shape[1]
    depth = w_own.shape[0]
    half = joined.shape[1]
    cols = stride // n
    share = block // PARTS
    hbm = (q_hbm, k_hbm, v_hbm)
    rows_in = (q_row, k_row, v_row)
    cols_in = (q_col, k_col, v_col)
    back_head = lax.div(me * cols, half)
    member = lax.rem(me, 4)
    sibling = me + 1 - 2 * lax.rem(me, 2)
    beside = me + 2 - 4 * lax.div(member, 2)
    piece = depth // (4 * SHARES)

    def col_copy(t, part, d):
        peer = lax.rem(me + d, n)
        lanes = pl.ds(part * share, share)
        return pltpu.make_async_remote_copy(
            src_ref=hbm[t].at[0, pl.ds(peer * cols, cols), pl.ds(block + part * share, share)],
            dst_ref=cols_in[t].at[me, :, lanes],
            send_sem=in_send.at[t * PARTS + part, d],
            recv_sem=in_recv.at[t * PARTS + part, d],
            device_id=(peer, head),
            device_id_type=MESH,
        )

    def col_arrival(t, part, d):
        source = lax.rem(me + n - d, n)
        lanes = pl.ds(part * share, share)
        return pltpu.make_async_remote_copy(
            src_ref=hbm[t].at[0, pl.ds(0, cols), pl.ds(block + part * share, share)],
            dst_ref=cols_in[t].at[source, :, lanes],
            send_sem=in_send.at[t * PARTS + part, d],
            recv_sem=in_recv.at[t * PARTS + part, d],
            device_id=(source, head),
            device_id_type=MESH,
        )

    def w_copy(source, index, way, to_ctx, to_head):
        rows = pl.ds(index * piece, piece)
        return pltpu.make_async_remote_copy(
            src_ref=source.at[rows],
            dst_ref=w_other.at[rows],
            send_sem=w_send.at[way, index],
            recv_sem=w_recv.at[index],
            device_id=(to_ctx, to_head),
            device_id_type=MESH,
        )

    def index_of(who, s):
        return who * SHARES + s

    member_sibling = lax.rem(sibling, 4)
    member_beside = lax.rem(beside, 4)
    member_far = lax.rem(member + 2, 4) + 1 - 2 * lax.rem(member, 2)

    for part in range(PARTS):

        @pl.loop(1, n)
        def _(d):
            for t in range(3):
                col_copy(t, part, d).start()

    @pl.loop(0, SHARES)
    def _(s):
        w_copy(w_hbm, index_of(member, s), 0, me, other).start()

    @pl.loop(SHARES - STRAIGHT, SHARES)
    def _(s):
        w_copy(w_hbm, index_of(member_beside, s), 0, me, other).start()

    local = [
        pltpu.make_async_copy(hbm[t].at[0, :, pl.ds(0, block)], rows_in[t], local_sem.at[t])
        for t in range(3)
    ]
    local += [
        pltpu.make_async_copy(
            hbm[t].at[0, pl.ds(me * cols, cols), pl.ds(block, block)],
            cols_in[t].at[me],
            local_sem.at[3 + t],
        )
        for t in range(3)
    ]
    local.append(pltpu.make_async_copy(w_hbm, w_own, local_sem.at[3]))
    for copy in local:
        copy.start()
    for copy in local[:3]:
        copy.wait()

    tile = min(256, half)
    row_index = lax.broadcasted_iota(jnp.int32, (tile, stride), 0)
    key_index = lax.broadcasted_iota(jnp.int32, (tile, stride), 1)

    @pl.loop(0, block // HD)
    def _(h):
        lanes = pl.ds(pl.multiple_of(h * HD, HD), HD)
        for start in range(0, stride, tile):
            end = start + tile
            row_out[pl.ds(start, tile), lanes] = attend(
                q_row[pl.ds(start, tile), lanes],
                k_row[pl.ds(0, end), lanes],
                v_row[pl.ds(0, end), lanes],
                key_index[:, :end] <= row_index[:, :end] + start,
            )

    row_copy = pltpu.make_async_remote_copy(
        src_ref=row_out.at[pl.ds(pl.multiple_of(other * half, half), half)],
        dst_ref=joined.at[head, :, pl.ds(0, block)],
        send_sem=row_send,
        recv_sem=row_recv,
        device_id=(me, other),
        device_id_type=MESH,
    )
    row_copy.start()
    joined[head, :, pl.ds(0, block)] = row_out[pl.ds(pl.multiple_of(head * half, half), half)]

    def onward(first, last):
        @pl.loop(first, last)
        def _(s):
            index = index_of(member, s)
            w_copy(w_hbm, index, 0, me, other).wait_recv()

            @pl.when(s < SHARES - STRAIGHT)
            def _():
                w_copy(w_other, index, 1, beside, head).start()

            w_copy(w_other, index, 2, sibling, head).start()

    onward(0, SHARES // 2)

    for copy in local[3:]:
        copy.wait()

    step = 512

    def tiles(add):
        @pl.loop(0, out_ref.shape[1] // step)
        def _(c):
            add(pl.ds(pl.multiple_of(c * step, step), step))

    def own_row_part(lanes):
        summed[:, lanes] = jnp.dot(
            joined[head, :, pl.ds(0, block)],
            w_own[pl.ds(0, block), lanes],
            preferred_element_type=jnp.float32,
        )

    tiles(own_row_part)
    width = min(cols, max(16, 256 // n))
    size = n * width
    r_index = lax.broadcasted_iota(jnp.int32, (size, size), 0)
    s_index = lax.broadcasted_iota(jnp.int32, (size, size), 1)
    allowed = (s_index <= r_index) & (((r_index - s_index) & (width - 1)) == 0)

    slot_here = lax.rem(me, n // 2)
    stays = back_head == head

    def landing(source_head, part, slot):
        return joined.at[
            source_head,
            pl.ds(pl.multiple_of(slot * cols, cols), cols),
            pl.ds(block + part * share, share),
        ]

    def back_copy(part, r):
        return pltpu.make_async_remote_copy(
            src_ref=col_out.at[r, :, pl.ds(part * share, share)],
            dst_ref=landing(head, part, slot_here),
            send_sem=back_send.at[part, r],
            recv_sem=back_recv.at[head * PARTS + part, slot_here],
            device_id=(r, back_head),
            device_id_type=MESH,
        )

    def back_arrival(source_head, part, slot):
        return pltpu.make_async_remote_copy(
            src_ref=col_out.at[0, :, pl.ds(part * share, share)],
            dst_ref=landing(source_head, part, slot),
            send_sem=back_send.at[part, 0],
            recv_sem=back_recv.at[source_head * PARTS + part, slot],
            device_id=(me, other),
            device_id_type=MESH,
        )

    for part in range(PARTS):

        @pl.loop(1, n)
        def _(d):
            for t in range(3):
                col_arrival(t, part, d).wait_recv()

        @pl.loop(part * (share // HD), (part + 1) * (share // HD))
        def _(h):
            lanes = pl.ds(pl.multiple_of(h * HD, HD), HD)
            for start in range(0, cols, width):
                at = (slice(None), pl.ds(start, width), lanes)
                got = attend(*(ref[at].reshape(size, HD) for ref in cols_in), allowed)
                col_out[at] = got.reshape(n, width, HD)

        @pl.loop(1, n)
        def _(d):
            back_copy(part, lax.rem(me + d, n)).start()

        @pl.when(stays)
        def _():
            rows = pl.ds(pl.multiple_of(slot_here * cols, cols), cols)
            joined[head, rows, pl.ds(block + part * share, share)] = col_out[
                me, :, pl.ds(part * share, share)
            ]

        @pl.when(jnp.logical_not(stays))
        def _():
            back_copy(part, me).start()

        if part == 0:
            onward(SHARES // 2, SHARES)

    @pl.loop(0, SHARES)
    def _(s):
        index = index_of(member_beside, s)
        w_copy(w_other, index, 1, beside, head).wait_recv()
        w_copy(w_other, index, 3, sibling, head).start()

    row_copy.wait_recv()

    def back_wait(source_head):
        @pl.loop(0, n // 2)
        def _(slot):
            mine = (head * (n // 2) + slot == me) & (head == source_head)

            @pl.when(jnp.logical_not(mine))
            def _():
                for part in range(PARTS):
                    back_arrival(source_head, part, slot).wait_recv()

    back_wait(head)

    def own_col_part(lanes):
        summed[:, lanes] += jnp.dot(
            joined[head, :, pl.ds(block, block)],
            w_own[pl.ds(block, block), lanes],
            preferred_element_type=jnp.float32,
        )

    tiles(own_col_part)

    @pl.loop(0, SHARES)
    def _(s):
        w_copy(w_other, index_of(member_sibling, s), 2, sibling, head).wait_recv()
        w_copy(w_other, index_of(member_far, s), 3, sibling, head).wait_recv()

    back_wait(other)

    def other_part(lanes):
        total = summed[:, lanes] + jnp.dot(
            joined[other], w_other[:, lanes], preferred_element_type=jnp.float32
        )
        out_ref[:, lanes] = total.astype(jnp.bfloat16)

    tiles(other_part)

    for part in range(PARTS):

        @pl.loop(1, n)
        def _(d):
            for t in range(3):
                col_copy(t, part, d).wait_send()

    @pl.loop(0, SHARES)
    def _(s):
        w_copy(w_hbm, index_of(member, s), 0, me, other).wait_send()
        w_copy(w_other, index_of(member, s), 2, sibling, head).wait_send()
        w_copy(w_other, index_of(member_beside, s), 3, sibling, head).wait_send()

    @pl.loop(0, SHARES - STRAIGHT)
    def _(s):
        w_copy(w_other, index_of(member, s), 1, beside, head).wait_send()

    @pl.loop(SHARES - STRAIGHT, SHARES)
    def _(s):
        w_copy(w_hbm, index_of(member_beside, s), 0, me, other).wait_send()

    row_copy.wait_send()

    for part in range(PARTS):

        @pl.loop(1, n)
        def _(d):
            back_copy(part, lax.rem(me + d, n)).wait_send()

        @pl.when(jnp.logical_not(stays))
        def _():
            back_copy(part, me).wait_send()


def on_device(n, queries, keys, values, w_out):
    _, stride, local_feat = queries.shape
    depth, model_width = w_out.shape
    block = GROUP * HD
    assert queries.shape[0] == 1 and local_feat == 2 * block
    half = stride // lax.axis_size("head")
    cols = stride // n
    if n == LAYER * LAYER and stride % (LAYER * CHUNKS * WIDTH) == 0:
        out = call_layered(n, queries, keys, values, w_out, half)
        return out.reshape((1, half, model_width))
    bf16 = jnp.bfloat16
    dma = pltpu.SemaphoreType.DMA
    out = pl.pallas_call(
        functools.partial(body, n),
        out_shape=jax.ShapeDtypeStruct((half, model_width), bf16),
        in_specs=[pl.BlockSpec(memory_space=pltpu.HBM)] * 4,
        out_specs=pl.BlockSpec(memory_space=pltpu.VMEM),
        scratch_shapes=[pltpu.VMEM((stride, block), bf16)] * 3
        + [pltpu.VMEM((n, cols, block), bf16)] * 4
        + [
            pltpu.VMEM((stride, block), bf16),
            pltpu.VMEM((2, half, local_feat), bf16),
            pltpu.VMEM((half, model_width), jnp.float32),
            pltpu.VMEM((depth, model_width), bf16),
            pltpu.VMEM((depth, model_width), bf16),
            dma((7,)),
            dma((3 * PARTS, n)),
            dma((3 * PARTS, n)),
            dma((PARTS, n)),
            dma((2 * PARTS, n // 2)),
            dma((4, 4 * SHARES)),
            dma((4 * SHARES,)),
            dma,
            dma,
        ],
        compiler_params=pltpu.CompilerParams(has_side_effects=True, vmem_limit_bytes=60 * 2**20),
    )(queries, keys, values, w_out)
    return out.reshape((1, half, model_width))


def solution(mesh):
    return jax.shard_map(
        functools.partial(on_device, mesh.shape["ctx"]),
        mesh=mesh,
        in_specs=(
            P("ctx", None, "head"),
            P("ctx", None, "head"),
            P("ctx", None, "head"),
            P("head", None),
        ),
        out_specs=P("ctx", "head", None),
        check_vma=False,
    )
```

```python
import functools

import jax
import jax.numpy as jnp
from jax import lax
from jax.experimental import pallas as pl
from jax.experimental.pallas import tpu as pltpu
from jax.sharding import PartitionSpec as P

HD = 128
GROUP = 4
MESH = pl.DeviceIdType.MESH
SHARES = 8
STRAIGHT = 2
PARTS = 2
LAYER = 4
CHUNKS = 8
WIDTH = 16
WIDTH_LOG = 4
PIECES = 4
AHEAD = 3

masked_score = -1e30


def attend(query, key, value, allowed):
    scores = lax.dot_general(
        query, key, (((1,), (1,)), ((), ())), preferred_element_type=jnp.float32
    ) * jnp.float32(1.0 / HD**0.5)
    scores = jnp.where(allowed, scores, masked_score)
    top = jnp.max(scores, axis=-1, keepdims=True)
    expo = jnp.exp(scores - top)
    total = jnp.sum(expo, axis=-1, keepdims=True)
    mixed = jnp.dot(expo.astype(jnp.bfloat16), value, preferred_element_type=jnp.float32)
    return (mixed / total).astype(jnp.bfloat16)


def weigh(queries, keys, values, allowed):
    scores = [
        lax.dot_general(q, k, (((1,), (1,)), ((), ())), preferred_element_type=jnp.float32)
        for q, k in zip(queries, keys)
    ]
    scores = [jnp.where(allowed, s * jnp.float32(1.0 / HD**0.5), masked_score) for s in scores]
    tops = [jnp.max(s, axis=-1, keepdims=True) for s in scores]
    expos = [jnp.exp(s - top) for s, top in zip(scores, tops)]
    totals = [jnp.sum(e, axis=-1, keepdims=True) for e in expos]
    mixed = [
        jnp.dot(e.astype(jnp.bfloat16), v, preferred_element_type=jnp.float32)
        for e, v in zip(expos, values)
    ]
    return [
        ((m / total).astype(jnp.bfloat16), top + jnp.log(total))
        for m, total, top in zip(mixed, totals, tops)
    ]


def layered(
    n, q_hbm, k_hbm, v_hbm, w_hbm, out_hbm, q_row, k_row, v_row, q_in, k_in, v_in, o_out, p_in,
    stats, stats_in, row_out, joined, summed, w_own, w_other, staged,
    local_sem, chunk_sem, lay_send, lay_recv, up_send, up_recv, part_send, part_recv,
    back_send, back_recv, w_send, w_recv, row_send, row_recv, out_sem,
):
    me, head = lax.axis_index("ctx"), lax.axis_index("head")
    other = 1 - head
    z, s = lax.div(me, LAYER), lax.rem(me, LAYER)
    core = lax.rem(s, 2)
    sib = s + 1 - 2 * core
    opp = s + 2 - 4 * lax.div(s, 2)
    far = sib + 2 - 4 * lax.div(sib, 2)
    peers = (s, sib, opp, far)
    stride = q_hbm.shape[1]
    block = q_row.shape[1]
    depth = w_own.shape[0]
    half = joined.shape[1]
    cols = stride // LAYER
    cw = cols // CHUNKS
    hbm = (q_hbm, k_hbm, v_hbm)
    ins = (q_in, k_in, v_in)
    own_at = (0, LAYER, LAYER)
    feats = pl.ds(block, block)

    def place(j, slot):
        return slot * (cols // 2) + lax.div(j, 2) * cw

    def chunk_of(j, slot):
        return pl.ds(pl.multiple_of(lax.rem(j, 2) * half + place(j, slot), cw), cw)

    def remote(src, dst, send, recv, ctx, at):
        return pltpu.make_async_remote_copy(
            src_ref=src, dst_ref=dst, send_sem=send, recv_sem=recv,
            device_id=(ctx, at), device_id_type=MESH,
        )

    def here(slot):
        return z * LAYER + slot

    def lay(t, j, d, source):
        row = peers[d] if source else s
        return remote(
            hbm[t].at[0, chunk_of(j, peers[d]), feats],
            ins[t].at[own_at[t] + row, pl.ds(j * cw, cw)],
            lay_send.at[t * CHUNKS + j, d], lay_recv.at[t * CHUNKS + j, d],
            here(peers[d]), head,
        )

    def up(kind, t, j, d, layer, base):
        if d < 2:
            src, slot, row = hbm[t].at[0, chunk_of(j, peers[d]), feats], peers[d], s
        else:
            src, slot, row = ins[t].at[own_at[t] + peers[d], pl.ds(j * cw, cw)], s, peers[d]
        return remote(
            src, ins[t].at[base + row, pl.ds(j * cw, cw)],
            up_send.at[kind * CHUNKS + j, d], up_recv.at[kind * CHUNKS + j, d],
            layer * LAYER + slot, head,
        )

    def up_arrival(kind, t, j, d, base):
        return remote(
            hbm[t].at[0, pl.ds(0, cw), feats], ins[t].at[base + peers[d], pl.ds(j * cw, cw)],
            up_send.at[kind * CHUNKS + j, d], up_recv.at[kind * CHUNKS + j, d],
            here(sib), head,
        )

    routes = {
        0: ((0, 1, 1, 0), (1, 2, 1, 0)),
        2: ((2, 0, 1, LAYER),),
        3: ((2, 0, 2, LAYER),),
    }

    def onward(j):
        at = pl.ds(j * cw, cw)
        return remote(
            q_in.at[pl.ds(LAYER, LAYER), at], q_in.at[pl.ds(2 * LAYER, LAYER), at],
            up_send.at[3 * CHUNKS + j, 0], up_recv.at[3 * CHUNKS + j, 0], LAYER + s, head,
        )

    def pass_on(j):
        for d in range(4):
            up_arrival(2, 0, j, d, LAYER).wait_recv()
        onward(j).start()

    def direct(layer, j):
        for kind, t, to, base in routes[layer]:
            for d in (0, 1):
                up(kind, t, j, d, to, base).start()

    def relay(layer, j):
        for t in sorted({t for _, t, _, _ in routes[layer]}):
            for d in (2, 3):
                lay(t, j, d, True).wait_recv()
                for kind, t2, to, base in routes[layer]:
                    if t2 == t:
                        up(kind, t, j, d, to, base).start()

    def piece_rows(q, c, k):
        eighth = depth // 16
        rows = eighth // (PIECES // 2)
        start = lax.div(k, PIECES // 2) * (depth // 2)
        start += (q * 2 + c) * eighth + lax.rem(k, PIECES // 2) * rows
        return pl.ds(start, rows)

    def w_copy(source, q, c, k, way, to_ctx, to_head):
        rows = piece_rows(q, c, k)
        index = (q * 2 + c) * PIECES + k
        return remote(
            source.at[rows], w_other.at[rows], w_send.at[way, index], w_recv.at[index], to_ctx, to_head
        )

    even = lax.rem(z + lax.div(s, 2), 2)
    y_next = here(opp)
    z_next = me + LAYER - 2 * LAYER * lax.rem(z, 2)
    z_early = (z == 1) | (z == 2)

    def w_first(q, k):
        return w_copy(w_hbm, 2 * even + q, core, k, 0, me, other)

    def w_side(q, k):
        return w_copy(w_other, 2 * even + q, core, k, 2, y_next if q == 0 else z_next, head)

    def w_beside(q, k):
        return w_copy(w_other, 2 * (1 - even) + q, core, k, 1, here(sib), head)

    def w_here(q, k):
        return w_copy(w_other, 2 * even + q, core, k, 1, here(sib), head)

    def w_in(q, k):
        w_first(q, k).wait_recv()
        w_here(q, k).start()
        if q == 0:
            w_side(q, k).start()
        else:

            @pl.when(z_early | (k > 0))
            def _():
                w_side(q, k).start()

    def w_on(q, k):
        w_copy(w_other, 2 * (1 - even) + q, core, k, 2, me, other).wait_recv()
        w_beside(q, k).start()

    ready = pltpu.get_barrier_semaphore()

    def greet(ctx, at):
        pl.semaphore_signal(ready, 1, device_id=(ctx, at), device_id_type=MESH)

    greet(me, other)
    for d in (1, 2, 3):
        greet(here(peers[d]), head)
        greet(here(peers[d]), other)
    for edge, towards in ((0, -LAYER), (LAYER - 1, LAYER)):

        @pl.when(z != edge)
        def _():
            greet(here(s) + towards, head)
            greet(here(sib) + towards, head)

    local = [
        pltpu.make_async_copy(hbm[t].at[0, :, pl.ds(0, block)], (q_row, k_row, v_row)[t], local_sem.at[t])
        for t in range(3)
    ]
    local += [
        pltpu.make_async_copy(
            hbm[t].at[0, chunk_of(j, s), feats],
            ins[t].at[own_at[t] + s, pl.ds(j * cw, cw)],
            chunk_sem.at[t, j],
        )
        for t in range(3)
        for j in range(CHUNKS)
    ]
    local.append(pltpu.make_async_copy(w_hbm, w_own, local_sem.at[3]))
    for copy in local:
        copy.start()

    inner = jnp.minimum(z, 1) + jnp.minimum(LAYER - 1 - z, 1)
    pl.semaphore_wait(ready, 2 * LAYER - 1 + 2 * inner)

    def exchange(ts):
        @pl.loop(0, CHUNKS)
        def _(j):
            for t in ts:
                for d in (2, 3, 1):
                    lay(t, j, d, False).start()

    for layer in routes:

        @pl.when(z == layer)
        def _():
            for j in range(AHEAD):
                direct(layer, j)

    @pl.when(z < 2)
    def _():
        exchange((1, 2))
        exchange((0,))

    @pl.when(z >= 2)
    def _():
        exchange((0,))
        exchange((1, 2))

    @pl.loop(0, PIECES)
    def _(k):
        w_first(0, k).start()
        w_first(1, k).start()

    for copy in local[:-1]:
        copy.wait()

    tile = min(256, half)
    row_index = lax.broadcasted_iota(jnp.int32, (tile, stride), 0)
    key_index = lax.broadcasted_iota(jnp.int32, (tile, stride), 1)

    def row_tile(h, start):
        lanes = pl.ds(pl.multiple_of(h * HD, HD), HD)
        end = start + tile
        row_out[pl.ds(start, tile), lanes] = attend(
            q_row[pl.ds(start, tile), lanes],
            k_row[pl.ds(0, end), lanes],
            v_row[pl.ds(0, end), lanes],
            key_index[:, :end] <= row_index[:, :end] + start,
        )

    def spread(sums):
        lane = lax.broadcasted_iota(jnp.int32, (HD, HD), 1)
        row = lax.broadcasted_iota(jnp.int32, (HD, HD), 0)
        return jnp.sum(jnp.where(lane == row, sums, 0.0), axis=0, keepdims=True)

    def laid(sums, off):
        lane = lax.broadcasted_iota(jnp.int32, (size, HD), 1)
        row = lax.broadcasted_iota(jnp.int32, (size, HD), 0)
        return jnp.sum(jnp.where(lane == row + off, sums, 0.0), axis=0, keepdims=True)

    def column(line, off, period):
        lane = lax.broadcasted_iota(jnp.int32, (size, HD), 1)
        row = lax.broadcasted_iota(jnp.int32, (size, HD), 0)
        at = off + (row & (WIDTH - 1)) + lax.shift_right_logical(row, WIDTH_LOG) * period
        return jnp.sum(jnp.where(lane == at, line, 0.0), axis=1, keepdims=True)

    heads = block // HD
    size = LAYER * WIDTH

    def small(q_at, q_rows, k_at, k_rows, c, b, width, causal, keep):
        start = pl.multiple_of(c * cw + b * width, width)
        shape = (q_rows * width, k_rows * width)
        r = lax.broadcasted_iota(jnp.int32, shape, 0)
        m = lax.broadcasted_iota(jnp.int32, shape, 1)
        allowed = ((r - m) & (width - 1)) == 0
        if causal is not None:
            allowed &= m <= r + causal * width
        slices = []
        for h in range(heads):
            lanes = pl.ds(h * HD, HD)
            slices.append(
                (
                    (pl.ds(q_at, q_rows), pl.ds(start, width), lanes),
                    (pl.ds(k_at, k_rows), pl.ds(start, width), lanes),
                )
            )
        found = weigh(
            [q_in[at].reshape(shape[0], HD) for at, _ in slices],
            [k_in[at].reshape(shape[1], HD) for _, at in slices],
            [v_in[at].reshape(shape[1], HD) for _, at in slices],
            allowed,
        )
        for h, (got, sums) in enumerate(found):
            o_out[slices[h][0]] = got.reshape(q_rows, width, HD)
            if keep:
                stats[c * strips + b, pl.ds(h, 1)] = spread(sums)

    strips = cw // WIDTH

    def partial(j, rows, layer):
        return remote(
            o_out.at[pl.ds(LAYER, rows), pl.ds(j * cw, cw)], p_in.at[pl.ds(0, rows), pl.ds(j * cw, cw)],
            part_send.at[0, j], part_recv.at[0, j], layer * LAYER + s, head,
        )

    def partial_stats(j, layer):
        at = pl.ds(j * strips, strips)
        return remote(
            stats.at[at], stats_in.at[at], part_send.at[1, j], part_recv.at[1, j], layer * LAYER + s, head
        )

    def back(j, d):
        return remote(
            o_out.at[peers[d], pl.ds(j * cw, cw)],
            joined.at[head, pl.ds(place(j, s), cw), feats],
            back_send.at[j, d], back_recv.at[head * LAYER + s, lax.div(j, 2)],
            here(peers[d]), lax.rem(j, 2),
        )

    def stays(j):
        return lax.rem(j, 2) == head

    def back_all(j):
        for d in (2, 3, 1):
            back(j, d).start()

        @pl.when(jnp.logical_not(stays(j)))
        def _():
            back(j, 0).start()

        @pl.when(stays(j))
        def _():
            joined[head, pl.ds(pl.multiple_of(place(j, s), cw), cw), feats] = o_out[
                s, pl.ds(pl.multiple_of(j * cw, cw), cw)
            ]

    def ext(j):
        for t in (1, 2):
            for d in (1, 2, 3):
                lay(t, j, d, True).wait_recv()
        for kind, t, base in ((0, 1, 0), (1, 2, 0), (2, 0, LAYER)):
            for d in range(4):
                up_arrival(kind, t, j, d, base).wait_recv()
        onward(j).wait_recv()
        for b in range(strips):
            small(LAYER, 2 * LAYER, 0, 2 * LAYER, j, b, WIDTH, None, True)
        partial(j, 2 * LAYER, 2).start()
        partial_stats(j, 2).start()

    def own(c):
        @pl.when(z == 0)
        def _():
            for t, ds in ((0, (1, 2, 3)), (1, (1,)), (2, (1,))):
                for d in ds:
                    lay(t, c, d, True).wait_recv()
            small(0, LAYER, LAYER, LAYER, c, 0, cw, 0, False)
            back_all(c)

        @pl.when(z == 1)
        def _():
            for d in (1, 2, 3):
                lay(0, c, d, True).wait_recv()
            small(0, LAYER, 0, 2 * LAYER, c, 0, cw, LAYER, False)
            back_all(c)

        @pl.when(z >= 2)
        def _():
            lay(0, c, 1, True).wait_recv()
            for t in (1, 2):
                for d in (1, 2, 3):
                    lay(t, c, d, True).wait_recv()

        @pl.when(z == 2)
        def _():
            for b in range(strips):
                small(0, 2 * LAYER, LAYER, LAYER, c, b, WIDTH, 0, True)

        @pl.when(z == 3)
        def _():
            small(0, LAYER, LAYER, LAYER, c, 0, cw, 0, True)

    def combine(c):
        def mix(b, base, parts, keep):
            start = pl.multiple_of(c * cw + b * WIDTH, WIDTH)
            rows = pl.ds(start, WIDTH)
            strip = c * strips + b
            for h in range(heads):
                lanes = pl.ds(h * HD, HD)
                lines = [column(ref[at, pl.ds(row + h, 1)], off, period) for _, _, ref, at, row, off, period in parts]
                top = functools.reduce(jnp.maximum, lines)
                terms = [jnp.exp(line - top) for line in lines]
                total = functools.reduce(jnp.add, terms)
                got = 0.0
                for (source, first, *_), term in zip(parts, terms):
                    value = source[pl.ds(first, LAYER), rows, lanes].reshape(size, HD)
                    got += value.astype(jnp.float32) * (term / total)
                o_out[pl.ds(base, LAYER), rows, lanes] = got.astype(jnp.bfloat16).reshape(LAYER, WIDTH, HD)
                if keep:
                    stats[strip, pl.ds(heads + h, 1)] = laid(top + jnp.log(total), size)

        @pl.when(z == 2)
        def _():
            partial(c, 2 * LAYER, 2).wait_recv()
            partial_stats(c, 2).wait_recv()
            for first in (LAYER, 0):
                off = size if first else 0
                for b in range(strips):
                    strip = c * strips + b
                    mix(
                        b,
                        first,
                        [
                            (o_out, first, stats, strip, 0, off, WIDTH),
                            (p_in, first, stats_in, strip, 0, off, WIDTH),
                        ],
                        first > 0,
                    )
                if first:
                    partial(c, LAYER, 3).start()
                    partial_stats(c, 3).start()

        @pl.when(z == 3)
        def _():
            partial(c, LAYER, 3).wait_recv()
            partial_stats(c, 3).wait_recv()
            for b in range(strips):
                strip = c * strips + b
                mix(
                    b,
                    0,
                    [
                        (o_out, 0, stats, c * strips, 0, b * WIDTH, cw),
                        (p_in, 0, stats_in, strip, heads, size, WIDTH),
                    ],
                    False,
                )

        back_all(c)

    row_copy = remote(
        row_out.at[pl.ds(pl.multiple_of(other * half, half), half)],
        joined.at[head, :, pl.ds(0, block)], row_send, row_recv, me, other,
    )
    step = 512
    count = staged.shape[1] // step

    def tiles(add):
        @pl.loop(0, count)
        def _(c):
            add(pl.ds(pl.multiple_of(c * step, step), step))

    def own_row_part(lanes):
        summed[:, lanes] = jnp.dot(
            joined[head, :, pl.ds(0, block)],
            w_own[pl.ds(0, block), lanes],
            preferred_element_type=jnp.float32,
        )

    @pl.loop(0, CHUNKS)
    def _(j):
        @pl.when(j < heads)
        def _():
            for start in range(0, stride, tile):
                row_tile(j, start)

        @pl.when(j == heads - 1)
        def _():
            row_copy.start()
            joined[head, :, pl.ds(0, block)] = row_out[pl.ds(pl.multiple_of(head * half, half), half)]

        for layer in routes:

            @pl.when((z == layer) & (j < CHUNKS // 2))
            def _():
                @pl.loop(2 * j, 2 * j + 2)
                def _(c):
                    relay(layer, c)
                    if layer == 2:
                        pass_on(c)

                    @pl.when(c + AHEAD < CHUNKS)
                    def _():
                        direct(layer, c + AHEAD)

        @pl.when(z == 1)
        def _():
            ext(j)

        @pl.when(j == heads)
        def _():
            local[-1].wait()
            tiles(own_row_part)

        @pl.when(jnp.logical_not(z_early) & (j == CHUNKS // 2))
        def _():
            w_side(1, 0).start()

        @pl.when((j > 0) & (lax.rem(j, 2) == 1))
        def _():
            w_in(0, lax.div(j, 2))

        @pl.when((j > 0) & (lax.rem(j, 2) == 0))
        def _():
            w_in(1, lax.div(j, 2) - 1)

        @pl.when(j >= CHUNKS // 2)
        def _():
            c = 2 * j - CHUNKS
            own(c)
            own(c + 1)

            @pl.when((z >= 2) & (j > CHUNKS // 2))
            def _():
                combine(j - CHUNKS // 2 - 1)

    w_in(1, PIECES - 1)

    def combine_some(first, last):
        @pl.when(z >= 2)
        def _():
            @pl.loop(first, last)
            def _(c):
                combine(c)

    def w_on_some(q, first, last):
        @pl.loop(first, last)
        def _(k):
            w_on(q, k)

    def w_from_sibling(qs, first, last):
        @pl.loop(first, last)
        def _(k):
            for q in qs:
                w_copy(w_other, q, 1 - core, k, 1, here(sib), head).wait_recv()

    def other_row_part(lanes):
        summed[:, lanes] += jnp.dot(
            joined[other, :, pl.ds(0, block)],
            w_other[pl.ds(0, block), lanes],
            preferred_element_type=jnp.float32,
        )

    def back_wait(u):
        for source_head in (head, other):
            for slot in range(LAYER):

                @pl.when(jnp.logical_not((slot == s) & (head == source_head)))
                def _():
                    for i in range(u * CHUNKS // 4, (u + 1) * CHUNKS // 4):
                        remote(
                            o_out.at[0, pl.ds(0, cw)],
                            joined.at[source_head, pl.ds(place(2 * i, slot), cw), feats],
                            back_send.at[i, 0], back_recv.at[source_head * LAYER + slot, i],
                            me, other,
                        ).wait_recv()

    quarter = block // 2
    early = pl.ds(pl.multiple_of(block + even * quarter, quarter), quarter)
    late = pl.ds(pl.multiple_of(block + (1 - even) * quarter, quarter), quarter)
    run = CHUNKS // 4 * cw

    def col_part(u):
        rows = [pl.ds(slot * (cols // 2) + u * run, run) for slot in range(LAYER)]

        def part(lanes):
            total = jnp.dot(
                jnp.concatenate([joined[head, at, feats] for at in rows]),
                w_own[feats, lanes],
                preferred_element_type=jnp.float32,
            )
            total += jnp.dot(
                jnp.concatenate([joined[other, at, early] for at in rows]),
                w_other[early, lanes],
                preferred_element_type=jnp.float32,
            )
            for slot, at in enumerate(rows):
                summed[at, lanes] += total[slot * run : (slot + 1) * run]

        tiles(part)

    combine_some(CHUNKS // 2 - 1, CHUNKS - 3)
    w_on_some(0, 0, PIECES // 2)
    w_on_some(1, 0, PIECES // 2)
    combine_some(CHUNKS - 3, CHUNKS - 1)
    w_from_sibling((0, 1, 2, 3), 0, PIECES // 2)
    row_copy.wait_recv()
    tiles(other_row_part)
    combine_some(CHUNKS - 1, CHUNKS)
    w_on_some(0, PIECES // 2, PIECES)
    w_from_sibling((2 * even, 2 * even + 1), PIECES // 2, PIECES)
    back_wait(0)
    col_part(0)
    back_wait(1)
    col_part(1)
    w_on_some(1, PIECES // 2, PIECES)
    w_from_sibling((2 - 2 * even, 3 - 2 * even), PIECES // 2, PIECES)

    def leave(c):
        lanes = pl.ds(pl.multiple_of(c * step, step), step)
        return pltpu.make_async_copy(staged.at[:, lanes], out_hbm.at[:, lanes], out_sem.at[c])

    @pl.loop(0, count)
    def _(c):
        lanes = pl.ds(pl.multiple_of(c * step, step), step)
        total = summed[:, lanes] + jnp.dot(
            joined[other, :, late], w_other[late, lanes], preferred_element_type=jnp.float32
        )
        staged[:, lanes] = total.astype(jnp.bfloat16)
        leave(c).start()

    @pl.loop(0, CHUNKS)
    def _(j):
        for t in range(3):
            for d in (1, 2, 3):
                lay(t, j, d, False).wait_send()
        for layer in routes:

            @pl.when(z == layer)
            def _():
                for kind, t, to, base in routes[layer]:
                    for d in range(4):
                        up(kind, t, j, d, to, base).wait_send()

        @pl.when(z == 1)
        def _():
            partial(j, 2 * LAYER, 2).wait_send()
            partial_stats(j, 2).wait_send()

        @pl.when(z == 2)
        def _():
            onward(j).wait_send()
            partial(j, LAYER, 3).wait_send()
            partial_stats(j, 3).wait_send()

        for d in (1, 2, 3):
            back(j, d).wait_send()

        @pl.when(jnp.logical_not(stays(j)))
        def _():
            back(j, 0).wait_send()

    @pl.loop(0, PIECES)
    def _(k):
        for q in (0, 1):
            w_first(q, k).wait_send()
            w_here(q, k).wait_send()
            w_side(q, k).wait_send()
            w_beside(q, k).wait_send()

    row_copy.wait_send()

    @pl.loop(0, count)
    def _(c):
        leave(c).wait()


def call_layered(n, queries, keys, values, w_out, half):
    _, stride, local_feat = queries.shape
    depth, width = w_out.shape
    block = local_feat // 2
    cols = stride // LAYER
    bf16, f32 = jnp.bfloat16, jnp.float32
    dma = pltpu.SemaphoreType.DMA
    blocks = cols // WIDTH
    return pl.pallas_call(
        functools.partial(layered, n),
        out_shape=jax.ShapeDtypeStruct((half, width), bf16),
        in_specs=[pl.BlockSpec(memory_space=pltpu.HBM)] * 4,
        out_specs=pl.BlockSpec(memory_space=pltpu.HBM),
        scratch_shapes=[pltpu.VMEM((stride, block), bf16)] * 3
        + [
            pltpu.VMEM((3 * LAYER, cols, block), bf16),
            pltpu.VMEM((2 * LAYER, cols, block), bf16),
            pltpu.VMEM((2 * LAYER, cols, block), bf16),
            pltpu.VMEM((3 * LAYER, cols, block), bf16),
            pltpu.VMEM((2 * LAYER, cols, block), bf16),
            pltpu.VMEM((blocks, 8, HD), f32),
            pltpu.VMEM((blocks, 8, HD), f32),
            pltpu.VMEM((stride, block), bf16),
            pltpu.VMEM((2, half, local_feat), bf16),
            pltpu.VMEM((half, width), f32),
            pltpu.VMEM((depth, width), bf16),
            pltpu.VMEM((depth, width), bf16),
            pltpu.VMEM((half, width), bf16),
            dma((4,)),
            dma((3, CHUNKS)),
            dma((3 * CHUNKS, LAYER)),
            dma((3 * CHUNKS, LAYER)),
            dma((4 * CHUNKS, LAYER)),
            dma((4 * CHUNKS, LAYER)),
            dma((2, CHUNKS)),
            dma((2, CHUNKS)),
            dma((CHUNKS, LAYER)),
            dma((2 * LAYER, CHUNKS // 2)),
            dma((3, 8 * PIECES)),
            dma((8 * PIECES,)),
            dma,
            dma,
            dma((width // 512,)),
        ],
        compiler_params=pltpu.CompilerParams(
            collective_id=0, has_side_effects=True, vmem_limit_bytes=60 * 2**20
        ),
    )(queries, keys, values, w_out)


def body(
    n, q_hbm, k_hbm, v_hbm, w_hbm, out_ref, q_row, k_row, v_row, q_col, k_col, v_col,
    col_out, row_out, joined, summed, w_own, w_other, local_sem, in_send, in_recv, back_send, back_recv,
    w_send, w_recv, row_send, row_recv,
):
    me, head = lax.axis_index("ctx"), lax.axis_index("head")
    other = 1 - head
    stride = q_hbm.shape[1]
    block = q_row.shape[1]
    depth = w_own.shape[0]
    half = joined.shape[1]
    cols = stride // n
    share = block // PARTS
    hbm = (q_hbm, k_hbm, v_hbm)
    rows_in = (q_row, k_row, v_row)
    cols_in = (q_col, k_col, v_col)
    back_head = lax.div(me * cols, half)
    member = lax.rem(me, 4)
    sibling = me + 1 - 2 * lax.rem(me, 2)
    beside = me + 2 - 4 * lax.div(member, 2)
    piece = depth // (4 * SHARES)

    def col_copy(t, part, d):
        peer = lax.rem(me + d, n)
        lanes = pl.ds(part * share, share)
        return pltpu.make_async_remote_copy(
            src_ref=hbm[t].at[0, pl.ds(peer * cols, cols), pl.ds(block + part * share, share)],
            dst_ref=cols_in[t].at[me, :, lanes],
            send_sem=in_send.at[t * PARTS + part, d],
            recv_sem=in_recv.at[t * PARTS + part, d],
            device_id=(peer, head),
            device_id_type=MESH,
        )

    def col_arrival(t, part, d):
        source = lax.rem(me + n - d, n)
        lanes = pl.ds(part * share, share)
        return pltpu.make_async_remote_copy(
            src_ref=hbm[t].at[0, pl.ds(0, cols), pl.ds(block + part * share, share)],
            dst_ref=cols_in[t].at[source, :, lanes],
            send_sem=in_send.at[t * PARTS + part, d],
            recv_sem=in_recv.at[t * PARTS + part, d],
            device_id=(source, head),
            device_id_type=MESH,
        )

    def w_copy(source, index, way, to_ctx, to_head):
        rows = pl.ds(index * piece, piece)
        return pltpu.make_async_remote_copy(
            src_ref=source.at[rows],
            dst_ref=w_other.at[rows],
            send_sem=w_send.at[way, index],
            recv_sem=w_recv.at[index],
            device_id=(to_ctx, to_head),
            device_id_type=MESH,
        )

    def index_of(who, s):
        return who * SHARES + s

    member_sibling = lax.rem(sibling, 4)
    member_beside = lax.rem(beside, 4)
    member_far = lax.rem(member + 2, 4) + 1 - 2 * lax.rem(member, 2)

    for part in range(PARTS):

        @pl.loop(1, n)
        def _(d):
            for t in range(3):
                col_copy(t, part, d).start()

    @pl.loop(0, SHARES)
    def _(s):
        w_copy(w_hbm, index_of(member, s), 0, me, other).start()

    @pl.loop(SHARES - STRAIGHT, SHARES)
    def _(s):
        w_copy(w_hbm, index_of(member_beside, s), 0, me, other).start()

    local = [
        pltpu.make_async_copy(hbm[t].at[0, :, pl.ds(0, block)], rows_in[t], local_sem.at[t])
        for t in range(3)
    ]
    local += [
        pltpu.make_async_copy(
            hbm[t].at[0, pl.ds(me * cols, cols), pl.ds(block, block)],
            cols_in[t].at[me],
            local_sem.at[3 + t],
        )
        for t in range(3)
    ]
    local.append(pltpu.make_async_copy(w_hbm, w_own, local_sem.at[3]))
    for copy in local:
        copy.start()
    for copy in local[:3]:
        copy.wait()

    tile = min(256, half)
    row_index = lax.broadcasted_iota(jnp.int32, (tile, stride), 0)
    key_index = lax.broadcasted_iota(jnp.int32, (tile, stride), 1)

    @pl.loop(0, block // HD)
    def _(h):
        lanes = pl.ds(pl.multiple_of(h * HD, HD), HD)
        for start in range(0, stride, tile):
            end = start + tile
            row_out[pl.ds(start, tile), lanes] = attend(
                q_row[pl.ds(start, tile), lanes],
                k_row[pl.ds(0, end), lanes],
                v_row[pl.ds(0, end), lanes],
                key_index[:, :end] <= row_index[:, :end] + start,
            )

    row_copy = pltpu.make_async_remote_copy(
        src_ref=row_out.at[pl.ds(pl.multiple_of(other * half, half), half)],
        dst_ref=joined.at[head, :, pl.ds(0, block)],
        send_sem=row_send,
        recv_sem=row_recv,
        device_id=(me, other),
        device_id_type=MESH,
    )
    row_copy.start()
    joined[head, :, pl.ds(0, block)] = row_out[pl.ds(pl.multiple_of(head * half, half), half)]

    def onward(first, last):
        @pl.loop(first, last)
        def _(s):
            index = index_of(member, s)
            w_copy(w_hbm, index, 0, me, other).wait_recv()

            @pl.when(s < SHARES - STRAIGHT)
            def _():
                w_copy(w_other, index, 1, beside, head).start()

            w_copy(w_other, index, 2, sibling, head).start()

    onward(0, SHARES // 2)

    for copy in local[3:]:
        copy.wait()

    step = 512

    def tiles(add):
        @pl.loop(0, out_ref.shape[1] // step)
        def _(c):
            add(pl.ds(pl.multiple_of(c * step, step), step))

    def own_row_part(lanes):
        summed[:, lanes] = jnp.dot(
            joined[head, :, pl.ds(0, block)],
            w_own[pl.ds(0, block), lanes],
            preferred_element_type=jnp.float32,
        )

    tiles(own_row_part)
    width = min(cols, max(16, 256 // n))
    size = n * width
    r_index = lax.broadcasted_iota(jnp.int32, (size, size), 0)
    s_index = lax.broadcasted_iota(jnp.int32, (size, size), 1)
    allowed = (s_index <= r_index) & (((r_index - s_index) & (width - 1)) == 0)

    slot_here = lax.rem(me, n // 2)
    stays = back_head == head

    def landing(source_head, part, slot):
        return joined.at[
            source_head,
            pl.ds(pl.multiple_of(slot * cols, cols), cols),
            pl.ds(block + part * share, share),
        ]

    def back_copy(part, r):
        return pltpu.make_async_remote_copy(
            src_ref=col_out.at[r, :, pl.ds(part * share, share)],
            dst_ref=landing(head, part, slot_here),
            send_sem=back_send.at[part, r],
            recv_sem=back_recv.at[head * PARTS + part, slot_here],
            device_id=(r, back_head),
            device_id_type=MESH,
        )

    def back_arrival(source_head, part, slot):
        return pltpu.make_async_remote_copy(
            src_ref=col_out.at[0, :, pl.ds(part * share, share)],
            dst_ref=landing(source_head, part, slot),
            send_sem=back_send.at[part, 0],
            recv_sem=back_recv.at[source_head * PARTS + part, slot],
            device_id=(me, other),
            device_id_type=MESH,
        )

    for part in range(PARTS):

        @pl.loop(1, n)
        def _(d):
            for t in range(3):
                col_arrival(t, part, d).wait_recv()

        @pl.loop(part * (share // HD), (part + 1) * (share // HD))
        def _(h):
            lanes = pl.ds(pl.multiple_of(h * HD, HD), HD)
            for start in range(0, cols, width):
                at = (slice(None), pl.ds(start, width), lanes)
                got = attend(*(ref[at].reshape(size, HD) for ref in cols_in), allowed)
                col_out[at] = got.reshape(n, width, HD)

        @pl.loop(1, n)
        def _(d):
            back_copy(part, lax.rem(me + d, n)).start()

        @pl.when(stays)
        def _():
            rows = pl.ds(pl.multiple_of(slot_here * cols, cols), cols)
            joined[head, rows, pl.ds(block + part * share, share)] = col_out[
                me, :, pl.ds(part * share, share)
            ]

        @pl.when(jnp.logical_not(stays))
        def _():
            back_copy(part, me).start()

        if part == 0:
            onward(SHARES // 2, SHARES)

    @pl.loop(0, SHARES)
    def _(s):
        index = index_of(member_beside, s)
        w_copy(w_other, index, 1, beside, head).wait_recv()
        w_copy(w_other, index, 3, sibling, head).start()

    row_copy.wait_recv()

    def back_wait(source_head):
        @pl.loop(0, n // 2)
        def _(slot):
            mine = (head * (n // 2) + slot == me) & (head == source_head)

            @pl.when(jnp.logical_not(mine))
            def _():
                for part in range(PARTS):
                    back_arrival(source_head, part, slot).wait_recv()

    back_wait(head)

    def own_col_part(lanes):
        summed[:, lanes] += jnp.dot(
            joined[head, :, pl.ds(block, block)],
            w_own[pl.ds(block, block), lanes],
            preferred_element_type=jnp.float32,
        )

    tiles(own_col_part)

    @pl.loop(0, SHARES)
    def _(s):
        w_copy(w_other, index_of(member_sibling, s), 2, sibling, head).wait_recv()
        w_copy(w_other, index_of(member_far, s), 3, sibling, head).wait_recv()

    back_wait(other)

    def other_part(lanes):
        total = summed[:, lanes] + jnp.dot(
            joined[other], w_other[:, lanes], preferred_element_type=jnp.float32
        )
        out_ref[:, lanes] = total.astype(jnp.bfloat16)

    tiles(other_part)

    for part in range(PARTS):

        @pl.loop(1, n)
        def _(d):
            for t in range(3):
                col_copy(t, part, d).wait_send()

    @pl.loop(0, SHARES)
    def _(s):
        w_copy(w_hbm, index_of(member, s), 0, me, other).wait_send()
        w_copy(w_other, index_of(member, s), 2, sibling, head).wait_send()
        w_copy(w_other, index_of(member_beside, s), 3, sibling, head).wait_send()

    @pl.loop(0, SHARES - STRAIGHT)
    def _(s):
        w_copy(w_other, index_of(member, s), 1, beside, head).wait_send()

    @pl.loop(SHARES - STRAIGHT, SHARES)
    def _(s):
        w_copy(w_hbm, index_of(member_beside, s), 0, me, other).wait_send()

    row_copy.wait_send()

    for part in range(PARTS):

        @pl.loop(1, n)
        def _(d):
            back_copy(part, lax.rem(me + d, n)).wait_send()

        @pl.when(jnp.logical_not(stays))
        def _():
            back_copy(part, me).wait_send()


def on_device(n, queries, keys, values, w_out):
    _, stride, local_feat = queries.shape
    depth, model_width = w_out.shape
    block = GROUP * HD
    assert queries.shape[0] == 1 and local_feat == 2 * block
    half = stride // lax.axis_size("head")
    cols = stride // n
    if n == LAYER * LAYER and stride % (LAYER * CHUNKS * WIDTH) == 0:
        out = call_layered(n, queries, keys, values, w_out, half)
        return out.reshape((1, half, model_width))
    bf16 = jnp.bfloat16
    dma = pltpu.SemaphoreType.DMA
    out = pl.pallas_call(
        functools.partial(body, n),
        out_shape=jax.ShapeDtypeStruct((half, model_width), bf16),
        in_specs=[pl.BlockSpec(memory_space=pltpu.HBM)] * 4,
        out_specs=pl.BlockSpec(memory_space=pltpu.VMEM),
        scratch_shapes=[pltpu.VMEM((stride, block), bf16)] * 3
        + [pltpu.VMEM((n, cols, block), bf16)] * 4
        + [
            pltpu.VMEM((stride, block), bf16),
            pltpu.VMEM((2, half, local_feat), bf16),
            pltpu.VMEM((half, model_width), jnp.float32),
            pltpu.VMEM((depth, model_width), bf16),
            pltpu.VMEM((depth, model_width), bf16),
            dma((7,)),
            dma((3 * PARTS, n)),
            dma((3 * PARTS, n)),
            dma((PARTS, n)),
            dma((2 * PARTS, n // 2)),
            dma((4, 4 * SHARES)),
            dma((4 * SHARES,)),
            dma,
            dma,
        ],
        compiler_params=pltpu.CompilerParams(has_side_effects=True, vmem_limit_bytes=60 * 2**20),
    )(queries, keys, values, w_out)
    return out.reshape((1, half, model_width))


def solution(mesh):
    return jax.shard_map(
        functools.partial(on_device, mesh.shape["ctx"]),
        mesh=mesh,
        in_specs=(
            P("ctx", None, "head"),
            P("ctx", None, "head"),
            P("ctx", None, "head"),
            P("head", None),
        ),
        out_specs=P("ctx", "head", None),
        check_vma=False,
    )
```

```python
import functools

import jax
import jax.numpy as jnp
from jax import lax
from jax.experimental import pallas as pl
from jax.experimental.pallas import tpu as pltpu
from jax.sharding import PartitionSpec as P

HD = 128
GROUP = 4
MESH = pl.DeviceIdType.MESH
SHARES = 8
STRAIGHT = 2
PARTS = 2
LAYER = 4
CHUNKS = 8
WIDTH = 16
WIDTH_LOG = 4
PIECES = 4
AHEAD = 3

masked_score = -1e30


def attend(query, key, value, allowed):
    scores = lax.dot_general(
        query, key, (((1,), (1,)), ((), ())), preferred_element_type=jnp.float32
    ) * jnp.float32(1.0 / HD**0.5)
    scores = jnp.where(allowed, scores, masked_score)
    top = jnp.max(scores, axis=-1, keepdims=True)
    expo = jnp.exp(scores - top)
    total = jnp.sum(expo, axis=-1, keepdims=True)
    mixed = jnp.dot(expo.astype(jnp.bfloat16), value, preferred_element_type=jnp.float32)
    return (mixed / total).astype(jnp.bfloat16)


def weigh(queries, keys, values, allowed):
    scores = [
        lax.dot_general(q, k, (((1,), (1,)), ((), ())), preferred_element_type=jnp.float32)
        for q, k in zip(queries, keys)
    ]
    scores = [jnp.where(allowed, s * jnp.float32(1.0 / HD**0.5), masked_score) for s in scores]
    tops = [jnp.max(s, axis=-1, keepdims=True) for s in scores]
    expos = [jnp.exp(s - top) for s, top in zip(scores, tops)]
    totals = [jnp.sum(e, axis=-1, keepdims=True) for e in expos]
    mixed = [
        jnp.dot(e.astype(jnp.bfloat16), v, preferred_element_type=jnp.float32)
        for e, v in zip(expos, values)
    ]
    return [
        ((m / total).astype(jnp.bfloat16), top + jnp.log(total))
        for m, total, top in zip(mixed, totals, tops)
    ]


def layered(
    n, q_hbm, k_hbm, v_hbm, w_hbm, out_hbm, q_row, k_row, v_row, q_in, k_in, v_in, o_out, p_in,
    stats, stats_in, row_out, joined, summed, w_own, w_other, staged,
    local_sem, chunk_sem, lay_send, lay_recv, up_send, up_recv, part_send, part_recv,
    back_send, back_recv, w_send, w_recv, row_send, row_recv, out_sem,
):
    me, head = lax.axis_index("ctx"), lax.axis_index("head")
    other = 1 - head
    z, s = lax.div(me, LAYER), lax.rem(me, LAYER)
    core = lax.rem(s, 2)
    sib = s + 1 - 2 * core
    opp = s + 2 - 4 * lax.div(s, 2)
    far = sib + 2 - 4 * lax.div(sib, 2)
    peers = (s, sib, opp, far)
    stride = q_hbm.shape[1]
    block = q_row.shape[1]
    depth = w_own.shape[0]
    half = joined.shape[1]
    cols = stride // LAYER
    cw = cols // CHUNKS
    hbm = (q_hbm, k_hbm, v_hbm)
    ins = (q_in, k_in, v_in)
    own_at = (0, LAYER, LAYER)
    feats = pl.ds(block, block)

    def place(j, slot):
        return slot * (cols // 2) + lax.div(j, 2) * cw

    def chunk_of(j, slot):
        return pl.ds(pl.multiple_of(lax.rem(j, 2) * half + place(j, slot), cw), cw)

    def remote(src, dst, send, recv, ctx, at):
        return pltpu.make_async_remote_copy(
            src_ref=src, dst_ref=dst, send_sem=send, recv_sem=recv,
            device_id=(ctx, at), device_id_type=MESH,
        )

    def here(slot):
        return z * LAYER + slot

    def lay(t, j, d, source):
        row = peers[d] if source else s
        return remote(
            hbm[t].at[0, chunk_of(j, peers[d]), feats],
            ins[t].at[own_at[t] + row, pl.ds(j * cw, cw)],
            lay_send.at[t * CHUNKS + j, d], lay_recv.at[t * CHUNKS + j, d],
            here(peers[d]), head,
        )

    def up(kind, t, j, d, layer, base):
        if d < 2:
            src, slot, row = hbm[t].at[0, chunk_of(j, peers[d]), feats], peers[d], s
        else:
            src, slot, row = ins[t].at[own_at[t] + peers[d], pl.ds(j * cw, cw)], s, peers[d]
        return remote(
            src, ins[t].at[base + row, pl.ds(j * cw, cw)],
            up_send.at[kind * CHUNKS + j, d], up_recv.at[kind * CHUNKS + j, d],
            layer * LAYER + slot, head,
        )

    def up_arrival(kind, t, j, d, base):
        return remote(
            hbm[t].at[0, pl.ds(0, cw), feats], ins[t].at[base + peers[d], pl.ds(j * cw, cw)],
            up_send.at[kind * CHUNKS + j, d], up_recv.at[kind * CHUNKS + j, d],
            here(sib), head,
        )

    routes = {
        0: ((0, 1, 1, 0), (1, 2, 1, 0)),
        2: ((2, 0, 1, LAYER),),
        3: ((2, 0, 2, LAYER),),
    }

    def onward(j):
        at = pl.ds(j * cw, cw)
        return remote(
            q_in.at[pl.ds(LAYER, LAYER), at], q_in.at[pl.ds(2 * LAYER, LAYER), at],
            up_send.at[3 * CHUNKS + j, 0], up_recv.at[3 * CHUNKS + j, 0], LAYER + s, head,
        )

    def pass_on(j):
        for d in range(4):
            up_arrival(2, 0, j, d, LAYER).wait_recv()
        onward(j).start()

    def direct(layer, j):
        for kind, t, to, base in routes[layer]:
            for d in (0, 1):
                up(kind, t, j, d, to, base).start()

    def relay(layer, j):
        for t in sorted({t for _, t, _, _ in routes[layer]}):
            for d in (2, 3):
                lay(t, j, d, True).wait_recv()
                for kind, t2, to, base in routes[layer]:
                    if t2 == t:
                        up(kind, t, j, d, to, base).start()

    def piece_rows(q, c, k):
        eighth = depth // 16
        rows = eighth // (PIECES // 2)
        start = lax.div(k, PIECES // 2) * (depth // 2)
        start += (q * 2 + c) * eighth + lax.rem(k, PIECES // 2) * rows
        return pl.ds(start, rows)

    def w_copy(source, q, c, k, way, to_ctx, to_head):
        rows = piece_rows(q, c, k)
        index = (q * 2 + c) * PIECES + k
        return remote(
            source.at[rows], w_other.at[rows], w_send.at[way, index], w_recv.at[index], to_ctx, to_head
        )

    even = lax.rem(z + lax.div(s, 2), 2)
    y_next = here(opp)
    z_next = me + LAYER - 2 * LAYER * lax.rem(z, 2)
    z_early = (z == 1) | (z == 2)

    def to_side(k):
        return (z > 0) | (k < PIECES // 2)

    def w_first(q, k):
        return w_copy(w_hbm, 2 * even + q, core, k, 0, me, other)

    def w_side(q, k):
        return w_copy(w_other, 2 * even + q, core, k, 2, y_next if q == 0 else z_next, head)

    def w_extra(k):
        return w_copy(w_other, 2 * even + 1, core, k, 3, me - LAYER, head)

    def w_beside(q, k):
        return w_copy(w_other, 2 * (1 - even) + q, core, k, 1, here(sib), head)

    def w_here(q, k):
        return w_copy(w_other, 2 * even + q, core, k, 1, here(sib), head)

    def w_in(q, k):
        w_first(q, k).wait_recv()
        w_here(q, k).start()
        if q == 0:
            w_side(q, k).start()
        else:

            @pl.when(z_early)
            def _():
                w_side(q, k).start()

            @pl.when((z == 2) & (k >= PIECES // 2))
            def _():
                w_extra(k).start()

    def w_step(i):
        high = z >= 2
        for_z = jnp.where(high, jnp.where(i < PIECES, 1, 0), lax.rem(i, 2))
        k = jnp.where(high, lax.rem(i, PIECES), lax.div(i, 2))

        @pl.when(for_z == 1)
        def _():
            w_in(1, k)

        @pl.when(for_z == 0)
        def _():
            w_in(0, k)

    def w_on(q, k):
        w_copy(w_other, 2 * (1 - even) + q, core, k, 2, me, other).wait_recv()
        w_beside(q, k).start()

    ready = pltpu.get_barrier_semaphore()

    def greet(ctx, at):
        pl.semaphore_signal(ready, 1, device_id=(ctx, at), device_id_type=MESH)

    greet(me, other)
    for d in (1, 2, 3):
        greet(here(peers[d]), head)
        greet(here(peers[d]), other)
    for edge, towards in ((0, -LAYER), (LAYER - 1, LAYER)):

        @pl.when(z != edge)
        def _():
            greet(here(s) + towards, head)
            greet(here(sib) + towards, head)

    local = [
        pltpu.make_async_copy(hbm[t].at[0, :, pl.ds(0, block)], (q_row, k_row, v_row)[t], local_sem.at[t])
        for t in range(3)
    ]
    local += [
        pltpu.make_async_copy(
            hbm[t].at[0, chunk_of(j, s), feats],
            ins[t].at[own_at[t] + s, pl.ds(j * cw, cw)],
            chunk_sem.at[t, j],
        )
        for t in range(3)
        for j in range(CHUNKS)
    ]
    local.append(pltpu.make_async_copy(w_hbm, w_own, local_sem.at[3]))
    for copy in local:
        copy.start()

    inner = jnp.minimum(z, 1) + jnp.minimum(LAYER - 1 - z, 1)
    pl.semaphore_wait(ready, 2 * LAYER - 1 + 2 * inner)

    def exchange(ts):
        @pl.loop(0, CHUNKS)
        def _(j):
            for t in ts:
                for d in (2, 3, 1):
                    lay(t, j, d, False).start()

    for layer in routes:

        @pl.when(z == layer)
        def _():
            for j in range(AHEAD):
                direct(layer, j)

    @pl.when(z < 2)
    def _():
        exchange((1, 2))
        exchange((0,))

    @pl.when(z >= 2)
    def _():
        exchange((0,))
        exchange((1, 2))

    @pl.when(z < 2)
    def _():
        @pl.loop(0, PIECES)
        def _(k):
            w_first(0, k).start()
            w_first(1, k).start()

    @pl.when(z >= 2)
    def _():
        for q in (1, 0):

            @pl.loop(0, PIECES)
            def _(k):
                w_first(q, k).start()

    for copy in local[:-1]:
        copy.wait()

    tile = min(256, half)
    row_index = lax.broadcasted_iota(jnp.int32, (tile, stride), 0)
    key_index = lax.broadcasted_iota(jnp.int32, (tile, stride), 1)

    def row_tile(h, start):
        lanes = pl.ds(pl.multiple_of(h * HD, HD), HD)
        end = start + tile
        row_out[pl.ds(start, tile), lanes] = attend(
            q_row[pl.ds(start, tile), lanes],
            k_row[pl.ds(0, end), lanes],
            v_row[pl.ds(0, end), lanes],
            key_index[:, :end] <= row_index[:, :end] + start,
        )

    def spread(sums):
        lane = lax.broadcasted_iota(jnp.int32, (HD, HD), 1)
        row = lax.broadcasted_iota(jnp.int32, (HD, HD), 0)
        return jnp.sum(jnp.where(lane == row, sums, 0.0), axis=0, keepdims=True)

    def laid(sums, off):
        lane = lax.broadcasted_iota(jnp.int32, (size, HD), 1)
        row = lax.broadcasted_iota(jnp.int32, (size, HD), 0)
        return jnp.sum(jnp.where(lane == row + off, sums, 0.0), axis=0, keepdims=True)

    def column(line, off, period):
        lane = lax.broadcasted_iota(jnp.int32, (size, HD), 1)
        row = lax.broadcasted_iota(jnp.int32, (size, HD), 0)
        at = off + (row & (WIDTH - 1)) + lax.shift_right_logical(row, WIDTH_LOG) * period
        return jnp.sum(jnp.where(lane == at, line, 0.0), axis=1, keepdims=True)

    heads = block // HD
    size = LAYER * WIDTH

    def small(q_at, q_rows, k_at, k_rows, c, b, width, causal, keep):
        start = pl.multiple_of(c * cw + b * width, width)
        shape = (q_rows * width, k_rows * width)
        r = lax.broadcasted_iota(jnp.int32, shape, 0)
        m = lax.broadcasted_iota(jnp.int32, shape, 1)
        allowed = ((r - m) & (width - 1)) == 0
        if causal is not None:
            allowed &= m <= r + causal * width
        slices = []
        for h in range(heads):
            lanes = pl.ds(h * HD, HD)
            slices.append(
                (
                    (pl.ds(q_at, q_rows), pl.ds(start, width), lanes),
                    (pl.ds(k_at, k_rows), pl.ds(start, width), lanes),
                )
            )
        found = weigh(
            [q_in[at].reshape(shape[0], HD) for at, _ in slices],
            [k_in[at].reshape(shape[1], HD) for _, at in slices],
            [v_in[at].reshape(shape[1], HD) for _, at in slices],
            allowed,
        )
        for h, (got, sums) in enumerate(found):
            o_out[slices[h][0]] = got.reshape(q_rows, width, HD)
            if keep:
                stats[c * strips + b, pl.ds(h, 1)] = spread(sums)

    strips = cw // WIDTH

    def partial(j, rows, layer):
        return remote(
            o_out.at[pl.ds(LAYER, rows), pl.ds(j * cw, cw)], p_in.at[pl.ds(0, rows), pl.ds(j * cw, cw)],
            part_send.at[0, j], part_recv.at[0, j], layer * LAYER + s, head,
        )

    def partial_stats(j, layer):
        at = pl.ds(j * strips, strips)
        return remote(
            stats.at[at], stats_in.at[at], part_send.at[1, j], part_recv.at[1, j], layer * LAYER + s, head
        )

    def back(j, d):
        return remote(
            o_out.at[peers[d], pl.ds(j * cw, cw)],
            joined.at[head, pl.ds(place(j, s), cw), feats],
            back_send.at[j, d], back_recv.at[head * LAYER + s, lax.div(j, 2)],
            here(peers[d]), lax.rem(j, 2),
        )

    def stays(j):
        return lax.rem(j, 2) == head

    def back_all(j):
        for d in (2, 3, 1):
            back(j, d).start()

        @pl.when(jnp.logical_not(stays(j)))
        def _():
            back(j, 0).start()

        @pl.when(stays(j))
        def _():
            joined[head, pl.ds(pl.multiple_of(place(j, s), cw), cw), feats] = o_out[
                s, pl.ds(pl.multiple_of(j * cw, cw), cw)
            ]

    def ext(j):
        for t in (1, 2):
            for d in (1, 2, 3):
                lay(t, j, d, True).wait_recv()
        for kind, t, base in ((0, 1, 0), (1, 2, 0), (2, 0, LAYER)):
            for d in range(4):
                up_arrival(kind, t, j, d, base).wait_recv()
        onward(j).wait_recv()
        for b in range(strips):
            small(LAYER, 2 * LAYER, 0, 2 * LAYER, j, b, WIDTH, None, True)
        partial(j, 2 * LAYER, 2).start()
        partial_stats(j, 2).start()

    def own(c):
        @pl.when(z == 0)
        def _():
            for t, ds in ((0, (1, 2, 3)), (1, (1,)), (2, (1,))):
                for d in ds:
                    lay(t, c, d, True).wait_recv()
            small(0, LAYER, LAYER, LAYER, c, 0, cw, 0, False)
            back_all(c)

        @pl.when(z == 1)
        def _():
            for d in (1, 2, 3):
                lay(0, c, d, True).wait_recv()
            small(0, LAYER, 0, 2 * LAYER, c, 0, cw, LAYER, False)
            back_all(c)

        @pl.when(z >= 2)
        def _():
            lay(0, c, 1, True).wait_recv()
            for t in (1, 2):
                for d in (1, 2, 3):
                    lay(t, c, d, True).wait_recv()

        @pl.when(z == 2)
        def _():
            for b in range(strips):
                small(0, 2 * LAYER, LAYER, LAYER, c, b, WIDTH, 0, True)

        @pl.when(z == 3)
        def _():
            small(0, LAYER, LAYER, LAYER, c, 0, cw, 0, True)

    def combine(c):
        def mix(b, base, parts, keep):
            start = pl.multiple_of(c * cw + b * WIDTH, WIDTH)
            rows = pl.ds(start, WIDTH)
            strip = c * strips + b
            for h in range(heads):
                lanes = pl.ds(h * HD, HD)
                lines = [column(ref[at, pl.ds(row + h, 1)], off, period) for _, _, ref, at, row, off, period in parts]
                top = functools.reduce(jnp.maximum, lines)
                terms = [jnp.exp(line - top) for line in lines]
                total = functools.reduce(jnp.add, terms)
                got = 0.0
                for (source, first, *_), term in zip(parts, terms):
                    value = source[pl.ds(first, LAYER), rows, lanes].reshape(size, HD)
                    got += value.astype(jnp.float32) * (term / total)
                o_out[pl.ds(base, LAYER), rows, lanes] = got.astype(jnp.bfloat16).reshape(LAYER, WIDTH, HD)
                if keep:
                    stats[strip, pl.ds(heads + h, 1)] = laid(top + jnp.log(total), size)

        @pl.when(z == 2)
        def _():
            partial(c, 2 * LAYER, 2).wait_recv()
            partial_stats(c, 2).wait_recv()
            for first in (LAYER, 0):
                off = size if first else 0
                for b in range(strips):
                    strip = c * strips + b
                    mix(
                        b,
                        first,
                        [
                            (o_out, first, stats, strip, 0, off, WIDTH),
                            (p_in, first, stats_in, strip, 0, off, WIDTH),
                        ],
                        first > 0,
                    )
                if first:
                    partial(c, LAYER, 3).start()
                    partial_stats(c, 3).start()

        @pl.when(z == 3)
        def _():
            partial(c, LAYER, 3).wait_recv()
            partial_stats(c, 3).wait_recv()
            for b in range(strips):
                strip = c * strips + b
                mix(
                    b,
                    0,
                    [
                        (o_out, 0, stats, c * strips, 0, b * WIDTH, cw),
                        (p_in, 0, stats_in, strip, heads, size, WIDTH),
                    ],
                    False,
                )

        back_all(c)

    row_copy = remote(
        row_out.at[pl.ds(pl.multiple_of(other * half, half), half)],
        joined.at[head, :, pl.ds(0, block)], row_send, row_recv, me, other,
    )
    step = 512
    count = w_own.shape[1] // step

    def tiles(add):
        @pl.loop(0, count)
        def _(c):
            add(pl.ds(pl.multiple_of(c * step, step), step))

    def own_row_part(lanes):
        summed[:, lanes] = jnp.dot(
            joined[head, :, pl.ds(0, block)],
            w_own[pl.ds(0, block), lanes],
            preferred_element_type=jnp.float32,
        )

    @pl.loop(0, CHUNKS)
    def _(j):
        @pl.when(j < heads)
        def _():
            for start in range(0, stride, tile):
                row_tile(j, start)

        @pl.when(j == heads - 1)
        def _():
            row_copy.start()
            joined[head, :, pl.ds(0, block)] = row_out[pl.ds(pl.multiple_of(head * half, half), half)]

        for layer in routes:

            @pl.when((z == layer) & (j < CHUNKS // 2))
            def _():
                @pl.loop(2 * j, 2 * j + 2)
                def _(c):
                    relay(layer, c)
                    if layer == 2:
                        pass_on(c)

                    @pl.when(c + AHEAD < CHUNKS)
                    def _():
                        direct(layer, c + AHEAD)

        @pl.when(z == 1)
        def _():
            ext(j)

        @pl.when(j == heads)
        def _():
            local[-1].wait()
            tiles(own_row_part)

        i = j - jnp.where(z == 1, 0, 1)

        @pl.when(i >= 0)
        def _():
            w_step(i)

        @pl.when(jnp.logical_not(z_early) & (j == PIECES))
        def _():
            @pl.loop(0, PIECES)
            def _(k):
                @pl.when(to_side(k))
                def _():
                    w_side(1, k).start()

        @pl.when(j >= CHUNKS // 2)
        def _():
            c = 2 * j - CHUNKS
            own(c)
            own(c + 1)

            lag = z - 2

            @pl.when((z >= 2) & (j >= CHUNKS // 2 + lag))
            def _():
                combine(j - CHUNKS // 2 - lag)

    @pl.when(z != 1)
    def _():
        w_step(2 * PIECES - 1)

    def combine_some(layer, first, last):
        @pl.when(z == layer)
        def _():
            @pl.loop(first, last)
            def _(c):
                combine(c)

    def w_on_some(q, first, last):
        @pl.loop(first, last)
        def _(k):
            w_on(q, k)

    def w_from_sibling(qs, first, last):
        @pl.loop(first, last)
        def _(k):
            for q in qs:
                w_copy(w_other, q, 1 - core, k, 1, here(sib), head).wait_recv()

    def other_row_part(lanes):
        summed[:, lanes] += jnp.dot(
            joined[other, :, pl.ds(0, block)],
            w_other[pl.ds(0, block), lanes],
            preferred_element_type=jnp.float32,
        )

    def back_wait(u):
        for source_head in (head, other):
            for slot in range(LAYER):

                @pl.when(jnp.logical_not((slot == s) & (head == source_head)))
                def _():
                    for i in range(u * CHUNKS // 4, (u + 1) * CHUNKS // 4):
                        remote(
                            o_out.at[0, pl.ds(0, cw)],
                            joined.at[source_head, pl.ds(place(2 * i, slot), cw), feats],
                            back_send.at[i, 0], back_recv.at[source_head * LAYER + slot, i],
                            me, other,
                        ).wait_recv()

    run = CHUNKS // 4 * cw

    def leave(u, c):
        lanes = pl.ds(pl.multiple_of(c * step, step), step)
        return pltpu.make_async_copy(
            staged.at[:, u, :, lanes], out_hbm.at[:, u, :, lanes], out_sem.at[u, c]
        )

    def finish(u):
        rows = [pl.ds(slot * (cols // 2) + u * run, run) for slot in range(LAYER)]

        @pl.loop(0, count)
        def _(c):
            lanes = pl.ds(pl.multiple_of(c * step, step), step)
            total = jnp.dot(
                jnp.concatenate([joined[head, at, feats] for at in rows]),
                w_own[feats, lanes],
                preferred_element_type=jnp.float32,
            )
            total += jnp.dot(
                jnp.concatenate([joined[other, at, feats] for at in rows]),
                w_other[feats, lanes],
                preferred_element_type=jnp.float32,
            )
            for slot, at in enumerate(rows):
                part = summed[at, lanes] + total[slot * run : (slot + 1) * run]
                staged[slot, u, :, lanes] = part.astype(jnp.bfloat16)
            leave(u, c).start()

    combine_some(2, CHUNKS // 2, CHUNKS)
    combine_some(3, CHUNKS // 2 - 1, CHUNKS - 3)
    w_on_some(0, 0, PIECES // 2)
    w_on_some(1, 0, PIECES // 2)
    combine_some(3, CHUNKS - 3, CHUNKS - 1)
    w_from_sibling((0, 1, 2, 3), 0, PIECES // 2)
    row_copy.wait_recv()
    tiles(other_row_part)
    combine_some(3, CHUNKS - 1, CHUNKS)
    w_on_some(0, PIECES // 2, PIECES)
    w_on_some(1, PIECES // 2, PIECES)
    w_from_sibling((0, 1, 2, 3), PIECES // 2, PIECES)
    back_wait(0)
    finish(0)
    back_wait(1)
    finish(1)

    @pl.loop(0, CHUNKS)
    def _(j):
        for t in range(3):
            for d in (1, 2, 3):
                lay(t, j, d, False).wait_send()
        for layer in routes:

            @pl.when(z == layer)
            def _():
                for kind, t, to, base in routes[layer]:
                    for d in range(4):
                        up(kind, t, j, d, to, base).wait_send()

        @pl.when(z == 1)
        def _():
            partial(j, 2 * LAYER, 2).wait_send()
            partial_stats(j, 2).wait_send()

        @pl.when(z == 2)
        def _():
            onward(j).wait_send()
            partial(j, LAYER, 3).wait_send()
            partial_stats(j, 3).wait_send()

        for d in (1, 2, 3):
            back(j, d).wait_send()

        @pl.when(jnp.logical_not(stays(j)))
        def _():
            back(j, 0).wait_send()

    @pl.loop(0, PIECES)
    def _(k):
        for q in (0, 1):
            w_first(q, k).wait_send()
            w_here(q, k).wait_send()
            w_beside(q, k).wait_send()
        w_side(0, k).wait_send()

        @pl.when(to_side(k))
        def _():
            w_side(1, k).wait_send()

        @pl.when((z == 2) & (k >= PIECES // 2))
        def _():
            w_extra(k).wait_send()

    row_copy.wait_send()

    @pl.loop(0, count)
    def _(c):
        leave(0, c).wait()
        leave(1, c).wait()


def call_layered(n, queries, keys, values, w_out, half):
    _, stride, local_feat = queries.shape
    depth, width = w_out.shape
    block = local_feat // 2
    cols = stride // LAYER
    bf16, f32 = jnp.bfloat16, jnp.float32
    dma = pltpu.SemaphoreType.DMA
    blocks = cols // WIDTH
    return pl.pallas_call(
        functools.partial(layered, n),
        out_shape=jax.ShapeDtypeStruct((LAYER, 2, half // (2 * LAYER), width), bf16),
        in_specs=[pl.BlockSpec(memory_space=pltpu.HBM)] * 4,
        out_specs=pl.BlockSpec(memory_space=pltpu.HBM),
        scratch_shapes=[pltpu.VMEM((stride, block), bf16)] * 3
        + [
            pltpu.VMEM((3 * LAYER, cols, block), bf16),
            pltpu.VMEM((2 * LAYER, cols, block), bf16),
            pltpu.VMEM((2 * LAYER, cols, block), bf16),
            pltpu.VMEM((3 * LAYER, cols, block), bf16),
            pltpu.VMEM((2 * LAYER, cols, block), bf16),
            pltpu.VMEM((blocks, 8, HD), f32),
            pltpu.VMEM((blocks, 8, HD), f32),
            pltpu.VMEM((stride, block), bf16),
            pltpu.VMEM((2, half, local_feat), bf16),
            pltpu.VMEM((half, width), f32),
            pltpu.VMEM((depth, width), bf16),
            pltpu.VMEM((depth, width), bf16),
            pltpu.VMEM((LAYER, 2, half // (2 * LAYER), width), bf16),
            dma((4,)),
            dma((3, CHUNKS)),
            dma((3 * CHUNKS, LAYER)),
            dma((3 * CHUNKS, LAYER)),
            dma((4 * CHUNKS, LAYER)),
            dma((4 * CHUNKS, LAYER)),
            dma((2, CHUNKS)),
            dma((2, CHUNKS)),
            dma((CHUNKS, LAYER)),
            dma((2 * LAYER, CHUNKS // 2)),
            dma((4, 8 * PIECES)),
            dma((8 * PIECES,)),
            dma,
            dma,
            dma((2, width // 512)),
        ],
        compiler_params=pltpu.CompilerParams(
            collective_id=0, has_side_effects=True, vmem_limit_bytes=60 * 2**20
        ),
    )(queries, keys, values, w_out)


def body(
    n, q_hbm, k_hbm, v_hbm, w_hbm, out_ref, q_row, k_row, v_row, q_col, k_col, v_col,
    col_out, row_out, joined, summed, w_own, w_other, local_sem, in_send, in_recv, back_send, back_recv,
    w_send, w_recv, row_send, row_recv,
):
    me, head = lax.axis_index("ctx"), lax.axis_index("head")
    other = 1 - head
    stride = q_hbm.shape[1]
    block = q_row.shape[1]
    depth = w_own.shape[0]
    half = joined.shape[1]
    cols = stride // n
    share = block // PARTS
    hbm = (q_hbm, k_hbm, v_hbm)
    rows_in = (q_row, k_row, v_row)
    cols_in = (q_col, k_col, v_col)
    back_head = lax.div(me * cols, half)
    member = lax.rem(me, 4)
    sibling = me + 1 - 2 * lax.rem(me, 2)
    beside = me + 2 - 4 * lax.div(member, 2)
    piece = depth // (4 * SHARES)

    def col_copy(t, part, d):
        peer = lax.rem(me + d, n)
        lanes = pl.ds(part * share, share)
        return pltpu.make_async_remote_copy(
            src_ref=hbm[t].at[0, pl.ds(peer * cols, cols), pl.ds(block + part * share, share)],
            dst_ref=cols_in[t].at[me, :, lanes],
            send_sem=in_send.at[t * PARTS + part, d],
            recv_sem=in_recv.at[t * PARTS + part, d],
            device_id=(peer, head),
            device_id_type=MESH,
        )

    def col_arrival(t, part, d):
        source = lax.rem(me + n - d, n)
        lanes = pl.ds(part * share, share)
        return pltpu.make_async_remote_copy(
            src_ref=hbm[t].at[0, pl.ds(0, cols), pl.ds(block + part * share, share)],
            dst_ref=cols_in[t].at[source, :, lanes],
            send_sem=in_send.at[t * PARTS + part, d],
            recv_sem=in_recv.at[t * PARTS + part, d],
            device_id=(source, head),
            device_id_type=MESH,
        )

    def w_copy(source, index, way, to_ctx, to_head):
        rows = pl.ds(index * piece, piece)
        return pltpu.make_async_remote_copy(
            src_ref=source.at[rows],
            dst_ref=w_other.at[rows],
            send_sem=w_send.at[way, index],
            recv_sem=w_recv.at[index],
            device_id=(to_ctx, to_head),
            device_id_type=MESH,
        )

    def index_of(who, s):
        return who * SHARES + s

    member_sibling = lax.rem(sibling, 4)
    member_beside = lax.rem(beside, 4)
    member_far = lax.rem(member + 2, 4) + 1 - 2 * lax.rem(member, 2)

    for part in range(PARTS):

        @pl.loop(1, n)
        def _(d):
            for t in range(3):
                col_copy(t, part, d).start()

    @pl.loop(0, SHARES)
    def _(s):
        w_copy(w_hbm, index_of(member, s), 0, me, other).start()

    @pl.loop(SHARES - STRAIGHT, SHARES)
    def _(s):
        w_copy(w_hbm, index_of(member_beside, s), 0, me, other).start()

    local = [
        pltpu.make_async_copy(hbm[t].at[0, :, pl.ds(0, block)], rows_in[t], local_sem.at[t])
        for t in range(3)
    ]
    local += [
        pltpu.make_async_copy(
            hbm[t].at[0, pl.ds(me * cols, cols), pl.ds(block, block)],
            cols_in[t].at[me],
            local_sem.at[3 + t],
        )
        for t in range(3)
    ]
    local.append(pltpu.make_async_copy(w_hbm, w_own, local_sem.at[3]))
    for copy in local:
        copy.start()
    for copy in local[:3]:
        copy.wait()

    tile = min(256, half)
    row_index = lax.broadcasted_iota(jnp.int32, (tile, stride), 0)
    key_index = lax.broadcasted_iota(jnp.int32, (tile, stride), 1)

    @pl.loop(0, block // HD)
    def _(h):
        lanes = pl.ds(pl.multiple_of(h * HD, HD), HD)
        for start in range(0, stride, tile):
            end = start + tile
            row_out[pl.ds(start, tile), lanes] = attend(
                q_row[pl.ds(start, tile), lanes],
                k_row[pl.ds(0, end), lanes],
                v_row[pl.ds(0, end), lanes],
                key_index[:, :end] <= row_index[:, :end] + start,
            )

    row_copy = pltpu.make_async_remote_copy(
        src_ref=row_out.at[pl.ds(pl.multiple_of(other * half, half), half)],
        dst_ref=joined.at[head, :, pl.ds(0, block)],
        send_sem=row_send,
        recv_sem=row_recv,
        device_id=(me, other),
        device_id_type=MESH,
    )
    row_copy.start()
    joined[head, :, pl.ds(0, block)] = row_out[pl.ds(pl.multiple_of(head * half, half), half)]

    def onward(first, last):
        @pl.loop(first, last)
        def _(s):
            index = index_of(member, s)
            w_copy(w_hbm, index, 0, me, other).wait_recv()

            @pl.when(s < SHARES - STRAIGHT)
            def _():
                w_copy(w_other, index, 1, beside, head).start()

            w_copy(w_other, index, 2, sibling, head).start()

    onward(0, SHARES // 2)

    for copy in local[3:]:
        copy.wait()

    step = 512

    def tiles(add):
        @pl.loop(0, out_ref.shape[1] // step)
        def _(c):
            add(pl.ds(pl.multiple_of(c * step, step), step))

    def own_row_part(lanes):
        summed[:, lanes] = jnp.dot(
            joined[head, :, pl.ds(0, block)],
            w_own[pl.ds(0, block), lanes],
            preferred_element_type=jnp.float32,
        )

    tiles(own_row_part)
    width = min(cols, max(16, 256 // n))
    size = n * width
    r_index = lax.broadcasted_iota(jnp.int32, (size, size), 0)
    s_index = lax.broadcasted_iota(jnp.int32, (size, size), 1)
    allowed = (s_index <= r_index) & (((r_index - s_index) & (width - 1)) == 0)

    slot_here = lax.rem(me, n // 2)
    stays = back_head == head

    def landing(source_head, part, slot):
        return joined.at[
            source_head,
            pl.ds(pl.multiple_of(slot * cols, cols), cols),
            pl.ds(block + part * share, share),
        ]

    def back_copy(part, r):
        return pltpu.make_async_remote_copy(
            src_ref=col_out.at[r, :, pl.ds(part * share, share)],
            dst_ref=landing(head, part, slot_here),
            send_sem=back_send.at[part, r],
            recv_sem=back_recv.at[head * PARTS + part, slot_here],
            device_id=(r, back_head),
            device_id_type=MESH,
        )

    def back_arrival(source_head, part, slot):
        return pltpu.make_async_remote_copy(
            src_ref=col_out.at[0, :, pl.ds(part * share, share)],
            dst_ref=landing(source_head, part, slot),
            send_sem=back_send.at[part, 0],
            recv_sem=back_recv.at[source_head * PARTS + part, slot],
            device_id=(me, other),
            device_id_type=MESH,
        )

    for part in range(PARTS):

        @pl.loop(1, n)
        def _(d):
            for t in range(3):
                col_arrival(t, part, d).wait_recv()

        @pl.loop(part * (share // HD), (part + 1) * (share // HD))
        def _(h):
            lanes = pl.ds(pl.multiple_of(h * HD, HD), HD)
            for start in range(0, cols, width):
                at = (slice(None), pl.ds(start, width), lanes)
                got = attend(*(ref[at].reshape(size, HD) for ref in cols_in), allowed)
                col_out[at] = got.reshape(n, width, HD)

        @pl.loop(1, n)
        def _(d):
            back_copy(part, lax.rem(me + d, n)).start()

        @pl.when(stays)
        def _():
            rows = pl.ds(pl.multiple_of(slot_here * cols, cols), cols)
            joined[head, rows, pl.ds(block + part * share, share)] = col_out[
                me, :, pl.ds(part * share, share)
            ]

        @pl.when(jnp.logical_not(stays))
        def _():
            back_copy(part, me).start()

        if part == 0:
            onward(SHARES // 2, SHARES)

    @pl.loop(0, SHARES)
    def _(s):
        index = index_of(member_beside, s)
        w_copy(w_other, index, 1, beside, head).wait_recv()
        w_copy(w_other, index, 3, sibling, head).start()

    row_copy.wait_recv()

    def back_wait(source_head):
        @pl.loop(0, n // 2)
        def _(slot):
            mine = (head * (n // 2) + slot == me) & (head == source_head)

            @pl.when(jnp.logical_not(mine))
            def _():
                for part in range(PARTS):
                    back_arrival(source_head, part, slot).wait_recv()

    back_wait(head)

    def own_col_part(lanes):
        summed[:, lanes] += jnp.dot(
            joined[head, :, pl.ds(block, block)],
            w_own[pl.ds(block, block), lanes],
            preferred_element_type=jnp.float32,
        )

    tiles(own_col_part)

    @pl.loop(0, SHARES)
    def _(s):
        w_copy(w_other, index_of(member_sibling, s), 2, sibling, head).wait_recv()
        w_copy(w_other, index_of(member_far, s), 3, sibling, head).wait_recv()

    back_wait(other)

    def other_part(lanes):
        total = summed[:, lanes] + jnp.dot(
            joined[other], w_other[:, lanes], preferred_element_type=jnp.float32
        )
        out_ref[:, lanes] = total.astype(jnp.bfloat16)

    tiles(other_part)

    for part in range(PARTS):

        @pl.loop(1, n)
        def _(d):
            for t in range(3):
                col_copy(t, part, d).wait_send()

    @pl.loop(0, SHARES)
    def _(s):
        w_copy(w_hbm, index_of(member, s), 0, me, other).wait_send()
        w_copy(w_other, index_of(member, s), 2, sibling, head).wait_send()
        w_copy(w_other, index_of(member_beside, s), 3, sibling, head).wait_send()

    @pl.loop(0, SHARES - STRAIGHT)
    def _(s):
        w_copy(w_other, index_of(member, s), 1, beside, head).wait_send()

    @pl.loop(SHARES - STRAIGHT, SHARES)
    def _(s):
        w_copy(w_hbm, index_of(member_beside, s), 0, me, other).wait_send()

    row_copy.wait_send()

    for part in range(PARTS):

        @pl.loop(1, n)
        def _(d):
            back_copy(part, lax.rem(me + d, n)).wait_send()

        @pl.when(jnp.logical_not(stays))
        def _():
            back_copy(part, me).wait_send()


def on_device(n, queries, keys, values, w_out):
    _, stride, local_feat = queries.shape
    depth, model_width = w_out.shape
    block = GROUP * HD
    assert queries.shape[0] == 1 and local_feat == 2 * block
    half = stride // lax.axis_size("head")
    cols = stride // n
    if n == LAYER * LAYER and stride % (LAYER * CHUNKS * WIDTH) == 0:
        out = call_layered(n, queries, keys, values, w_out, half)
        return out.reshape((1, half, model_width))
    bf16 = jnp.bfloat16
    dma = pltpu.SemaphoreType.DMA
    out = pl.pallas_call(
        functools.partial(body, n),
        out_shape=jax.ShapeDtypeStruct((half, model_width), bf16),
        in_specs=[pl.BlockSpec(memory_space=pltpu.HBM)] * 4,
        out_specs=pl.BlockSpec(memory_space=pltpu.VMEM),
        scratch_shapes=[pltpu.VMEM((stride, block), bf16)] * 3
        + [pltpu.VMEM((n, cols, block), bf16)] * 4
        + [
            pltpu.VMEM((stride, block), bf16),
            pltpu.VMEM((2, half, local_feat), bf16),
            pltpu.VMEM((half, model_width), jnp.float32),
            pltpu.VMEM((depth, model_width), bf16),
            pltpu.VMEM((depth, model_width), bf16),
            dma((7,)),
            dma((3 * PARTS, n)),
            dma((3 * PARTS, n)),
            dma((PARTS, n)),
            dma((2 * PARTS, n // 2)),
            dma((4, 4 * SHARES)),
            dma((4 * SHARES,)),
            dma,
            dma,
        ],
        compiler_params=pltpu.CompilerParams(has_side_effects=True, vmem_limit_bytes=60 * 2**20),
    )(queries, keys, values, w_out)
    return out.reshape((1, half, model_width))


def solution(mesh):
    return jax.shard_map(
        functools.partial(on_device, mesh.shape["ctx"]),
        mesh=mesh,
        in_specs=(
            P("ctx", None, "head"),
            P("ctx", None, "head"),
            P("ctx", None, "head"),
            P("head", None),
        ),
        out_specs=P("ctx", "head", None),
        check_vma=False,
    )
```

```python
import functools

import jax
import jax.numpy as jnp
from jax import lax
from jax.experimental import pallas as pl
from jax.experimental.pallas import tpu as pltpu
from jax.sharding import PartitionSpec as P

HD = 128
GROUP = 4
MESH = pl.DeviceIdType.MESH
SHARES = 8
STRAIGHT = 2
PARTS = 2
LAYER = 4
CHUNKS = 8
WIDTH = 16
WIDTH_LOG = 4
PIECES = 4
AHEAD = 3

masked_score = -1e30


def attend(query, key, value, allowed):
    scores = lax.dot_general(
        query, key, (((1,), (1,)), ((), ())), preferred_element_type=jnp.float32
    ) * jnp.float32(1.0 / HD**0.5)
    scores = jnp.where(allowed, scores, masked_score)
    top = jnp.max(scores, axis=-1, keepdims=True)
    expo = jnp.exp(scores - top)
    total = jnp.sum(expo, axis=-1, keepdims=True)
    mixed = jnp.dot(expo.astype(jnp.bfloat16), value, preferred_element_type=jnp.float32)
    return (mixed / total).astype(jnp.bfloat16)


def weigh(queries, keys, values, allowed):
    scores = [
        lax.dot_general(q, k, (((1,), (1,)), ((), ())), preferred_element_type=jnp.float32)
        for q, k in zip(queries, keys)
    ]
    scores = [jnp.where(allowed, s * jnp.float32(1.0 / HD**0.5), masked_score) for s in scores]
    tops = [jnp.max(s, axis=-1, keepdims=True) for s in scores]
    expos = [jnp.exp(s - top) for s, top in zip(scores, tops)]
    totals = [jnp.sum(e, axis=-1, keepdims=True) for e in expos]
    mixed = [
        jnp.dot(e.astype(jnp.bfloat16), v, preferred_element_type=jnp.float32)
        for e, v in zip(expos, values)
    ]
    return [
        ((m / total).astype(jnp.bfloat16), top + jnp.log(total))
        for m, total, top in zip(mixed, totals, tops)
    ]


def layered(
    n, q_hbm, k_hbm, v_hbm, w_hbm, staged, q_row, k_row, v_row, q_in, k_in, v_in, o_out, p_in,
    stats, stats_in, row_out, joined, summed, w_own, w_other,
    local_sem, chunk_sem, lay_send, lay_recv, up_send, up_recv, part_send, part_recv,
    back_send, back_recv, w_send, w_recv, row_send, row_recv,
):
    me, head = lax.axis_index("ctx"), lax.axis_index("head")
    other = 1 - head
    z, s = lax.div(me, LAYER), lax.rem(me, LAYER)
    core = lax.rem(s, 2)
    sib = s + 1 - 2 * core
    opp = s + 2 - 4 * lax.div(s, 2)
    far = sib + 2 - 4 * lax.div(sib, 2)
    peers = (s, sib, opp, far)
    stride = q_hbm.shape[1]
    block = q_row.shape[1]
    depth = w_own.shape[0]
    half = joined.shape[1]
    cols = stride // LAYER
    cw = cols // CHUNKS
    hbm = (q_hbm, k_hbm, v_hbm)
    ins = (q_in, k_in, v_in)
    own_at = (0, LAYER, LAYER)
    feats = pl.ds(block, block)

    def place(j, slot):
        return slot * (cols // 2) + lax.div(j, 2) * cw

    def chunk_of(j, slot):
        return pl.ds(pl.multiple_of(lax.rem(j, 2) * half + place(j, slot), cw), cw)

    def remote(src, dst, send, recv, ctx, at):
        return pltpu.make_async_remote_copy(
            src_ref=src, dst_ref=dst, send_sem=send, recv_sem=recv,
            device_id=(ctx, at), device_id_type=MESH,
        )

    def here(slot):
        return z * LAYER + slot

    def lay(t, j, d, source):
        row = peers[d] if source else s
        return remote(
            hbm[t].at[0, chunk_of(j, peers[d]), feats],
            ins[t].at[own_at[t] + row, pl.ds(j * cw, cw)],
            lay_send.at[t * CHUNKS + j, d], lay_recv.at[t * CHUNKS + j, d],
            here(peers[d]), head,
        )

    def up(kind, t, j, d, layer, base):
        if d < 2:
            src, slot, row = hbm[t].at[0, chunk_of(j, peers[d]), feats], peers[d], s
        else:
            src, slot, row = ins[t].at[own_at[t] + peers[d], pl.ds(j * cw, cw)], s, peers[d]
        return remote(
            src, ins[t].at[base + row, pl.ds(j * cw, cw)],
            up_send.at[kind * CHUNKS + j, d], up_recv.at[kind * CHUNKS + j, d],
            layer * LAYER + slot, head,
        )

    def up_arrival(kind, t, j, d, base):
        return remote(
            hbm[t].at[0, pl.ds(0, cw), feats], ins[t].at[base + peers[d], pl.ds(j * cw, cw)],
            up_send.at[kind * CHUNKS + j, d], up_recv.at[kind * CHUNKS + j, d],
            here(sib), head,
        )

    routes = {
        0: ((0, 1, 1, 0), (1, 2, 1, 0)),
        2: ((2, 0, 1, LAYER),),
        3: ((2, 0, 2, LAYER),),
    }

    def onward(j):
        at = pl.ds(j * cw, cw)
        return remote(
            q_in.at[pl.ds(LAYER, LAYER), at], q_in.at[pl.ds(2 * LAYER, LAYER), at],
            up_send.at[3 * CHUNKS + j, 0], up_recv.at[3 * CHUNKS + j, 0], LAYER + s, head,
        )

    def pass_on(j):
        for d in range(4):
            up_arrival(2, 0, j, d, LAYER).wait_recv()
        onward(j).start()

    def direct(layer, j):
        for kind, t, to, base in routes[layer]:
            for d in (0, 1):
                up(kind, t, j, d, to, base).start()

    def relay(layer, j):
        for t in sorted({t for _, t, _, _ in routes[layer]}):
            for d in (2, 3):
                lay(t, j, d, True).wait_recv()
                for kind, t2, to, base in routes[layer]:
                    if t2 == t:
                        up(kind, t, j, d, to, base).start()

    def piece_rows(q, c, k):
        eighth = depth // 16
        rows = eighth // (PIECES // 2)
        start = lax.div(k, PIECES // 2) * (depth // 2)
        start += (q * 2 + c) * eighth + lax.rem(k, PIECES // 2) * rows
        return pl.ds(start, rows)

    def w_copy(source, q, c, k, way, to_ctx, to_head):
        rows = piece_rows(q, c, k)
        index = (q * 2 + c) * PIECES + k
        return remote(
            source.at[rows], w_other.at[rows], w_send.at[way, index], w_recv.at[index], to_ctx, to_head
        )

    even = lax.rem(z + lax.div(s, 2), 2)
    y_next = here(opp)
    z_next = me + LAYER - 2 * LAYER * lax.rem(z, 2)
    z_early = (z == 1) | (z == 2)

    def to_side(k):
        return (z > 0) | (k < PIECES // 2)

    def w_first(q, k):
        return w_copy(w_hbm, 2 * even + q, core, k, 0, me, other)

    def w_side(q, k):
        return w_copy(w_other, 2 * even + q, core, k, 2, y_next if q == 0 else z_next, head)

    def w_extra(k):
        return w_copy(w_other, 2 * even + 1, core, k, 3, me - LAYER, head)

    def w_beside(q, k):
        return w_copy(w_other, 2 * (1 - even) + q, core, k, 1, here(sib), head)

    def w_here(q, k):
        return w_copy(w_other, 2 * even + q, core, k, 1, here(sib), head)

    def w_in(q, k):
        w_first(q, k).wait_recv()
        w_here(q, k).start()
        if q == 0:
            w_side(q, k).start()
        else:

            @pl.when(z_early)
            def _():
                w_side(q, k).start()

            @pl.when((z == 2) & (k >= PIECES // 2))
            def _():
                w_extra(k).start()

    def w_step(i):
        high = z >= 2
        for_z = jnp.where(high, jnp.where(i < PIECES, 1, 0), lax.rem(i, 2))
        k = jnp.where(high, lax.rem(i, PIECES), lax.div(i, 2))

        @pl.when(for_z == 1)
        def _():
            w_in(1, k)

        @pl.when(for_z == 0)
        def _():
            w_in(0, k)

    def w_on(q, k):
        w_copy(w_other, 2 * (1 - even) + q, core, k, 2, me, other).wait_recv()
        w_beside(q, k).start()

    ready = pltpu.get_barrier_semaphore()

    def greet(ctx, at):
        pl.semaphore_signal(ready, 1, device_id=(ctx, at), device_id_type=MESH)

    greet(me, other)
    for d in (1, 2, 3):
        greet(here(peers[d]), head)
        greet(here(peers[d]), other)
    for edge, towards in ((0, -LAYER), (LAYER - 1, LAYER)):

        @pl.when(z != edge)
        def _():
            greet(here(s) + towards, head)
            greet(here(sib) + towards, head)

    local = [
        pltpu.make_async_copy(hbm[t].at[0, :, pl.ds(0, block)], (q_row, k_row, v_row)[t], local_sem.at[t])
        for t in range(3)
    ]
    local += [
        pltpu.make_async_copy(
            hbm[t].at[0, chunk_of(j, s), feats],
            ins[t].at[own_at[t] + s, pl.ds(j * cw, cw)],
            chunk_sem.at[t, j],
        )
        for t in range(3)
        for j in range(CHUNKS)
    ]
    local.append(pltpu.make_async_copy(w_hbm, w_own, local_sem.at[3]))
    for copy in local:
        copy.start()

    inner = jnp.minimum(z, 1) + jnp.minimum(LAYER - 1 - z, 1)
    pl.semaphore_wait(ready, 2 * LAYER - 1 + 2 * inner)

    def exchange(ts):
        @pl.loop(0, CHUNKS)
        def _(j):
            for t in ts:
                for d in (2, 3, 1):
                    lay(t, j, d, False).start()

    for layer in routes:

        @pl.when(z == layer)
        def _():
            for j in range(AHEAD):
                direct(layer, j)

    @pl.when(z < 2)
    def _():
        exchange((1, 2))
        exchange((0,))

    @pl.when(z >= 2)
    def _():
        exchange((0,))
        exchange((1, 2))

    @pl.when(z < 2)
    def _():
        @pl.loop(0, PIECES)
        def _(k):
            w_first(0, k).start()
            w_first(1, k).start()

    @pl.when(z >= 2)
    def _():
        for q in (1, 0):

            @pl.loop(0, PIECES)
            def _(k):
                w_first(q, k).start()

    for copy in local[:-1]:
        copy.wait()

    tile = min(256, half)
    row_index = lax.broadcasted_iota(jnp.int32, (tile, stride), 0)
    key_index = lax.broadcasted_iota(jnp.int32, (tile, stride), 1)

    def row_tile(h, start):
        lanes = pl.ds(pl.multiple_of(h * HD, HD), HD)
        end = start + tile
        row_out[pl.ds(start, tile), lanes] = attend(
            q_row[pl.ds(start, tile), lanes],
            k_row[pl.ds(0, end), lanes],
            v_row[pl.ds(0, end), lanes],
            key_index[:, :end] <= row_index[:, :end] + start,
        )

    def spread(sums):
        lane = lax.broadcasted_iota(jnp.int32, (HD, HD), 1)
        row = lax.broadcasted_iota(jnp.int32, (HD, HD), 0)
        return jnp.sum(jnp.where(lane == row, sums, 0.0), axis=0, keepdims=True)

    def laid(sums, off):
        lane = lax.broadcasted_iota(jnp.int32, (size, HD), 1)
        row = lax.broadcasted_iota(jnp.int32, (size, HD), 0)
        return jnp.sum(jnp.where(lane == row + off, sums, 0.0), axis=0, keepdims=True)

    def column(line, off, period):
        lane = lax.broadcasted_iota(jnp.int32, (size, HD), 1)
        row = lax.broadcasted_iota(jnp.int32, (size, HD), 0)
        at = off + (row & (WIDTH - 1)) + lax.shift_right_logical(row, WIDTH_LOG) * period
        return jnp.sum(jnp.where(lane == at, line, 0.0), axis=1, keepdims=True)

    heads = block // HD
    size = LAYER * WIDTH

    def small(q_at, q_rows, k_at, k_rows, c, b, width, causal, keep):
        start = pl.multiple_of(c * cw + b * width, width)
        shape = (q_rows * width, k_rows * width)
        r = lax.broadcasted_iota(jnp.int32, shape, 0)
        m = lax.broadcasted_iota(jnp.int32, shape, 1)
        allowed = ((r - m) & (width - 1)) == 0
        if causal is not None:
            allowed &= m <= r + causal * width
        slices = []
        for h in range(heads):
            lanes = pl.ds(h * HD, HD)
            slices.append(
                (
                    (pl.ds(q_at, q_rows), pl.ds(start, width), lanes),
                    (pl.ds(k_at, k_rows), pl.ds(start, width), lanes),
                )
            )
        found = weigh(
            [q_in[at].reshape(shape[0], HD) for at, _ in slices],
            [k_in[at].reshape(shape[1], HD) for _, at in slices],
            [v_in[at].reshape(shape[1], HD) for _, at in slices],
            allowed,
        )
        for h, (got, sums) in enumerate(found):
            o_out[slices[h][0]] = got.reshape(q_rows, width, HD)
            if keep:
                stats[c * strips + b, pl.ds(h, 1)] = spread(sums)

    strips = cw // WIDTH

    def partial(j, rows, layer):
        return remote(
            o_out.at[pl.ds(LAYER, rows), pl.ds(j * cw, cw)], p_in.at[pl.ds(0, rows), pl.ds(j * cw, cw)],
            part_send.at[0, j], part_recv.at[0, j], layer * LAYER + s, head,
        )

    def partial_stats(j, layer):
        at = pl.ds(j * strips, strips)
        return remote(
            stats.at[at], stats_in.at[at], part_send.at[1, j], part_recv.at[1, j], layer * LAYER + s, head
        )

    def back(j, d):
        return remote(
            o_out.at[peers[d], pl.ds(j * cw, cw)],
            joined.at[head, pl.ds(place(j, s), cw), feats],
            back_send.at[j, d], back_recv.at[head * LAYER + s, lax.div(j, 2)],
            here(peers[d]), lax.rem(j, 2),
        )

    def stays(j):
        return lax.rem(j, 2) == head

    def back_all(j):
        for d in (2, 3, 1):
            back(j, d).start()

        @pl.when(jnp.logical_not(stays(j)))
        def _():
            back(j, 0).start()

        @pl.when(stays(j))
        def _():
            joined[head, pl.ds(pl.multiple_of(place(j, s), cw), cw), feats] = o_out[
                s, pl.ds(pl.multiple_of(j * cw, cw), cw)
            ]

    def ext(j):
        for t in (1, 2):
            for d in (1, 2, 3):
                lay(t, j, d, True).wait_recv()
        for kind, t, base in ((0, 1, 0), (1, 2, 0), (2, 0, LAYER)):
            for d in range(4):
                up_arrival(kind, t, j, d, base).wait_recv()
        onward(j).wait_recv()
        for b in range(strips):
            small(LAYER, 2 * LAYER, 0, 2 * LAYER, j, b, WIDTH, None, True)
        partial(j, 2 * LAYER, 2).start()
        partial_stats(j, 2).start()

    def own(c):
        @pl.when(z == 0)
        def _():
            for t, ds in ((0, (1, 2, 3)), (1, (1,)), (2, (1,))):
                for d in ds:
                    lay(t, c, d, True).wait_recv()
            small(0, LAYER, LAYER, LAYER, c, 0, cw, 0, False)
            back_all(c)

        @pl.when(z == 1)
        def _():
            for d in (1, 2, 3):
                lay(0, c, d, True).wait_recv()
            small(0, LAYER, 0, 2 * LAYER, c, 0, cw, LAYER, False)
            back_all(c)

        @pl.when(z >= 2)
        def _():
            lay(0, c, 1, True).wait_recv()
            for t in (1, 2):
                for d in (1, 2, 3):
                    lay(t, c, d, True).wait_recv()

        @pl.when(z == 2)
        def _():
            for b in range(strips):
                small(0, 2 * LAYER, LAYER, LAYER, c, b, WIDTH, 0, True)

        @pl.when(z == 3)
        def _():
            small(0, LAYER, LAYER, LAYER, c, 0, cw, 0, True)

    def combine(c):
        def mix(b, base, parts, keep):
            start = pl.multiple_of(c * cw + b * WIDTH, WIDTH)
            rows = pl.ds(start, WIDTH)
            strip = c * strips + b
            for h in range(heads):
                lanes = pl.ds(h * HD, HD)
                lines = [column(ref[at, pl.ds(row + h, 1)], off, period) for _, _, ref, at, row, off, period in parts]
                top = functools.reduce(jnp.maximum, lines)
                terms = [jnp.exp(line - top) for line in lines]
                total = functools.reduce(jnp.add, terms)
                got = 0.0
                for (source, first, *_), term in zip(parts, terms):
                    value = source[pl.ds(first, LAYER), rows, lanes].reshape(size, HD)
                    got += value.astype(jnp.float32) * (term / total)
                o_out[pl.ds(base, LAYER), rows, lanes] = got.astype(jnp.bfloat16).reshape(LAYER, WIDTH, HD)
                if keep:
                    stats[strip, pl.ds(heads + h, 1)] = laid(top + jnp.log(total), size)

        @pl.when(z == 2)
        def _():
            partial(c, 2 * LAYER, 2).wait_recv()
            partial_stats(c, 2).wait_recv()
            for first in (LAYER, 0):
                off = size if first else 0
                for b in range(strips):
                    strip = c * strips + b
                    mix(
                        b,
                        first,
                        [
                            (o_out, first, stats, strip, 0, off, WIDTH),
                            (p_in, first, stats_in, strip, 0, off, WIDTH),
                        ],
                        first > 0,
                    )
                if first:
                    partial(c, LAYER, 3).start()
                    partial_stats(c, 3).start()

        @pl.when(z == 3)
        def _():
            partial(c, LAYER, 3).wait_recv()
            partial_stats(c, 3).wait_recv()
            for b in range(strips):
                strip = c * strips + b
                mix(
                    b,
                    0,
                    [
                        (o_out, 0, stats, c * strips, 0, b * WIDTH, cw),
                        (p_in, 0, stats_in, strip, heads, size, WIDTH),
                    ],
                    False,
                )

        back_all(c)

    row_copy = remote(
        row_out.at[pl.ds(pl.multiple_of(other * half, half), half)],
        joined.at[head, :, pl.ds(0, block)], row_send, row_recv, me, other,
    )
    step = 512
    count = w_own.shape[1] // step

    def tiles(add):
        @pl.loop(0, count)
        def _(c):
            add(pl.ds(pl.multiple_of(c * step, step), step))

    def own_row_part(lanes):
        summed[:, lanes] = jnp.dot(
            joined[head, :, pl.ds(0, block)],
            w_own[pl.ds(0, block), lanes],
            preferred_element_type=jnp.float32,
        )

    @pl.loop(0, CHUNKS)
    def _(j):
        @pl.when(j < heads)
        def _():
            for start in range(0, stride, tile):
                row_tile(j, start)

        @pl.when(j == heads - 1)
        def _():
            row_copy.start()
            joined[head, :, pl.ds(0, block)] = row_out[pl.ds(pl.multiple_of(head * half, half), half)]

        for layer in routes:

            @pl.when((z == layer) & (j < CHUNKS // 2))
            def _():
                @pl.loop(2 * j, 2 * j + 2)
                def _(c):
                    relay(layer, c)
                    if layer == 2:
                        pass_on(c)

                    @pl.when(c + AHEAD < CHUNKS)
                    def _():
                        direct(layer, c + AHEAD)

        @pl.when(z == 1)
        def _():
            ext(j)

        @pl.when(j == heads)
        def _():
            local[-1].wait()
            tiles(own_row_part)

        i = j - jnp.where(z == 1, 0, 1)

        @pl.when(i >= 0)
        def _():
            w_step(i)

        @pl.when(jnp.logical_not(z_early) & (j == PIECES))
        def _():
            @pl.loop(0, PIECES)
            def _(k):
                @pl.when(to_side(k))
                def _():
                    w_side(1, k).start()

        @pl.when(j >= CHUNKS // 2)
        def _():
            c = 2 * j - CHUNKS
            own(c)
            own(c + 1)

            lag = z - 2

            @pl.when((z >= 2) & (j >= CHUNKS // 2 + lag))
            def _():
                combine(j - CHUNKS // 2 - lag)

    @pl.when(z != 1)
    def _():
        w_step(2 * PIECES - 1)

    def combine_some(layer, first, last):
        @pl.when(z == layer)
        def _():
            @pl.loop(first, last)
            def _(c):
                combine(c)

    def w_on_some(q, first, last):
        @pl.loop(first, last)
        def _(k):
            w_on(q, k)

    def w_from_sibling(qs, first, last):
        @pl.loop(first, last)
        def _(k):
            for q in qs:
                w_copy(w_other, q, 1 - core, k, 1, here(sib), head).wait_recv()

    def other_row_part(lanes):
        summed[:, lanes] += jnp.dot(
            joined[other, :, pl.ds(0, block)],
            w_other[pl.ds(0, block), lanes],
            preferred_element_type=jnp.float32,
        )

    def back_wait(u):
        for source_head in (head, other):
            for slot in range(LAYER):

                @pl.when(jnp.logical_not((slot == s) & (head == source_head)))
                def _():
                    for i in range(u * CHUNKS // 4, (u + 1) * CHUNKS // 4):
                        remote(
                            o_out.at[0, pl.ds(0, cw)],
                            joined.at[source_head, pl.ds(place(2 * i, slot), cw), feats],
                            back_send.at[i, 0], back_recv.at[source_head * LAYER + slot, i],
                            me, other,
                        ).wait_recv()

    run = CHUNKS // 4 * cw

    def finish(u):
        rows = [pl.ds(slot * (cols // 2) + u * run, run) for slot in range(LAYER)]

        @pl.loop(0, count)
        def _(c):
            lanes = pl.ds(pl.multiple_of(c * step, step), step)
            total = jnp.dot(
                jnp.concatenate([joined[head, at, feats] for at in rows]),
                w_own[feats, lanes],
                preferred_element_type=jnp.float32,
            )
            total += jnp.dot(
                jnp.concatenate([joined[other, at, feats] for at in rows]),
                w_other[feats, lanes],
                preferred_element_type=jnp.float32,
            )
            for slot, at in enumerate(rows):
                part = summed[at, lanes] + total[slot * run : (slot + 1) * run]
                staged[slot, u, :, lanes] = part.astype(jnp.bfloat16)

    combine_some(2, CHUNKS // 2, CHUNKS)
    combine_some(3, CHUNKS // 2 - 1, CHUNKS - 3)
    w_on_some(0, 0, PIECES // 2)
    w_on_some(1, 0, PIECES // 2)
    combine_some(3, CHUNKS - 3, CHUNKS - 1)
    w_from_sibling((0, 1, 2, 3), 0, PIECES // 2)
    row_copy.wait_recv()
    tiles(other_row_part)
    combine_some(3, CHUNKS - 1, CHUNKS)
    w_on_some(0, PIECES // 2, PIECES)
    w_on_some(1, PIECES // 2, PIECES)
    w_from_sibling((0, 1, 2, 3), PIECES // 2, PIECES)
    back_wait(0)
    finish(0)
    back_wait(1)
    finish(1)

    @pl.loop(0, CHUNKS)
    def _(j):
        for t in range(3):
            for d in (1, 2, 3):
                lay(t, j, d, False).wait_send()
        for layer in routes:

            @pl.when(z == layer)
            def _():
                for kind, t, to, base in routes[layer]:
                    for d in range(4):
                        up(kind, t, j, d, to, base).wait_send()

        @pl.when(z == 1)
        def _():
            partial(j, 2 * LAYER, 2).wait_send()
            partial_stats(j, 2).wait_send()

        @pl.when(z == 2)
        def _():
            onward(j).wait_send()
            partial(j, LAYER, 3).wait_send()
            partial_stats(j, 3).wait_send()

        for d in (1, 2, 3):
            back(j, d).wait_send()

        @pl.when(jnp.logical_not(stays(j)))
        def _():
            back(j, 0).wait_send()

    @pl.loop(0, PIECES)
    def _(k):
        for q in (0, 1):
            w_first(q, k).wait_send()
            w_here(q, k).wait_send()
            w_beside(q, k).wait_send()
        w_side(0, k).wait_send()

        @pl.when(to_side(k))
        def _():
            w_side(1, k).wait_send()

        @pl.when((z == 2) & (k >= PIECES // 2))
        def _():
            w_extra(k).wait_send()

    row_copy.wait_send()


def call_layered(n, queries, keys, values, w_out, half):
    _, stride, local_feat = queries.shape
    depth, width = w_out.shape
    block = local_feat // 2
    cols = stride // LAYER
    bf16, f32 = jnp.bfloat16, jnp.float32
    dma = pltpu.SemaphoreType.DMA
    blocks = cols // WIDTH
    return pl.pallas_call(
        functools.partial(layered, n),
        out_shape=pltpu.VMEM((LAYER, 2, half // (2 * LAYER), width), bf16),
        in_specs=[pl.BlockSpec(memory_space=pltpu.HBM)] * 4,
        out_specs=pl.BlockSpec(memory_space=pltpu.VMEM),
        scratch_shapes=[pltpu.VMEM((stride, block), bf16)] * 3
        + [
            pltpu.VMEM((3 * LAYER, cols, block), bf16),
            pltpu.VMEM((2 * LAYER, cols, block), bf16),
            pltpu.VMEM((2 * LAYER, cols, block), bf16),
            pltpu.VMEM((3 * LAYER, cols, block), bf16),
            pltpu.VMEM((2 * LAYER, cols, block), bf16),
            pltpu.VMEM((blocks, 8, HD), f32),
            pltpu.VMEM((blocks, 8, HD), f32),
            pltpu.VMEM((stride, block), bf16),
            pltpu.VMEM((2, half, local_feat), bf16),
            pltpu.VMEM((half, width), f32),
            pltpu.VMEM((depth, width), bf16),
            pltpu.VMEM((depth, width), bf16),
            dma((4,)),
            dma((3, CHUNKS)),
            dma((3 * CHUNKS, LAYER)),
            dma((3 * CHUNKS, LAYER)),
            dma((4 * CHUNKS, LAYER)),
            dma((4 * CHUNKS, LAYER)),
            dma((2, CHUNKS)),
            dma((2, CHUNKS)),
            dma((CHUNKS, LAYER)),
            dma((2 * LAYER, CHUNKS // 2)),
            dma((4, 8 * PIECES)),
            dma((8 * PIECES,)),
            dma,
            dma,
        ],
        compiler_params=pltpu.CompilerParams(
            collective_id=0, has_side_effects=True, vmem_limit_bytes=56 * 2**20
        ),
    )(queries, keys, values, w_out)


def body(
    n, q_hbm, k_hbm, v_hbm, w_hbm, out_ref, q_row, k_row, v_row, q_col, k_col, v_col,
    col_out, row_out, joined, summed, w_own, w_other, local_sem, in_send, in_recv, back_send, back_recv,
    w_send, w_recv, row_send, row_recv,
):
    me, head = lax.axis_index("ctx"), lax.axis_index("head")
    other = 1 - head
    stride = q_hbm.shape[1]
    block = q_row.shape[1]
    depth = w_own.shape[0]
    half = joined.shape[1]
    cols = stride // n
    share = block // PARTS
    hbm = (q_hbm, k_hbm, v_hbm)
    rows_in = (q_row, k_row, v_row)
    cols_in = (q_col, k_col, v_col)
    back_head = lax.div(me * cols, half)
    member = lax.rem(me, 4)
    sibling = me + 1 - 2 * lax.rem(me, 2)
    beside = me + 2 - 4 * lax.div(member, 2)
    piece = depth // (4 * SHARES)

    def col_copy(t, part, d):
        peer = lax.rem(me + d, n)
        lanes = pl.ds(part * share, share)
        return pltpu.make_async_remote_copy(
            src_ref=hbm[t].at[0, pl.ds(peer * cols, cols), pl.ds(block + part * share, share)],
            dst_ref=cols_in[t].at[me, :, lanes],
            send_sem=in_send.at[t * PARTS + part, d],
            recv_sem=in_recv.at[t * PARTS + part, d],
            device_id=(peer, head),
            device_id_type=MESH,
        )

    def col_arrival(t, part, d):
        source = lax.rem(me + n - d, n)
        lanes = pl.ds(part * share, share)
        return pltpu.make_async_remote_copy(
            src_ref=hbm[t].at[0, pl.ds(0, cols), pl.ds(block + part * share, share)],
            dst_ref=cols_in[t].at[source, :, lanes],
            send_sem=in_send.at[t * PARTS + part, d],
            recv_sem=in_recv.at[t * PARTS + part, d],
            device_id=(source, head),
            device_id_type=MESH,
        )

    def w_copy(source, index, way, to_ctx, to_head):
        rows = pl.ds(index * piece, piece)
        return pltpu.make_async_remote_copy(
            src_ref=source.at[rows],
            dst_ref=w_other.at[rows],
            send_sem=w_send.at[way, index],
            recv_sem=w_recv.at[index],
            device_id=(to_ctx, to_head),
            device_id_type=MESH,
        )

    def index_of(who, s):
        return who * SHARES + s

    member_sibling = lax.rem(sibling, 4)
    member_beside = lax.rem(beside, 4)
    member_far = lax.rem(member + 2, 4) + 1 - 2 * lax.rem(member, 2)

    for part in range(PARTS):

        @pl.loop(1, n)
        def _(d):
            for t in range(3):
                col_copy(t, part, d).start()

    @pl.loop(0, SHARES)
    def _(s):
        w_copy(w_hbm, index_of(member, s), 0, me, other).start()

    @pl.loop(SHARES - STRAIGHT, SHARES)
    def _(s):
        w_copy(w_hbm, index_of(member_beside, s), 0, me, other).start()

    local = [
        pltpu.make_async_copy(hbm[t].at[0, :, pl.ds(0, block)], rows_in[t], local_sem.at[t])
        for t in range(3)
    ]
    local += [
        pltpu.make_async_copy(
            hbm[t].at[0, pl.ds(me * cols, cols), pl.ds(block, block)],
            cols_in[t].at[me],
            local_sem.at[3 + t],
        )
        for t in range(3)
    ]
    local.append(pltpu.make_async_copy(w_hbm, w_own, local_sem.at[3]))
    for copy in local:
        copy.start()
    for copy in local[:3]:
        copy.wait()

    tile = min(256, half)
    row_index = lax.broadcasted_iota(jnp.int32, (tile, stride), 0)
    key_index = lax.broadcasted_iota(jnp.int32, (tile, stride), 1)

    @pl.loop(0, block // HD)
    def _(h):
        lanes = pl.ds(pl.multiple_of(h * HD, HD), HD)
        for start in range(0, stride, tile):
            end = start + tile
            row_out[pl.ds(start, tile), lanes] = attend(
                q_row[pl.ds(start, tile), lanes],
                k_row[pl.ds(0, end), lanes],
                v_row[pl.ds(0, end), lanes],
                key_index[:, :end] <= row_index[:, :end] + start,
            )

    row_copy = pltpu.make_async_remote_copy(
        src_ref=row_out.at[pl.ds(pl.multiple_of(other * half, half), half)],
        dst_ref=joined.at[head, :, pl.ds(0, block)],
        send_sem=row_send,
        recv_sem=row_recv,
        device_id=(me, other),
        device_id_type=MESH,
    )
    row_copy.start()
    joined[head, :, pl.ds(0, block)] = row_out[pl.ds(pl.multiple_of(head * half, half), half)]

    def onward(first, last):
        @pl.loop(first, last)
        def _(s):
            index = index_of(member, s)
            w_copy(w_hbm, index, 0, me, other).wait_recv()

            @pl.when(s < SHARES - STRAIGHT)
            def _():
                w_copy(w_other, index, 1, beside, head).start()

            w_copy(w_other, index, 2, sibling, head).start()

    onward(0, SHARES // 2)

    for copy in local[3:]:
        copy.wait()

    step = 512

    def tiles(add):
        @pl.loop(0, out_ref.shape[1] // step)
        def _(c):
            add(pl.ds(pl.multiple_of(c * step, step), step))

    def own_row_part(lanes):
        summed[:, lanes] = jnp.dot(
            joined[head, :, pl.ds(0, block)],
            w_own[pl.ds(0, block), lanes],
            preferred_element_type=jnp.float32,
        )

    tiles(own_row_part)
    width = min(cols, max(16, 256 // n))
    size = n * width
    r_index = lax.broadcasted_iota(jnp.int32, (size, size), 0)
    s_index = lax.broadcasted_iota(jnp.int32, (size, size), 1)
    allowed = (s_index <= r_index) & (((r_index - s_index) & (width - 1)) == 0)

    slot_here = lax.rem(me, n // 2)
    stays = back_head == head

    def landing(source_head, part, slot):
        return joined.at[
            source_head,
            pl.ds(pl.multiple_of(slot * cols, cols), cols),
            pl.ds(block + part * share, share),
        ]

    def back_copy(part, r):
        return pltpu.make_async_remote_copy(
            src_ref=col_out.at[r, :, pl.ds(part * share, share)],
            dst_ref=landing(head, part, slot_here),
            send_sem=back_send.at[part, r],
            recv_sem=back_recv.at[head * PARTS + part, slot_here],
            device_id=(r, back_head),
            device_id_type=MESH,
        )

    def back_arrival(source_head, part, slot):
        return pltpu.make_async_remote_copy(
            src_ref=col_out.at[0, :, pl.ds(part * share, share)],
            dst_ref=landing(source_head, part, slot),
            send_sem=back_send.at[part, 0],
            recv_sem=back_recv.at[source_head * PARTS + part, slot],
            device_id=(me, other),
            device_id_type=MESH,
        )

    for part in range(PARTS):

        @pl.loop(1, n)
        def _(d):
            for t in range(3):
                col_arrival(t, part, d).wait_recv()

        @pl.loop(part * (share // HD), (part + 1) * (share // HD))
        def _(h):
            lanes = pl.ds(pl.multiple_of(h * HD, HD), HD)
            for start in range(0, cols, width):
                at = (slice(None), pl.ds(start, width), lanes)
                got = attend(*(ref[at].reshape(size, HD) for ref in cols_in), allowed)
                col_out[at] = got.reshape(n, width, HD)

        @pl.loop(1, n)
        def _(d):
            back_copy(part, lax.rem(me + d, n)).start()

        @pl.when(stays)
        def _():
            rows = pl.ds(pl.multiple_of(slot_here * cols, cols), cols)
            joined[head, rows, pl.ds(block + part * share, share)] = col_out[
                me, :, pl.ds(part * share, share)
            ]

        @pl.when(jnp.logical_not(stays))
        def _():
            back_copy(part, me).start()

        if part == 0:
            onward(SHARES // 2, SHARES)

    @pl.loop(0, SHARES)
    def _(s):
        index = index_of(member_beside, s)
        w_copy(w_other, index, 1, beside, head).wait_recv()
        w_copy(w_other, index, 3, sibling, head).start()

    row_copy.wait_recv()

    def back_wait(source_head):
        @pl.loop(0, n // 2)
        def _(slot):
            mine = (head * (n // 2) + slot == me) & (head == source_head)

            @pl.when(jnp.logical_not(mine))
            def _():
                for part in range(PARTS):
                    back_arrival(source_head, part, slot).wait_recv()

    back_wait(head)

    def own_col_part(lanes):
        summed[:, lanes] += jnp.dot(
            joined[head, :, pl.ds(block, block)],
            w_own[pl.ds(block, block), lanes],
            preferred_element_type=jnp.float32,
        )

    tiles(own_col_part)

    @pl.loop(0, SHARES)
    def _(s):
        w_copy(w_other, index_of(member_sibling, s), 2, sibling, head).wait_recv()
        w_copy(w_other, index_of(member_far, s), 3, sibling, head).wait_recv()

    back_wait(other)

    def other_part(lanes):
        total = summed[:, lanes] + jnp.dot(
            joined[other], w_other[:, lanes], preferred_element_type=jnp.float32
        )
        out_ref[:, lanes] = total.astype(jnp.bfloat16)

    tiles(other_part)

    for part in range(PARTS):

        @pl.loop(1, n)
        def _(d):
            for t in range(3):
                col_copy(t, part, d).wait_send()

    @pl.loop(0, SHARES)
    def _(s):
        w_copy(w_hbm, index_of(member, s), 0, me, other).wait_send()
        w_copy(w_other, index_of(member, s), 2, sibling, head).wait_send()
        w_copy(w_other, index_of(member_beside, s), 3, sibling, head).wait_send()

    @pl.loop(0, SHARES - STRAIGHT)
    def _(s):
        w_copy(w_other, index_of(member, s), 1, beside, head).wait_send()

    @pl.loop(SHARES - STRAIGHT, SHARES)
    def _(s):
        w_copy(w_hbm, index_of(member_beside, s), 0, me, other).wait_send()

    row_copy.wait_send()

    for part in range(PARTS):

        @pl.loop(1, n)
        def _(d):
            back_copy(part, lax.rem(me + d, n)).wait_send()

        @pl.when(jnp.logical_not(stays))
        def _():
            back_copy(part, me).wait_send()


def on_device(n, queries, keys, values, w_out):
    _, stride, local_feat = queries.shape
    depth, model_width = w_out.shape
    block = GROUP * HD
    assert queries.shape[0] == 1 and local_feat == 2 * block
    half = stride // lax.axis_size("head")
    cols = stride // n
    if n == LAYER * LAYER and stride % (LAYER * CHUNKS * WIDTH) == 0:
        out = call_layered(n, queries, keys, values, w_out, half)
        return out.reshape((1, half, model_width))
    bf16 = jnp.bfloat16
    dma = pltpu.SemaphoreType.DMA
    out = pl.pallas_call(
        functools.partial(body, n),
        out_shape=jax.ShapeDtypeStruct((half, model_width), bf16),
        in_specs=[pl.BlockSpec(memory_space=pltpu.HBM)] * 4,
        out_specs=pl.BlockSpec(memory_space=pltpu.VMEM),
        scratch_shapes=[pltpu.VMEM((stride, block), bf16)] * 3
        + [pltpu.VMEM((n, cols, block), bf16)] * 4
        + [
            pltpu.VMEM((stride, block), bf16),
            pltpu.VMEM((2, half, local_feat), bf16),
            pltpu.VMEM((half, model_width), jnp.float32),
            pltpu.VMEM((depth, model_width), bf16),
            pltpu.VMEM((depth, model_width), bf16),
            dma((7,)),
            dma((3 * PARTS, n)),
            dma((3 * PARTS, n)),
            dma((PARTS, n)),
            dma((2 * PARTS, n // 2)),
            dma((4, 4 * SHARES)),
            dma((4 * SHARES,)),
            dma,
            dma,
        ],
        compiler_params=pltpu.CompilerParams(has_side_effects=True, vmem_limit_bytes=60 * 2**20),
    )(queries, keys, values, w_out)
    return out.reshape((1, half, model_width))


def solution(mesh):
    return jax.shard_map(
        functools.partial(on_device, mesh.shape["ctx"]),
        mesh=mesh,
        in_specs=(
            P("ctx", None, "head"),
            P("ctx", None, "head"),
            P("ctx", None, "head"),
            P("head", None),
        ),
        out_specs=P("ctx", "head", None),
        check_vma=False,
    )
```

```python
import functools

import jax
import jax.numpy as jnp
from jax import lax
from jax.experimental import pallas as pl
from jax.experimental.pallas import tpu as pltpu
from jax.sharding import PartitionSpec as P

HD = 128
GROUP = 4
MESH = pl.DeviceIdType.MESH
SHARES = 8
STRAIGHT = 2
PARTS = 2
LAYER = 4
CHUNKS = 8
WIDTH = 16
WIDTH_LOG = 4
PIECES = 4
AHEAD = 3

masked_score = -1e30


def attend(query, key, value, allowed):
    scores = lax.dot_general(
        query, key, (((1,), (1,)), ((), ())), preferred_element_type=jnp.float32
    ) * jnp.float32(1.0 / HD**0.5)
    scores = jnp.where(allowed, scores, masked_score)
    top = jnp.max(scores, axis=-1, keepdims=True)
    expo = jnp.exp(scores - top)
    total = jnp.sum(expo, axis=-1, keepdims=True)
    mixed = jnp.dot(expo.astype(jnp.bfloat16), value, preferred_element_type=jnp.float32)
    return (mixed / total).astype(jnp.bfloat16)


def weigh(queries, keys, values, allowed):
    scores = [
        lax.dot_general(q, k, (((1,), (1,)), ((), ())), preferred_element_type=jnp.float32)
        for q, k in zip(queries, keys)
    ]
    scores = [jnp.where(allowed, s * jnp.float32(1.0 / HD**0.5), masked_score) for s in scores]
    tops = [jnp.max(s, axis=-1, keepdims=True) for s in scores]
    expos = [jnp.exp(s - top) for s, top in zip(scores, tops)]
    totals = [jnp.sum(e, axis=-1, keepdims=True) for e in expos]
    mixed = [
        jnp.dot(e.astype(jnp.bfloat16), v, preferred_element_type=jnp.float32)
        for e, v in zip(expos, values)
    ]
    return [
        ((m / total).astype(jnp.bfloat16), top + jnp.log(total))
        for m, total, top in zip(mixed, totals, tops)
    ]


def layered(
    n, q_hbm, k_hbm, v_hbm, w_hbm, staged, q_row, k_row, v_row, q_in, k_in, v_in, o_out, p_in,
    stats, stats_in, row_out, joined, summed, w_own, w_other,
    local_sem, chunk_sem, lay_send, lay_recv, up_send, up_recv, part_send, part_recv,
    back_send, back_recv, w_send, w_recv, row_send, row_recv,
):
    me, head = lax.axis_index("ctx"), lax.axis_index("head")
    other = 1 - head
    z, s = lax.div(me, LAYER), lax.rem(me, LAYER)
    core = lax.rem(s, 2)
    sib = s + 1 - 2 * core
    opp = s + 2 - 4 * lax.div(s, 2)
    far = sib + 2 - 4 * lax.div(sib, 2)
    peers = (s, sib, opp, far)
    stride = q_hbm.shape[1]
    block = q_row.shape[1]
    depth = w_own.shape[0]
    half = joined.shape[1]
    cols = stride // LAYER
    cw = cols // CHUNKS
    hbm = (q_hbm, k_hbm, v_hbm)
    ins = (q_in, k_in, v_in)
    own_at = (0, LAYER, LAYER)
    feats = pl.ds(block, block)

    def place(j, slot):
        return slot * (cols // 2) + lax.div(j, 2) * cw

    def chunk_of(j, slot):
        return pl.ds(pl.multiple_of(lax.rem(j, 2) * half + place(j, slot), cw), cw)

    def remote(src, dst, send, recv, ctx, at):
        return pltpu.make_async_remote_copy(
            src_ref=src, dst_ref=dst, send_sem=send, recv_sem=recv,
            device_id=(ctx, at), device_id_type=MESH,
        )

    def here(slot):
        return z * LAYER + slot

    def lay(t, j, d, source):
        row = peers[d] if source else s
        return remote(
            hbm[t].at[0, chunk_of(j, peers[d]), feats],
            ins[t].at[own_at[t] + row, pl.ds(j * cw, cw)],
            lay_send.at[t * CHUNKS + j, d], lay_recv.at[t * CHUNKS + j, d],
            here(peers[d]), head,
        )

    def up(kind, t, j, d, layer, base):
        if d < 2:
            src, slot, row = hbm[t].at[0, chunk_of(j, peers[d]), feats], peers[d], s
        else:
            src, slot, row = ins[t].at[own_at[t] + peers[d], pl.ds(j * cw, cw)], s, peers[d]
        return remote(
            src, ins[t].at[base + row, pl.ds(j * cw, cw)],
            up_send.at[kind * CHUNKS + j, d], up_recv.at[kind * CHUNKS + j, d],
            layer * LAYER + slot, head,
        )

    def up_arrival(kind, t, j, d, base):
        return remote(
            hbm[t].at[0, pl.ds(0, cw), feats], ins[t].at[base + peers[d], pl.ds(j * cw, cw)],
            up_send.at[kind * CHUNKS + j, d], up_recv.at[kind * CHUNKS + j, d],
            here(sib), head,
        )

    routes = {
        0: ((0, 1, 1, 0), (1, 2, 1, 0)),
        2: ((2, 0, 1, LAYER),),
        3: ((2, 0, 2, LAYER),),
    }

    def onward(j):
        at = pl.ds(j * cw, cw)
        return remote(
            q_in.at[pl.ds(LAYER, LAYER), at], q_in.at[pl.ds(2 * LAYER, LAYER), at],
            up_send.at[3 * CHUNKS + j, 0], up_recv.at[3 * CHUNKS + j, 0], LAYER + s, head,
        )

    def pass_on(j):
        for d in range(4):
            up_arrival(2, 0, j, d, LAYER).wait_recv()
        onward(j).start()

    def direct(layer, j):
        for kind, t, to, base in routes[layer]:
            for d in (0, 1):
                up(kind, t, j, d, to, base).start()

    def relay(layer, j):
        for t in sorted({t for _, t, _, _ in routes[layer]}):
            for d in (2, 3):
                lay(t, j, d, True).wait_recv()
                for kind, t2, to, base in routes[layer]:
                    if t2 == t:
                        up(kind, t, j, d, to, base).start()

    def piece_rows(q, c, k):
        eighth = depth // 16
        rows = eighth // (PIECES // 2)
        start = lax.div(k, PIECES // 2) * (depth // 2)
        start += (q * 2 + c) * eighth + lax.rem(k, PIECES // 2) * rows
        return pl.ds(start, rows)

    def w_copy(source, q, c, k, way, to_ctx, to_head):
        rows = piece_rows(q, c, k)
        index = (q * 2 + c) * PIECES + k
        return remote(
            source.at[rows], w_other.at[rows], w_send.at[way, index], w_recv.at[index], to_ctx, to_head
        )

    even = lax.rem(z + lax.div(s, 2), 2)
    y_next = here(opp)
    z_next = me + LAYER - 2 * LAYER * lax.rem(z, 2)
    z_early = (z == 1) | (z == 2)

    def to_side(k):
        return (z > 0) | (k < PIECES // 2)

    def w_first(q, k):
        return w_copy(w_hbm, 2 * even + q, core, k, 0, me, other)

    def w_side(q, k):
        return w_copy(w_other, 2 * even + q, core, k, 2, y_next if q == 0 else z_next, head)

    def w_extra(k):
        return w_copy(w_other, 2 * even + 1, core, k, 3, me - LAYER, head)

    def w_beside(q, k):
        return w_copy(w_other, 2 * (1 - even) + q, core, k, 1, here(sib), head)

    def w_here(q, k):
        return w_copy(w_other, 2 * even + q, core, k, 1, here(sib), head)

    def w_in(q, k):
        w_first(q, k).wait_recv()
        w_here(q, k).start()
        if q == 0:
            w_side(q, k).start()
        else:

            @pl.when(z_early)
            def _():
                w_side(q, k).start()

            @pl.when((z == 2) & (k >= PIECES // 2))
            def _():
                w_extra(k).start()

    def w_step(i):
        high = z >= 2
        for_z = jnp.where(high, jnp.where(i < PIECES, 1, 0), lax.rem(i, 2))
        k = jnp.where(high, lax.rem(i, PIECES), lax.div(i, 2))

        @pl.when(for_z == 1)
        def _():
            w_in(1, k)

        @pl.when(for_z == 0)
        def _():
            w_in(0, k)

    def w_on(q, k):
        w_copy(w_other, 2 * (1 - even) + q, core, k, 2, me, other).wait_recv()
        w_beside(q, k).start()

    ready = pltpu.get_barrier_semaphore()

    def greet(ctx, at):
        pl.semaphore_signal(ready, 1, device_id=(ctx, at), device_id_type=MESH)

    greet(me, other)
    for d in (1, 2, 3):
        greet(here(peers[d]), head)
        greet(here(peers[d]), other)
    for edge, towards in ((0, -LAYER), (LAYER - 1, LAYER)):

        @pl.when(z != edge)
        def _():
            greet(here(s) + towards, head)
            greet(here(sib) + towards, head)

    local = [
        pltpu.make_async_copy(hbm[t].at[0, :, pl.ds(0, block)], (q_row, k_row, v_row)[t], local_sem.at[t])
        for t in range(3)
    ]
    local += [
        pltpu.make_async_copy(
            hbm[t].at[0, chunk_of(j, s), feats],
            ins[t].at[own_at[t] + s, pl.ds(j * cw, cw)],
            chunk_sem.at[t, j],
        )
        for t in range(3)
        for j in range(CHUNKS)
    ]
    local.append(pltpu.make_async_copy(w_hbm, w_own, local_sem.at[3]))
    for copy in local:
        copy.start()

    inner = jnp.minimum(z, 1) + jnp.minimum(LAYER - 1 - z, 1)
    pl.semaphore_wait(ready, 2 * LAYER - 1 + 2 * inner)

    def exchange(ts):
        @pl.loop(0, CHUNKS)
        def _(j):
            for t in ts:
                for d in (2, 3, 1):
                    lay(t, j, d, False).start()

    for layer in routes:

        @pl.when(z == layer)
        def _():
            for j in range(AHEAD):
                direct(layer, j)

    @pl.when(z < 2)
    def _():
        exchange((1, 2))
        exchange((0,))

    @pl.when(z >= 2)
    def _():
        exchange((0,))
        exchange((1, 2))

    @pl.when(z < 2)
    def _():
        @pl.loop(0, PIECES)
        def _(k):
            w_first(0, k).start()
            w_first(1, k).start()

    @pl.when(z >= 2)
    def _():
        for q in (1, 0):

            @pl.loop(0, PIECES)
            def _(k):
                w_first(q, k).start()

    for copy in local[:-1]:
        copy.wait()

    tile = min(256, half)
    row_index = lax.broadcasted_iota(jnp.int32, (tile, stride), 0)
    key_index = lax.broadcasted_iota(jnp.int32, (tile, stride), 1)

    def row_tile(h, start):
        lanes = pl.ds(pl.multiple_of(h * HD, HD), HD)
        end = start + tile
        row_out[pl.ds(start, tile), lanes] = attend(
            q_row[pl.ds(start, tile), lanes],
            k_row[pl.ds(0, end), lanes],
            v_row[pl.ds(0, end), lanes],
            key_index[:, :end] <= row_index[:, :end] + start,
        )

    def spread(sums):
        lane = lax.broadcasted_iota(jnp.int32, (HD, HD), 1)
        row = lax.broadcasted_iota(jnp.int32, (HD, HD), 0)
        return jnp.sum(jnp.where(lane == row, sums, 0.0), axis=0, keepdims=True)

    def laid(sums, off):
        lane = lax.broadcasted_iota(jnp.int32, (size, HD), 1)
        row = lax.broadcasted_iota(jnp.int32, (size, HD), 0)
        return jnp.sum(jnp.where(lane == row + off, sums, 0.0), axis=0, keepdims=True)

    def column(line, off, period):
        lane = lax.broadcasted_iota(jnp.int32, (size, HD), 1)
        row = lax.broadcasted_iota(jnp.int32, (size, HD), 0)
        at = off + (row & (WIDTH - 1)) + lax.shift_right_logical(row, WIDTH_LOG) * period
        return jnp.sum(jnp.where(lane == at, line, 0.0), axis=1, keepdims=True)

    heads = block // HD
    size = LAYER * WIDTH

    def small(q_at, q_rows, k_at, k_rows, c, b, width, causal, keep):
        start = pl.multiple_of(c * cw + b * width, width)
        shape = (q_rows * width, k_rows * width)
        r = lax.broadcasted_iota(jnp.int32, shape, 0)
        m = lax.broadcasted_iota(jnp.int32, shape, 1)
        allowed = ((r - m) & (width - 1)) == 0
        if causal is not None:
            allowed &= m <= r + causal * width
        slices = []
        for h in range(heads):
            lanes = pl.ds(h * HD, HD)
            slices.append(
                (
                    (pl.ds(q_at, q_rows), pl.ds(start, width), lanes),
                    (pl.ds(k_at, k_rows), pl.ds(start, width), lanes),
                )
            )
        found = weigh(
            [q_in[at].reshape(shape[0], HD) for at, _ in slices],
            [k_in[at].reshape(shape[1], HD) for _, at in slices],
            [v_in[at].reshape(shape[1], HD) for _, at in slices],
            allowed,
        )
        for h, (got, sums) in enumerate(found):
            o_out[slices[h][0]] = got.reshape(q_rows, width, HD)
            if keep:
                stats[c * strips + b, pl.ds(h, 1)] = spread(sums)

    strips = cw // WIDTH

    def partial(j, rows, layer):
        return remote(
            o_out.at[pl.ds(LAYER, rows), pl.ds(j * cw, cw)], p_in.at[pl.ds(0, rows), pl.ds(j * cw, cw)],
            part_send.at[0, j], part_recv.at[0, j], layer * LAYER + s, head,
        )

    def partial_stats(j, layer):
        at = pl.ds(j * strips, strips)
        return remote(
            stats.at[at], stats_in.at[at], part_send.at[1, j], part_recv.at[1, j], layer * LAYER + s, head
        )

    def back(j, d):
        return remote(
            o_out.at[peers[d], pl.ds(j * cw, cw)],
            joined.at[head, pl.ds(place(j, s), cw), feats],
            back_send.at[j, d], back_recv.at[head * LAYER + s, lax.div(j, 2)],
            here(peers[d]), lax.rem(j, 2),
        )

    def stays(j):
        return lax.rem(j, 2) == head

    def back_all(j):
        for d in (2, 3, 1):
            back(j, d).start()

        @pl.when(jnp.logical_not(stays(j)))
        def _():
            back(j, 0).start()

        @pl.when(stays(j))
        def _():
            joined[head, pl.ds(pl.multiple_of(place(j, s), cw), cw), feats] = o_out[
                s, pl.ds(pl.multiple_of(j * cw, cw), cw)
            ]

    def ext(j):
        for t in (1, 2):
            for d in (1, 2, 3):
                lay(t, j, d, True).wait_recv()
        for kind, t, base in ((0, 1, 0), (1, 2, 0), (2, 0, LAYER)):
            for d in range(4):
                up_arrival(kind, t, j, d, base).wait_recv()
        onward(j).wait_recv()
        for b in range(strips):
            small(LAYER, 2 * LAYER, 0, 2 * LAYER, j, b, WIDTH, None, True)
        partial(j, 2 * LAYER, 2).start()
        partial_stats(j, 2).start()

    def own(c):
        @pl.when(z == 0)
        def _():
            for t, ds in ((0, (1, 2, 3)), (1, (1,)), (2, (1,))):
                for d in ds:
                    lay(t, c, d, True).wait_recv()
            small(0, LAYER, LAYER, LAYER, c, 0, cw, 0, False)
            back_all(c)

        @pl.when(z == 1)
        def _():
            for d in (1, 2, 3):
                lay(0, c, d, True).wait_recv()
            small(0, LAYER, 0, 2 * LAYER, c, 0, cw, LAYER, False)
            back_all(c)

        @pl.when(z >= 2)
        def _():
            lay(0, c, 1, True).wait_recv()
            for t in (1, 2):
                for d in (1, 2, 3):
                    lay(t, c, d, True).wait_recv()

        @pl.when(z == 2)
        def _():
            for b in range(strips):
                small(0, 2 * LAYER, LAYER, LAYER, c, b, WIDTH, 0, True)

        @pl.when(z == 3)
        def _():
            small(0, LAYER, LAYER, LAYER, c, 0, cw, 0, True)

    def combine(c):
        def mix(b, base, parts, keep):
            start = pl.multiple_of(c * cw + b * WIDTH, WIDTH)
            rows = pl.ds(start, WIDTH)
            strip = c * strips + b
            for h in range(heads):
                lanes = pl.ds(h * HD, HD)
                lines = [column(ref[at, pl.ds(row + h, 1)], off, period) for _, _, ref, at, row, off, period in parts]
                top = functools.reduce(jnp.maximum, lines)
                terms = [jnp.exp(line - top) for line in lines]
                total = functools.reduce(jnp.add, terms)
                got = 0.0
                for (source, first, *_), term in zip(parts, terms):
                    value = source[pl.ds(first, LAYER), rows, lanes].reshape(size, HD)
                    got += value.astype(jnp.float32) * (term / total)
                o_out[pl.ds(base, LAYER), rows, lanes] = got.astype(jnp.bfloat16).reshape(LAYER, WIDTH, HD)
                if keep:
                    stats[strip, pl.ds(heads + h, 1)] = laid(top + jnp.log(total), size)

        @pl.when(z == 2)
        def _():
            partial(c, 2 * LAYER, 2).wait_recv()
            partial_stats(c, 2).wait_recv()
            for first in (LAYER, 0):
                off = size if first else 0
                for b in range(strips):
                    strip = c * strips + b
                    mix(
                        b,
                        first,
                        [
                            (o_out, first, stats, strip, 0, off, WIDTH),
                            (p_in, first, stats_in, strip, 0, off, WIDTH),
                        ],
                        first > 0,
                    )
                if first:
                    partial(c, LAYER, 3).start()
                    partial_stats(c, 3).start()

        @pl.when(z == 3)
        def _():
            partial(c, LAYER, 3).wait_recv()
            partial_stats(c, 3).wait_recv()
            for b in range(strips):
                strip = c * strips + b
                mix(
                    b,
                    0,
                    [
                        (o_out, 0, stats, c * strips, 0, b * WIDTH, cw),
                        (p_in, 0, stats_in, strip, heads, size, WIDTH),
                    ],
                    False,
                )

        back_all(c)

    row_copy = remote(
        row_out.at[pl.ds(pl.multiple_of(other * half, half), half)],
        joined.at[head, :, pl.ds(0, block)], row_send, row_recv, me, other,
    )
    step = 2048
    count = w_own.shape[1] // step

    def tiles(add):
        @pl.loop(0, count)
        def _(c):
            add(pl.ds(pl.multiple_of(c * step, step), step))

    def own_row_part(lanes):
        summed[:, lanes] = jnp.dot(
            joined[head, :, pl.ds(0, block)],
            w_own[pl.ds(0, block), lanes],
            preferred_element_type=jnp.float32,
        )

    @pl.loop(0, CHUNKS)
    def _(j):
        @pl.when(j < heads)
        def _():
            for start in range(0, stride, tile):
                row_tile(j, start)

        @pl.when(j == heads - 1)
        def _():
            row_copy.start()
            joined[head, :, pl.ds(0, block)] = row_out[pl.ds(pl.multiple_of(head * half, half), half)]

        for layer in routes:

            @pl.when((z == layer) & (j < CHUNKS // 2))
            def _():
                @pl.loop(2 * j, 2 * j + 2)
                def _(c):
                    relay(layer, c)
                    if layer == 2:
                        pass_on(c)

                    @pl.when(c + AHEAD < CHUNKS)
                    def _():
                        direct(layer, c + AHEAD)

        @pl.when(z == 1)
        def _():
            ext(j)

        @pl.when(j == heads)
        def _():
            local[-1].wait()
            tiles(own_row_part)

        i = j - jnp.where(z == 1, 0, 1)

        @pl.when(i >= 0)
        def _():
            w_step(i)

        @pl.when(jnp.logical_not(z_early) & (j == PIECES))
        def _():
            @pl.loop(0, PIECES)
            def _(k):
                @pl.when(to_side(k))
                def _():
                    w_side(1, k).start()

        @pl.when(j >= CHUNKS // 2)
        def _():
            c = 2 * j - CHUNKS
            own(c)
            own(c + 1)

            lag = z - 2

            @pl.when((z >= 2) & (j >= CHUNKS // 2 + lag))
            def _():
                combine(j - CHUNKS // 2 - lag)

    @pl.when(z != 1)
    def _():
        w_step(2 * PIECES - 1)

    def combine_some(layer, first, last):
        @pl.when(z == layer)
        def _():
            @pl.loop(first, last)
            def _(c):
                combine(c)

    def w_on_some(q, first, last):
        @pl.loop(first, last)
        def _(k):
            w_on(q, k)

    def w_from_sibling(qs, first, last):
        @pl.loop(first, last)
        def _(k):
            for q in qs:
                w_copy(w_other, q, 1 - core, k, 1, here(sib), head).wait_recv()

    def other_row_part(lanes):
        summed[:, lanes] += jnp.dot(
            joined[other, :, pl.ds(0, block)],
            w_other[pl.ds(0, block), lanes],
            preferred_element_type=jnp.float32,
        )

    def back_wait(u):
        for source_head in (head, other):
            for slot in range(LAYER):

                @pl.when(jnp.logical_not((slot == s) & (head == source_head)))
                def _():
                    for i in range(u * CHUNKS // 4, (u + 1) * CHUNKS // 4):
                        remote(
                            o_out.at[0, pl.ds(0, cw)],
                            joined.at[source_head, pl.ds(place(2 * i, slot), cw), feats],
                            back_send.at[i, 0], back_recv.at[source_head * LAYER + slot, i],
                            me, other,
                        ).wait_recv()

    run = CHUNKS // 4 * cw

    def finish(u):
        rows = [pl.ds(slot * (cols // 2) + u * run, run) for slot in range(LAYER)]

        @pl.loop(0, count)
        def _(c):
            lanes = pl.ds(pl.multiple_of(c * step, step), step)
            total = jnp.dot(
                jnp.concatenate([joined[head, at, feats] for at in rows]),
                w_own[feats, lanes],
                preferred_element_type=jnp.float32,
            )
            total += jnp.dot(
                jnp.concatenate([joined[other, at, feats] for at in rows]),
                w_other[feats, lanes],
                preferred_element_type=jnp.float32,
            )
            for slot, at in enumerate(rows):
                part = summed[at, lanes] + total[slot * run : (slot + 1) * run]
                staged[slot, u, :, lanes] = part.astype(jnp.bfloat16)

    combine_some(2, CHUNKS // 2, CHUNKS)
    combine_some(3, CHUNKS // 2 - 1, CHUNKS - 3)
    w_on_some(0, 0, PIECES // 2)
    w_on_some(1, 0, PIECES // 2)
    combine_some(3, CHUNKS - 3, CHUNKS - 1)
    w_from_sibling((0, 1, 2, 3), 0, PIECES // 2)
    row_copy.wait_recv()
    tiles(other_row_part)
    combine_some(3, CHUNKS - 1, CHUNKS)
    w_on_some(0, PIECES // 2, PIECES)
    w_on_some(1, PIECES // 2, PIECES)
    w_from_sibling((0, 1, 2, 3), PIECES // 2, PIECES)
    back_wait(0)
    finish(0)
    back_wait(1)
    finish(1)

    @pl.loop(0, CHUNKS)
    def _(j):
        for t in range(3):
            for d in (1, 2, 3):
                lay(t, j, d, False).wait_send()
        for layer in routes:

            @pl.when(z == layer)
            def _():
                for kind, t, to, base in routes[layer]:
                    for d in range(4):
                        up(kind, t, j, d, to, base).wait_send()

        @pl.when(z == 1)
        def _():
            partial(j, 2 * LAYER, 2).wait_send()
            partial_stats(j, 2).wait_send()

        @pl.when(z == 2)
        def _():
            onward(j).wait_send()
            partial(j, LAYER, 3).wait_send()
            partial_stats(j, 3).wait_send()

        for d in (1, 2, 3):
            back(j, d).wait_send()

        @pl.when(jnp.logical_not(stays(j)))
        def _():
            back(j, 0).wait_send()

    @pl.loop(0, PIECES)
    def _(k):
        for q in (0, 1):
            w_first(q, k).wait_send()
            w_here(q, k).wait_send()
            w_beside(q, k).wait_send()
        w_side(0, k).wait_send()

        @pl.when(to_side(k))
        def _():
            w_side(1, k).wait_send()

        @pl.when((z == 2) & (k >= PIECES // 2))
        def _():
            w_extra(k).wait_send()

    row_copy.wait_send()


def call_layered(n, queries, keys, values, w_out, half):
    _, stride, local_feat = queries.shape
    depth, width = w_out.shape
    block = local_feat // 2
    cols = stride // LAYER
    bf16, f32 = jnp.bfloat16, jnp.float32
    dma = pltpu.SemaphoreType.DMA
    blocks = cols // WIDTH
    return pl.pallas_call(
        functools.partial(layered, n),
        out_shape=pltpu.VMEM((LAYER, 2, half // (2 * LAYER), width), bf16),
        in_specs=[pl.BlockSpec(memory_space=pltpu.HBM)] * 4,
        out_specs=pl.BlockSpec(memory_space=pltpu.VMEM),
        scratch_shapes=[pltpu.VMEM((stride, block), bf16)] * 3
        + [
            pltpu.VMEM((3 * LAYER, cols, block), bf16),
            pltpu.VMEM((2 * LAYER, cols, block), bf16),
            pltpu.VMEM((2 * LAYER, cols, block), bf16),
            pltpu.VMEM((3 * LAYER, cols, block), bf16),
            pltpu.VMEM((2 * LAYER, cols, block), bf16),
            pltpu.VMEM((blocks, 8, HD), f32),
            pltpu.VMEM((blocks, 8, HD), f32),
            pltpu.VMEM((stride, block), bf16),
            pltpu.VMEM((2, half, local_feat), bf16),
            pltpu.VMEM((half, width), f32),
            pltpu.VMEM((depth, width), bf16),
            pltpu.VMEM((depth, width), bf16),
            dma((4,)),
            dma((3, CHUNKS)),
            dma((3 * CHUNKS, LAYER)),
            dma((3 * CHUNKS, LAYER)),
            dma((4 * CHUNKS, LAYER)),
            dma((4 * CHUNKS, LAYER)),
            dma((2, CHUNKS)),
            dma((2, CHUNKS)),
            dma((CHUNKS, LAYER)),
            dma((2 * LAYER, CHUNKS // 2)),
            dma((4, 8 * PIECES)),
            dma((8 * PIECES,)),
            dma,
            dma,
        ],
        compiler_params=pltpu.CompilerParams(
            collective_id=0, has_side_effects=True, vmem_limit_bytes=56 * 2**20
        ),
    )(queries, keys, values, w_out)


def body(
    n, q_hbm, k_hbm, v_hbm, w_hbm, out_ref, q_row, k_row, v_row, q_col, k_col, v_col,
    col_out, row_out, joined, summed, w_own, w_other, local_sem, in_send, in_recv, back_send, back_recv,
    w_send, w_recv, row_send, row_recv,
):
    me, head = lax.axis_index("ctx"), lax.axis_index("head")
    other = 1 - head
    stride = q_hbm.shape[1]
    block = q_row.shape[1]
    depth = w_own.shape[0]
    half = joined.shape[1]
    cols = stride // n
    share = block // PARTS
    hbm = (q_hbm, k_hbm, v_hbm)
    rows_in = (q_row, k_row, v_row)
    cols_in = (q_col, k_col, v_col)
    back_head = lax.div(me * cols, half)
    member = lax.rem(me, 4)
    sibling = me + 1 - 2 * lax.rem(me, 2)
    beside = me + 2 - 4 * lax.div(member, 2)
    piece = depth // (4 * SHARES)

    def col_copy(t, part, d):
        peer = lax.rem(me + d, n)
        lanes = pl.ds(part * share, share)
        return pltpu.make_async_remote_copy(
            src_ref=hbm[t].at[0, pl.ds(peer * cols, cols), pl.ds(block + part * share, share)],
            dst_ref=cols_in[t].at[me, :, lanes],
            send_sem=in_send.at[t * PARTS + part, d],
            recv_sem=in_recv.at[t * PARTS + part, d],
            device_id=(peer, head),
            device_id_type=MESH,
        )

    def col_arrival(t, part, d):
        source = lax.rem(me + n - d, n)
        lanes = pl.ds(part * share, share)
        return pltpu.make_async_remote_copy(
            src_ref=hbm[t].at[0, pl.ds(0, cols), pl.ds(block + part * share, share)],
            dst_ref=cols_in[t].at[source, :, lanes],
            send_sem=in_send.at[t * PARTS + part, d],
            recv_sem=in_recv.at[t * PARTS + part, d],
            device_id=(source, head),
            device_id_type=MESH,
        )

    def w_copy(source, index, way, to_ctx, to_head):
        rows = pl.ds(index * piece, piece)
        return pltpu.make_async_remote_copy(
            src_ref=source.at[rows],
            dst_ref=w_other.at[rows],
            send_sem=w_send.at[way, index],
            recv_sem=w_recv.at[index],
            device_id=(to_ctx, to_head),
            device_id_type=MESH,
        )

    def index_of(who, s):
        return who * SHARES + s

    member_sibling = lax.rem(sibling, 4)
    member_beside = lax.rem(beside, 4)
    member_far = lax.rem(member + 2, 4) + 1 - 2 * lax.rem(member, 2)

    for part in range(PARTS):

        @pl.loop(1, n)
        def _(d):
            for t in range(3):
                col_copy(t, part, d).start()

    @pl.loop(0, SHARES)
    def _(s):
        w_copy(w_hbm, index_of(member, s), 0, me, other).start()

    @pl.loop(SHARES - STRAIGHT, SHARES)
    def _(s):
        w_copy(w_hbm, index_of(member_beside, s), 0, me, other).start()

    local = [
        pltpu.make_async_copy(hbm[t].at[0, :, pl.ds(0, block)], rows_in[t], local_sem.at[t])
        for t in range(3)
    ]
    local += [
        pltpu.make_async_copy(
            hbm[t].at[0, pl.ds(me * cols, cols), pl.ds(block, block)],
            cols_in[t].at[me],
            local_sem.at[3 + t],
        )
        for t in range(3)
    ]
    local.append(pltpu.make_async_copy(w_hbm, w_own, local_sem.at[3]))
    for copy in local:
        copy.start()
    for copy in local[:3]:
        copy.wait()

    tile = min(256, half)
    row_index = lax.broadcasted_iota(jnp.int32, (tile, stride), 0)
    key_index = lax.broadcasted_iota(jnp.int32, (tile, stride), 1)

    @pl.loop(0, block // HD)
    def _(h):
        lanes = pl.ds(pl.multiple_of(h * HD, HD), HD)
        for start in range(0, stride, tile):
            end = start + tile
            row_out[pl.ds(start, tile), lanes] = attend(
                q_row[pl.ds(start, tile), lanes],
                k_row[pl.ds(0, end), lanes],
                v_row[pl.ds(0, end), lanes],
                key_index[:, :end] <= row_index[:, :end] + start,
            )

    row_copy = pltpu.make_async_remote_copy(
        src_ref=row_out.at[pl.ds(pl.multiple_of(other * half, half), half)],
        dst_ref=joined.at[head, :, pl.ds(0, block)],
        send_sem=row_send,
        recv_sem=row_recv,
        device_id=(me, other),
        device_id_type=MESH,
    )
    row_copy.start()
    joined[head, :, pl.ds(0, block)] = row_out[pl.ds(pl.multiple_of(head * half, half), half)]

    def onward(first, last):
        @pl.loop(first, last)
        def _(s):
            index = index_of(member, s)
            w_copy(w_hbm, index, 0, me, other).wait_recv()

            @pl.when(s < SHARES - STRAIGHT)
            def _():
                w_copy(w_other, index, 1, beside, head).start()

            w_copy(w_other, index, 2, sibling, head).start()

    onward(0, SHARES // 2)

    for copy in local[3:]:
        copy.wait()

    step = 512

    def tiles(add):
        @pl.loop(0, out_ref.shape[1] // step)
        def _(c):
            add(pl.ds(pl.multiple_of(c * step, step), step))

    def own_row_part(lanes):
        summed[:, lanes] = jnp.dot(
            joined[head, :, pl.ds(0, block)],
            w_own[pl.ds(0, block), lanes],
            preferred_element_type=jnp.float32,
        )

    tiles(own_row_part)
    width = min(cols, max(16, 256 // n))
    size = n * width
    r_index = lax.broadcasted_iota(jnp.int32, (size, size), 0)
    s_index = lax.broadcasted_iota(jnp.int32, (size, size), 1)
    allowed = (s_index <= r_index) & (((r_index - s_index) & (width - 1)) == 0)

    slot_here = lax.rem(me, n // 2)
    stays = back_head == head

    def landing(source_head, part, slot):
        return joined.at[
            source_head,
            pl.ds(pl.multiple_of(slot * cols, cols), cols),
            pl.ds(block + part * share, share),
        ]

    def back_copy(part, r):
        return pltpu.make_async_remote_copy(
            src_ref=col_out.at[r, :, pl.ds(part * share, share)],
            dst_ref=landing(head, part, slot_here),
            send_sem=back_send.at[part, r],
            recv_sem=back_recv.at[head * PARTS + part, slot_here],
            device_id=(r, back_head),
            device_id_type=MESH,
        )

    def back_arrival(source_head, part, slot):
        return pltpu.make_async_remote_copy(
            src_ref=col_out.at[0, :, pl.ds(part * share, share)],
            dst_ref=landing(source_head, part, slot),
            send_sem=back_send.at[part, 0],
            recv_sem=back_recv.at[source_head * PARTS + part, slot],
            device_id=(me, other),
            device_id_type=MESH,
        )

    for part in range(PARTS):

        @pl.loop(1, n)
        def _(d):
            for t in range(3):
                col_arrival(t, part, d).wait_recv()

        @pl.loop(part * (share // HD), (part + 1) * (share // HD))
        def _(h):
            lanes = pl.ds(pl.multiple_of(h * HD, HD), HD)
            for start in range(0, cols, width):
                at = (slice(None), pl.ds(start, width), lanes)
                got = attend(*(ref[at].reshape(size, HD) for ref in cols_in), allowed)
                col_out[at] = got.reshape(n, width, HD)

        @pl.loop(1, n)
        def _(d):
            back_copy(part, lax.rem(me + d, n)).start()

        @pl.when(stays)
        def _():
            rows = pl.ds(pl.multiple_of(slot_here * cols, cols), cols)
            joined[head, rows, pl.ds(block + part * share, share)] = col_out[
                me, :, pl.ds(part * share, share)
            ]

        @pl.when(jnp.logical_not(stays))
        def _():
            back_copy(part, me).start()

        if part == 0:
            onward(SHARES // 2, SHARES)

    @pl.loop(0, SHARES)
    def _(s):
        index = index_of(member_beside, s)
        w_copy(w_other, index, 1, beside, head).wait_recv()
        w_copy(w_other, index, 3, sibling, head).start()

    row_copy.wait_recv()

    def back_wait(source_head):
        @pl.loop(0, n // 2)
        def _(slot):
            mine = (head * (n // 2) + slot == me) & (head == source_head)

            @pl.when(jnp.logical_not(mine))
            def _():
                for part in range(PARTS):
                    back_arrival(source_head, part, slot).wait_recv()

    back_wait(head)

    def own_col_part(lanes):
        summed[:, lanes] += jnp.dot(
            joined[head, :, pl.ds(block, block)],
            w_own[pl.ds(block, block), lanes],
            preferred_element_type=jnp.float32,
        )

    tiles(own_col_part)

    @pl.loop(0, SHARES)
    def _(s):
        w_copy(w_other, index_of(member_sibling, s), 2, sibling, head).wait_recv()
        w_copy(w_other, index_of(member_far, s), 3, sibling, head).wait_recv()

    back_wait(other)

    def other_part(lanes):
        total = summed[:, lanes] + jnp.dot(
            joined[other], w_other[:, lanes], preferred_element_type=jnp.float32
        )
        out_ref[:, lanes] = total.astype(jnp.bfloat16)

    tiles(other_part)

    for part in range(PARTS):

        @pl.loop(1, n)
        def _(d):
            for t in range(3):
                col_copy(t, part, d).wait_send()

    @pl.loop(0, SHARES)
    def _(s):
        w_copy(w_hbm, index_of(member, s), 0, me, other).wait_send()
        w_copy(w_other, index_of(member, s), 2, sibling, head).wait_send()
        w_copy(w_other, index_of(member_beside, s), 3, sibling, head).wait_send()

    @pl.loop(0, SHARES - STRAIGHT)
    def _(s):
        w_copy(w_other, index_of(member, s), 1, beside, head).wait_send()

    @pl.loop(SHARES - STRAIGHT, SHARES)
    def _(s):
        w_copy(w_hbm, index_of(member_beside, s), 0, me, other).wait_send()

    row_copy.wait_send()

    for part in range(PARTS):

        @pl.loop(1, n)
        def _(d):
            back_copy(part, lax.rem(me + d, n)).wait_send()

        @pl.when(jnp.logical_not(stays))
        def _():
            back_copy(part, me).wait_send()


def on_device(n, queries, keys, values, w_out):
    _, stride, local_feat = queries.shape
    depth, model_width = w_out.shape
    block = GROUP * HD
    assert queries.shape[0] == 1 and local_feat == 2 * block
    half = stride // lax.axis_size("head")
    cols = stride // n
    if n == LAYER * LAYER and stride % (LAYER * CHUNKS * WIDTH) == 0:
        out = call_layered(n, queries, keys, values, w_out, half)
        return out.reshape((1, half, model_width))
    bf16 = jnp.bfloat16
    dma = pltpu.SemaphoreType.DMA
    out = pl.pallas_call(
        functools.partial(body, n),
        out_shape=jax.ShapeDtypeStruct((half, model_width), bf16),
        in_specs=[pl.BlockSpec(memory_space=pltpu.HBM)] * 4,
        out_specs=pl.BlockSpec(memory_space=pltpu.VMEM),
        scratch_shapes=[pltpu.VMEM((stride, block), bf16)] * 3
        + [pltpu.VMEM((n, cols, block), bf16)] * 4
        + [
            pltpu.VMEM((stride, block), bf16),
            pltpu.VMEM((2, half, local_feat), bf16),
            pltpu.VMEM((half, model_width), jnp.float32),
            pltpu.VMEM((depth, model_width), bf16),
            pltpu.VMEM((depth, model_width), bf16),
            dma((7,)),
            dma((3 * PARTS, n)),
            dma((3 * PARTS, n)),
            dma((PARTS, n)),
            dma((2 * PARTS, n // 2)),
            dma((4, 4 * SHARES)),
            dma((4 * SHARES,)),
            dma,
            dma,
        ],
        compiler_params=pltpu.CompilerParams(has_side_effects=True, vmem_limit_bytes=60 * 2**20),
    )(queries, keys, values, w_out)
    return out.reshape((1, half, model_width))


def solution(mesh):
    return jax.shard_map(
        functools.partial(on_device, mesh.shape["ctx"]),
        mesh=mesh,
        in_specs=(
            P("ctx", None, "head"),
            P("ctx", None, "head"),
            P("ctx", None, "head"),
            P("head", None),
        ),
        out_specs=P("ctx", "head", None),
        check_vma=False,
    )
```

```python
import functools

import jax
import jax.numpy as jnp
from jax import lax
from jax.experimental import pallas as pl
from jax.experimental.pallas import tpu as pltpu
from jax.sharding import PartitionSpec as P

HD = 128
GROUP = 4
MESH = pl.DeviceIdType.MESH
SHARES = 8
STRAIGHT = 2
PARTS = 2
LAYER = 4
CHUNKS = 8
WIDTH = 16
WIDTH_LOG = 4
PIECES = 4
AHEAD = 3

masked_score = -1e30


def attend(query, key, value, allowed):
    scores = lax.dot_general(
        query, key, (((1,), (1,)), ((), ())), preferred_element_type=jnp.float32
    ) * jnp.float32(1.0 / HD**0.5)
    scores = jnp.where(allowed, scores, masked_score)
    top = jnp.max(scores, axis=-1, keepdims=True)
    expo = jnp.exp(scores - top)
    total = jnp.sum(expo, axis=-1, keepdims=True)
    mixed = jnp.dot(expo.astype(jnp.bfloat16), value, preferred_element_type=jnp.float32)
    return (mixed / total).astype(jnp.bfloat16)


def weigh(queries, keys, values, allowed):
    scores = [
        lax.dot_general(q, k, (((1,), (1,)), ((), ())), preferred_element_type=jnp.float32)
        for q, k in zip(queries, keys)
    ]
    scores = [jnp.where(allowed, s * jnp.float32(1.0 / HD**0.5), masked_score) for s in scores]
    tops = [jnp.max(s, axis=-1, keepdims=True) for s in scores]
    expos = [jnp.exp(s - top) for s, top in zip(scores, tops)]
    totals = [jnp.sum(e, axis=-1, keepdims=True) for e in expos]
    mixed = [
        jnp.dot(e.astype(jnp.bfloat16), v, preferred_element_type=jnp.float32)
        for e, v in zip(expos, values)
    ]
    return [
        ((m / total).astype(jnp.bfloat16), top + jnp.log(total))
        for m, total, top in zip(mixed, totals, tops)
    ]


def layered(
    n, q_hbm, k_hbm, v_hbm, w_hbm, staged, q_row, k_row, v_row, q_in, k_in, v_in, o_out, p_in,
    stats, stats_in, row_out, joined, summed, w_own, w_other,
    local_sem, chunk_sem, lay_send, lay_recv, up_send, up_recv, part_send, part_recv,
    back_send, back_recv, w_send, w_recv, row_send, row_recv,
):
    me, head = lax.axis_index("ctx"), lax.axis_index("head")
    other = 1 - head
    z, s = lax.div(me, LAYER), lax.rem(me, LAYER)
    core = lax.rem(s, 2)
    sib = s + 1 - 2 * core
    opp = s + 2 - 4 * lax.div(s, 2)
    far = sib + 2 - 4 * lax.div(sib, 2)
    peers = (s, sib, opp, far)
    stride = q_hbm.shape[1]
    block = q_row.shape[1]
    depth = w_own.shape[0]
    half = joined.shape[1]
    cols = stride // LAYER
    cw = cols // CHUNKS
    hbm = (q_hbm, k_hbm, v_hbm)
    ins = (q_in, k_in, v_in)
    own_at = (0, LAYER, LAYER)
    feats = pl.ds(block, block)

    def place(j, slot):
        return slot * (cols // 2) + lax.div(j, 2) * cw

    def chunk_of(j, slot):
        return pl.ds(pl.multiple_of(lax.rem(j, 2) * half + place(j, slot), cw), cw)

    def remote(src, dst, send, recv, ctx, at):
        return pltpu.make_async_remote_copy(
            src_ref=src, dst_ref=dst, send_sem=send, recv_sem=recv,
            device_id=(ctx, at), device_id_type=MESH,
        )

    def here(slot):
        return z * LAYER + slot

    def lay(t, j, d, source):
        row = peers[d] if source else s
        return remote(
            hbm[t].at[0, chunk_of(j, peers[d]), feats],
            ins[t].at[own_at[t] + row, pl.ds(j * cw, cw)],
            lay_send.at[t * CHUNKS + j, d], lay_recv.at[t * CHUNKS + j, d],
            here(peers[d]), head,
        )

    def up(kind, t, j, d, layer, base):
        if d < 2:
            src, slot, row = hbm[t].at[0, chunk_of(j, peers[d]), feats], peers[d], s
        else:
            src, slot, row = ins[t].at[own_at[t] + peers[d], pl.ds(j * cw, cw)], s, peers[d]
        return remote(
            src, ins[t].at[base + row, pl.ds(j * cw, cw)],
            up_send.at[kind * CHUNKS + j, d], up_recv.at[kind * CHUNKS + j, d],
            layer * LAYER + slot, head,
        )

    def up_arrival(kind, t, j, d, base):
        return remote(
            hbm[t].at[0, pl.ds(0, cw), feats], ins[t].at[base + peers[d], pl.ds(j * cw, cw)],
            up_send.at[kind * CHUNKS + j, d], up_recv.at[kind * CHUNKS + j, d],
            here(sib), head,
        )

    routes = {
        0: ((0, 1, 1, 0), (1, 2, 1, 0)),
        2: ((2, 0, 1, LAYER),),
        3: ((2, 0, 2, LAYER),),
    }

    def onward(j):
        at = pl.ds(j * cw, cw)
        return remote(
            q_in.at[pl.ds(LAYER, LAYER), at], q_in.at[pl.ds(2 * LAYER, LAYER), at],
            up_send.at[3 * CHUNKS + j, 0], up_recv.at[3 * CHUNKS + j, 0], LAYER + s, head,
        )

    def pass_on(j):
        for d in range(4):
            up_arrival(2, 0, j, d, LAYER).wait_recv()
        onward(j).start()

    def direct(layer, j):
        for kind, t, to, base in routes[layer]:
            for d in (0, 1):
                up(kind, t, j, d, to, base).start()

    def relay(layer, j):
        for t in sorted({t for _, t, _, _ in routes[layer]}):
            for d in (2, 3):
                lay(t, j, d, True).wait_recv()
                for kind, t2, to, base in routes[layer]:
                    if t2 == t:
                        up(kind, t, j, d, to, base).start()

    def piece_rows(q, c, k):
        eighth = depth // 16
        rows = eighth // (PIECES // 2)
        start = lax.div(k, PIECES // 2) * (depth // 2)
        start += (q * 2 + c) * eighth + lax.rem(k, PIECES // 2) * rows
        return pl.ds(start, rows)

    def w_copy(source, q, c, k, way, to_ctx, to_head):
        rows = piece_rows(q, c, k)
        index = (q * 2 + c) * PIECES + k
        return remote(
            source.at[rows], w_other.at[rows], w_send.at[way, index], w_recv.at[index], to_ctx, to_head
        )

    even = lax.rem(z + lax.div(s, 2), 2)
    y_next = here(opp)
    z_next = me + LAYER - 2 * LAYER * lax.rem(z, 2)
    z_early = (z == 1) | (z == 2)

    def to_side(k):
        return (z > 0) | (k < PIECES // 2)

    def w_first(q, k):
        return w_copy(w_hbm, 2 * even + q, core, k, 0, me, other)

    def w_side(q, k):
        return w_copy(w_other, 2 * even + q, core, k, 2, y_next if q == 0 else z_next, head)

    def w_extra(k):
        return w_copy(w_other, 2 * even + 1, core, k, 3, me - LAYER, head)

    def w_beside(q, k):
        return w_copy(w_other, 2 * (1 - even) + q, core, k, 1, here(sib), head)

    def w_here(q, k):
        return w_copy(w_other, 2 * even + q, core, k, 1, here(sib), head)

    def w_in(q, k):
        w_first(q, k).wait_recv()
        w_here(q, k).start()
        if q == 0:
            w_side(q, k).start()
        else:

            @pl.when(z_early)
            def _():
                w_side(q, k).start()

            @pl.when((z == 2) & (k >= PIECES // 2))
            def _():
                w_extra(k).start()

    def w_step(i):
        high = z >= 2
        for_z = jnp.where(high, jnp.where(i < PIECES, 1, 0), lax.rem(i, 2))
        k = jnp.where(high, lax.rem(i, PIECES), lax.div(i, 2))

        @pl.when(for_z == 1)
        def _():
            w_in(1, k)

        @pl.when(for_z == 0)
        def _():
            w_in(0, k)

    def w_on(q, k):
        w_copy(w_other, 2 * (1 - even) + q, core, k, 2, me, other).wait_recv()
        w_beside(q, k).start()

    ready = pltpu.get_barrier_semaphore()

    def greet(ctx, at):
        pl.semaphore_signal(ready, 1, device_id=(ctx, at), device_id_type=MESH)

    greet(me, other)
    for d in (1, 2, 3):
        greet(here(peers[d]), head)
        greet(here(peers[d]), other)
    for edge, towards in ((0, -LAYER), (LAYER - 1, LAYER)):

        @pl.when(z != edge)
        def _():
            greet(here(s) + towards, head)
            greet(here(sib) + towards, head)

    local = [
        pltpu.make_async_copy(hbm[t].at[0, :, pl.ds(0, block)], (q_row, k_row, v_row)[t], local_sem.at[t])
        for t in range(3)
    ]
    local += [
        pltpu.make_async_copy(
            hbm[t].at[0, chunk_of(j, s), feats],
            ins[t].at[own_at[t] + s, pl.ds(j * cw, cw)],
            chunk_sem.at[t, j],
        )
        for t in range(3)
        for j in range(CHUNKS)
    ]
    local.append(pltpu.make_async_copy(w_hbm, w_own, local_sem.at[3]))
    for copy in local:
        copy.start()

    inner = jnp.minimum(z, 1) + jnp.minimum(LAYER - 1 - z, 1)
    pl.semaphore_wait(ready, 2 * LAYER - 1 + 2 * inner)

    def exchange(ts):
        @pl.loop(0, CHUNKS)
        def _(j):
            for t in ts:
                for d in (2, 3, 1):
                    lay(t, j, d, False).start()

    for layer in routes:

        @pl.when(z == layer)
        def _():
            for j in range(AHEAD):
                direct(layer, j)

    @pl.when(z < 2)
    def _():
        exchange((1, 2))
        exchange((0,))

    @pl.when(z >= 2)
    def _():
        exchange((0,))
        exchange((1, 2))

    @pl.when(z < 2)
    def _():
        @pl.loop(0, PIECES)
        def _(k):
            w_first(0, k).start()
            w_first(1, k).start()

    @pl.when(z >= 2)
    def _():
        for q in (1, 0):

            @pl.loop(0, PIECES)
            def _(k):
                w_first(q, k).start()

    for copy in local[:-1]:
        copy.wait()

    tile = min(256, half)
    row_index = lax.broadcasted_iota(jnp.int32, (tile, stride), 0)
    key_index = lax.broadcasted_iota(jnp.int32, (tile, stride), 1)

    def row_tile(h, start):
        lanes = pl.ds(pl.multiple_of(h * HD, HD), HD)
        end = start + tile
        row_out[pl.ds(start, tile), lanes] = attend(
            q_row[pl.ds(start, tile), lanes],
            k_row[pl.ds(0, end), lanes],
            v_row[pl.ds(0, end), lanes],
            key_index[:, :end] <= row_index[:, :end] + start,
        )

    def spread(sums):
        lane = lax.broadcasted_iota(jnp.int32, (HD, HD), 1)
        row = lax.broadcasted_iota(jnp.int32, (HD, HD), 0)
        return jnp.sum(jnp.where(lane == row, sums, 0.0), axis=0, keepdims=True)

    def laid(sums, off):
        lane = lax.broadcasted_iota(jnp.int32, (size, HD), 1)
        row = lax.broadcasted_iota(jnp.int32, (size, HD), 0)
        return jnp.sum(jnp.where(lane == row + off, sums, 0.0), axis=0, keepdims=True)

    def column(line, off, period):
        lane = lax.broadcasted_iota(jnp.int32, (size, HD), 1)
        row = lax.broadcasted_iota(jnp.int32, (size, HD), 0)
        at = off + (row & (WIDTH - 1)) + lax.shift_right_logical(row, WIDTH_LOG) * period
        return jnp.sum(jnp.where(lane == at, line, 0.0), axis=1, keepdims=True)

    heads = block // HD
    size = LAYER * WIDTH

    def small(q_at, q_rows, k_at, k_rows, c, b, width, causal, keep):
        start = pl.multiple_of(c * cw + b * width, width)
        shape = (q_rows * width, k_rows * width)
        r = lax.broadcasted_iota(jnp.int32, shape, 0)
        m = lax.broadcasted_iota(jnp.int32, shape, 1)
        allowed = ((r - m) & (width - 1)) == 0
        if causal is not None:
            allowed &= m <= r + causal * width
        slices = []
        for h in range(heads):
            lanes = pl.ds(h * HD, HD)
            slices.append(
                (
                    (pl.ds(q_at, q_rows), pl.ds(start, width), lanes),
                    (pl.ds(k_at, k_rows), pl.ds(start, width), lanes),
                )
            )
        found = weigh(
            [q_in[at].reshape(shape[0], HD) for at, _ in slices],
            [k_in[at].reshape(shape[1], HD) for _, at in slices],
            [v_in[at].reshape(shape[1], HD) for _, at in slices],
            allowed,
        )
        for h, (got, sums) in enumerate(found):
            o_out[slices[h][0]] = got.reshape(q_rows, width, HD)
            if keep:
                stats[c * strips + b, pl.ds(h, 1)] = spread(sums)

    strips = cw // WIDTH

    def partial(j, rows, layer):
        return remote(
            o_out.at[pl.ds(LAYER, rows), pl.ds(j * cw, cw)], p_in.at[pl.ds(0, rows), pl.ds(j * cw, cw)],
            part_send.at[0, j], part_recv.at[0, j], layer * LAYER + s, head,
        )

    def partial_stats(j, layer):
        at = pl.ds(j * strips, strips)
        return remote(
            stats.at[at], stats_in.at[at], part_send.at[1, j], part_recv.at[1, j], layer * LAYER + s, head
        )

    def back(j, d):
        return remote(
            o_out.at[peers[d], pl.ds(j * cw, cw)],
            joined.at[head, pl.ds(place(j, s), cw), feats],
            back_send.at[j, d], back_recv.at[head * LAYER + s, lax.div(j, 2)],
            here(peers[d]), lax.rem(j, 2),
        )

    def stays(j):
        return lax.rem(j, 2) == head

    def back_all(j):
        for d in (2, 3, 1):
            back(j, d).start()

        @pl.when(jnp.logical_not(stays(j)))
        def _():
            back(j, 0).start()

        @pl.when(stays(j))
        def _():
            joined[head, pl.ds(pl.multiple_of(place(j, s), cw), cw), feats] = o_out[
                s, pl.ds(pl.multiple_of(j * cw, cw), cw)
            ]

    def ext(j):
        for t in (1, 2):
            for d in (1, 2, 3):
                lay(t, j, d, True).wait_recv()
        for kind, t, base in ((0, 1, 0), (1, 2, 0), (2, 0, LAYER)):
            for d in range(4):
                up_arrival(kind, t, j, d, base).wait_recv()
        onward(j).wait_recv()
        for b in range(strips):
            small(LAYER, 2 * LAYER, 0, 2 * LAYER, j, b, WIDTH, None, True)
        partial(j, 2 * LAYER, 2).start()
        partial_stats(j, 2).start()

    def own(c):
        @pl.when(z == 0)
        def _():
            for t, ds in ((0, (1, 2, 3)), (1, (1,)), (2, (1,))):
                for d in ds:
                    lay(t, c, d, True).wait_recv()
            small(0, LAYER, LAYER, LAYER, c, 0, cw, 0, False)
            back_all(c)

        @pl.when(z == 1)
        def _():
            for d in (1, 2, 3):
                lay(0, c, d, True).wait_recv()
            small(0, LAYER, 0, 2 * LAYER, c, 0, cw, LAYER, False)
            back_all(c)

        @pl.when(z >= 2)
        def _():
            lay(0, c, 1, True).wait_recv()
            for t in (1, 2):
                for d in (1, 2, 3):
                    lay(t, c, d, True).wait_recv()

        @pl.when(z == 2)
        def _():
            for b in range(strips):
                small(0, 2 * LAYER, LAYER, LAYER, c, b, WIDTH, 0, True)

        @pl.when(z == 3)
        def _():
            small(0, LAYER, LAYER, LAYER, c, 0, cw, 0, True)

    def combine(c):
        def mix(b, base, parts, keep):
            start = pl.multiple_of(c * cw + b * WIDTH, WIDTH)
            rows = pl.ds(start, WIDTH)
            strip = c * strips + b
            for h in range(heads):
                lanes = pl.ds(h * HD, HD)
                lines = [column(ref[at, pl.ds(row + h, 1)], off, period) for _, _, ref, at, row, off, period in parts]
                top = functools.reduce(jnp.maximum, lines)
                terms = [jnp.exp(line - top) for line in lines]
                total = functools.reduce(jnp.add, terms)
                got = 0.0
                for (source, first, *_), term in zip(parts, terms):
                    value = source[pl.ds(first, LAYER), rows, lanes].reshape(size, HD)
                    got += value.astype(jnp.float32) * (term / total)
                o_out[pl.ds(base, LAYER), rows, lanes] = got.astype(jnp.bfloat16).reshape(LAYER, WIDTH, HD)
                if keep:
                    stats[strip, pl.ds(heads + h, 1)] = laid(top + jnp.log(total), size)

        @pl.when(z == 2)
        def _():
            partial(c, 2 * LAYER, 2).wait_recv()
            partial_stats(c, 2).wait_recv()
            for first in (LAYER, 0):
                off = size if first else 0
                for b in range(strips):
                    strip = c * strips + b
                    mix(
                        b,
                        first,
                        [
                            (o_out, first, stats, strip, 0, off, WIDTH),
                            (p_in, first, stats_in, strip, 0, off, WIDTH),
                        ],
                        first > 0,
                    )
                if first:
                    partial(c, LAYER, 3).start()
                    partial_stats(c, 3).start()

        @pl.when(z == 3)
        def _():
            partial(c, LAYER, 3).wait_recv()
            partial_stats(c, 3).wait_recv()
            for b in range(strips):
                strip = c * strips + b
                mix(
                    b,
                    0,
                    [
                        (o_out, 0, stats, c * strips, 0, b * WIDTH, cw),
                        (p_in, 0, stats_in, strip, heads, size, WIDTH),
                    ],
                    False,
                )

        back_all(c)

    row_copy = remote(
        row_out.at[pl.ds(pl.multiple_of(other * half, half), half)],
        joined.at[head, :, pl.ds(0, block)], row_send, row_recv, me, other,
    )
    step = 4096
    count = w_own.shape[1] // step

    def tiles(add):
        @pl.loop(0, count)
        def _(c):
            add(pl.ds(pl.multiple_of(c * step, step), step))

    def own_row_part(lanes):
        summed[:, lanes] = jnp.dot(
            joined[head, :, pl.ds(0, block)],
            w_own[pl.ds(0, block), lanes],
            preferred_element_type=jnp.float32,
        )

    @pl.loop(0, CHUNKS)
    def _(j):
        @pl.when(j < heads)
        def _():
            for start in range(0, stride, tile):
                row_tile(j, start)

        @pl.when(j == heads - 1)
        def _():
            row_copy.start()
            joined[head, :, pl.ds(0, block)] = row_out[pl.ds(pl.multiple_of(head * half, half), half)]

        for layer in routes:

            @pl.when((z == layer) & (j < CHUNKS // 2))
            def _():
                @pl.loop(2 * j, 2 * j + 2)
                def _(c):
                    relay(layer, c)
                    if layer == 2:
                        pass_on(c)

                    @pl.when(c + AHEAD < CHUNKS)
                    def _():
                        direct(layer, c + AHEAD)

        @pl.when(z == 1)
        def _():
            ext(j)

        @pl.when(j == heads)
        def _():
            local[-1].wait()
            tiles(own_row_part)

        i = j - jnp.where(z == 1, 0, 1)

        @pl.when(i >= 0)
        def _():
            w_step(i)

        @pl.when(jnp.logical_not(z_early) & (j == PIECES))
        def _():
            @pl.loop(0, PIECES)
            def _(k):
                @pl.when(to_side(k))
                def _():
                    w_side(1, k).start()

        @pl.when(j >= CHUNKS // 2)
        def _():
            c = 2 * j - CHUNKS
            own(c)
            own(c + 1)

            lag = z - 2

            @pl.when((z >= 2) & (j >= CHUNKS // 2 + lag))
            def _():
                combine(j - CHUNKS // 2 - lag)

    @pl.when(z != 1)
    def _():
        w_step(2 * PIECES - 1)

    def combine_some(layer, first, last):
        @pl.when(z == layer)
        def _():
            @pl.loop(first, last)
            def _(c):
                combine(c)

    def w_on_some(q, first, last):
        @pl.loop(first, last)
        def _(k):
            w_on(q, k)

    def w_from_sibling(qs, first, last):
        @pl.loop(first, last)
        def _(k):
            for q in qs:
                w_copy(w_other, q, 1 - core, k, 1, here(sib), head).wait_recv()

    def other_row_part(lanes):
        summed[:, lanes] += jnp.dot(
            joined[other, :, pl.ds(0, block)],
            w_other[pl.ds(0, block), lanes],
            preferred_element_type=jnp.float32,
        )

    def back_wait(u):
        for source_head in (head, other):
            for slot in range(LAYER):

                @pl.when(jnp.logical_not((slot == s) & (head == source_head)))
                def _():
                    for i in range(u * CHUNKS // 4, (u + 1) * CHUNKS // 4):
                        remote(
                            o_out.at[0, pl.ds(0, cw)],
                            joined.at[source_head, pl.ds(place(2 * i, slot), cw), feats],
                            back_send.at[i, 0], back_recv.at[source_head * LAYER + slot, i],
                            me, other,
                        ).wait_recv()

    run = CHUNKS // 4 * cw

    def finish(u):
        rows = [pl.ds(slot * (cols // 2) + u * run, run) for slot in range(LAYER)]

        @pl.loop(0, count)
        def _(c):
            lanes = pl.ds(pl.multiple_of(c * step, step), step)
            total = jnp.dot(
                jnp.concatenate([joined[head, at, feats] for at in rows]),
                w_own[feats, lanes],
                preferred_element_type=jnp.float32,
            )
            total += jnp.dot(
                jnp.concatenate([joined[other, at, feats] for at in rows]),
                w_other[feats, lanes],
                preferred_element_type=jnp.float32,
            )
            for slot, at in enumerate(rows):
                part = summed[at, lanes] + total[slot * run : (slot + 1) * run]
                staged[slot, u, :, lanes] = part.astype(jnp.bfloat16)

    combine_some(2, CHUNKS // 2, CHUNKS)
    combine_some(3, CHUNKS // 2 - 1, CHUNKS - 3)
    w_on_some(0, 0, PIECES // 2)
    w_on_some(1, 0, PIECES // 2)
    combine_some(3, CHUNKS - 3, CHUNKS - 1)
    w_from_sibling((0, 1, 2, 3), 0, PIECES // 2)
    row_copy.wait_recv()
    tiles(other_row_part)
    combine_some(3, CHUNKS - 1, CHUNKS)
    w_on_some(0, PIECES // 2, PIECES)
    w_on_some(1, PIECES // 2, PIECES)
    w_from_sibling((0, 1, 2, 3), PIECES // 2, PIECES)
    back_wait(0)
    finish(0)
    back_wait(1)
    finish(1)

    @pl.loop(0, CHUNKS)
    def _(j):
        for t in range(3):
            for d in (1, 2, 3):
                lay(t, j, d, False).wait_send()
        for layer in routes:

            @pl.when(z == layer)
            def _():
                for kind, t, to, base in routes[layer]:
                    for d in range(4):
                        up(kind, t, j, d, to, base).wait_send()

        @pl.when(z == 1)
        def _():
            partial(j, 2 * LAYER, 2).wait_send()
            partial_stats(j, 2).wait_send()

        @pl.when(z == 2)
        def _():
            onward(j).wait_send()
            partial(j, LAYER, 3).wait_send()
            partial_stats(j, 3).wait_send()

        for d in (1, 2, 3):
            back(j, d).wait_send()

        @pl.when(jnp.logical_not(stays(j)))
        def _():
            back(j, 0).wait_send()

    @pl.loop(0, PIECES)
    def _(k):
        for q in (0, 1):
            w_first(q, k).wait_send()
            w_here(q, k).wait_send()
            w_beside(q, k).wait_send()
        w_side(0, k).wait_send()

        @pl.when(to_side(k))
        def _():
            w_side(1, k).wait_send()

        @pl.when((z == 2) & (k >= PIECES // 2))
        def _():
            w_extra(k).wait_send()

    row_copy.wait_send()


def call_layered(n, queries, keys, values, w_out, half):
    _, stride, local_feat = queries.shape
    depth, width = w_out.shape
    block = local_feat // 2
    cols = stride // LAYER
    bf16, f32 = jnp.bfloat16, jnp.float32
    dma = pltpu.SemaphoreType.DMA
    blocks = cols // WIDTH
    return pl.pallas_call(
        functools.partial(layered, n),
        out_shape=pltpu.VMEM((LAYER, 2, half // (2 * LAYER), width), bf16),
        in_specs=[pl.BlockSpec(memory_space=pltpu.HBM)] * 4,
        out_specs=pl.BlockSpec(memory_space=pltpu.VMEM),
        scratch_shapes=[pltpu.VMEM((stride, block), bf16)] * 3
        + [
            pltpu.VMEM((3 * LAYER, cols, block), bf16),
            pltpu.VMEM((2 * LAYER, cols, block), bf16),
            pltpu.VMEM((2 * LAYER, cols, block), bf16),
            pltpu.VMEM((3 * LAYER, cols, block), bf16),
            pltpu.VMEM((2 * LAYER, cols, block), bf16),
            pltpu.VMEM((blocks, 8, HD), f32),
            pltpu.VMEM((blocks, 8, HD), f32),
            pltpu.VMEM((stride, block), bf16),
            pltpu.VMEM((2, half, local_feat), bf16),
            pltpu.VMEM((half, width), f32),
            pltpu.VMEM((depth, width), bf16),
            pltpu.VMEM((depth, width), bf16),
            dma((4,)),
            dma((3, CHUNKS)),
            dma((3 * CHUNKS, LAYER)),
            dma((3 * CHUNKS, LAYER)),
            dma((4 * CHUNKS, LAYER)),
            dma((4 * CHUNKS, LAYER)),
            dma((2, CHUNKS)),
            dma((2, CHUNKS)),
            dma((CHUNKS, LAYER)),
            dma((2 * LAYER, CHUNKS // 2)),
            dma((4, 8 * PIECES)),
            dma((8 * PIECES,)),
            dma,
            dma,
        ],
        compiler_params=pltpu.CompilerParams(
            collective_id=0, has_side_effects=True, vmem_limit_bytes=56 * 2**20
        ),
    )(queries, keys, values, w_out)


def body(
    n, q_hbm, k_hbm, v_hbm, w_hbm, out_ref, q_row, k_row, v_row, q_col, k_col, v_col,
    col_out, row_out, joined, summed, w_own, w_other, local_sem, in_send, in_recv, back_send, back_recv,
    w_send, w_recv, row_send, row_recv,
):
    me, head = lax.axis_index("ctx"), lax.axis_index("head")
    other = 1 - head
    stride = q_hbm.shape[1]
    block = q_row.shape[1]
    depth = w_own.shape[0]
    half = joined.shape[1]
    cols = stride // n
    share = block // PARTS
    hbm = (q_hbm, k_hbm, v_hbm)
    rows_in = (q_row, k_row, v_row)
    cols_in = (q_col, k_col, v_col)
    back_head = lax.div(me * cols, half)
    member = lax.rem(me, 4)
    sibling = me + 1 - 2 * lax.rem(me, 2)
    beside = me + 2 - 4 * lax.div(member, 2)
    piece = depth // (4 * SHARES)

    def col_copy(t, part, d):
        peer = lax.rem(me + d, n)
        lanes = pl.ds(part * share, share)
        return pltpu.make_async_remote_copy(
            src_ref=hbm[t].at[0, pl.ds(peer * cols, cols), pl.ds(block + part * share, share)],
            dst_ref=cols_in[t].at[me, :, lanes],
            send_sem=in_send.at[t * PARTS + part, d],
            recv_sem=in_recv.at[t * PARTS + part, d],
            device_id=(peer, head),
            device_id_type=MESH,
        )

    def col_arrival(t, part, d):
        source = lax.rem(me + n - d, n)
        lanes = pl.ds(part * share, share)
        return pltpu.make_async_remote_copy(
            src_ref=hbm[t].at[0, pl.ds(0, cols), pl.ds(block + part * share, share)],
            dst_ref=cols_in[t].at[source, :, lanes],
            send_sem=in_send.at[t * PARTS + part, d],
            recv_sem=in_recv.at[t * PARTS + part, d],
            device_id=(source, head),
            device_id_type=MESH,
        )

    def w_copy(source, index, way, to_ctx, to_head):
        rows = pl.ds(index * piece, piece)
        return pltpu.make_async_remote_copy(
            src_ref=source.at[rows],
            dst_ref=w_other.at[rows],
            send_sem=w_send.at[way, index],
            recv_sem=w_recv.at[index],
            device_id=(to_ctx, to_head),
            device_id_type=MESH,
        )

    def index_of(who, s):
        return who * SHARES + s

    member_sibling = lax.rem(sibling, 4)
    member_beside = lax.rem(beside, 4)
    member_far = lax.rem(member + 2, 4) + 1 - 2 * lax.rem(member, 2)

    for part in range(PARTS):

        @pl.loop(1, n)
        def _(d):
            for t in range(3):
                col_copy(t, part, d).start()

    @pl.loop(0, SHARES)
    def _(s):
        w_copy(w_hbm, index_of(member, s), 0, me, other).start()

    @pl.loop(SHARES - STRAIGHT, SHARES)
    def _(s):
        w_copy(w_hbm, index_of(member_beside, s), 0, me, other).start()

    local = [
        pltpu.make_async_copy(hbm[t].at[0, :, pl.ds(0, block)], rows_in[t], local_sem.at[t])
        for t in range(3)
    ]
    local += [
        pltpu.make_async_copy(
            hbm[t].at[0, pl.ds(me * cols, cols), pl.ds(block, block)],
            cols_in[t].at[me],
            local_sem.at[3 + t],
        )
        for t in range(3)
    ]
    local.append(pltpu.make_async_copy(w_hbm, w_own, local_sem.at[3]))
    for copy in local:
        copy.start()
    for copy in local[:3]:
        copy.wait()

    tile = min(256, half)
    row_index = lax.broadcasted_iota(jnp.int32, (tile, stride), 0)
    key_index = lax.broadcasted_iota(jnp.int32, (tile, stride), 1)

    @pl.loop(0, block // HD)
    def _(h):
        lanes = pl.ds(pl.multiple_of(h * HD, HD), HD)
        for start in range(0, stride, tile):
            end = start + tile
            row_out[pl.ds(start, tile), lanes] = attend(
                q_row[pl.ds(start, tile), lanes],
                k_row[pl.ds(0, end), lanes],
                v_row[pl.ds(0, end), lanes],
                key_index[:, :end] <= row_index[:, :end] + start,
            )

    row_copy = pltpu.make_async_remote_copy(
        src_ref=row_out.at[pl.ds(pl.multiple_of(other * half, half), half)],
        dst_ref=joined.at[head, :, pl.ds(0, block)],
        send_sem=row_send,
        recv_sem=row_recv,
        device_id=(me, other),
        device_id_type=MESH,
    )
    row_copy.start()
    joined[head, :, pl.ds(0, block)] = row_out[pl.ds(pl.multiple_of(head * half, half), half)]

    def onward(first, last):
        @pl.loop(first, last)
        def _(s):
            index = index_of(member, s)
            w_copy(w_hbm, index, 0, me, other).wait_recv()

            @pl.when(s < SHARES - STRAIGHT)
            def _():
                w_copy(w_other, index, 1, beside, head).start()

            w_copy(w_other, index, 2, sibling, head).start()

    onward(0, SHARES // 2)

    for copy in local[3:]:
        copy.wait()

    step = 512

    def tiles(add):
        @pl.loop(0, out_ref.shape[1] // step)
        def _(c):
            add(pl.ds(pl.multiple_of(c * step, step), step))

    def own_row_part(lanes):
        summed[:, lanes] = jnp.dot(
            joined[head, :, pl.ds(0, block)],
            w_own[pl.ds(0, block), lanes],
            preferred_element_type=jnp.float32,
        )

    tiles(own_row_part)
    width = min(cols, max(16, 256 // n))
    size = n * width
    r_index = lax.broadcasted_iota(jnp.int32, (size, size), 0)
    s_index = lax.broadcasted_iota(jnp.int32, (size, size), 1)
    allowed = (s_index <= r_index) & (((r_index - s_index) & (width - 1)) == 0)

    slot_here = lax.rem(me, n // 2)
    stays = back_head == head

    def landing(source_head, part, slot):
        return joined.at[
            source_head,
            pl.ds(pl.multiple_of(slot * cols, cols), cols),
            pl.ds(block + part * share, share),
        ]

    def back_copy(part, r):
        return pltpu.make_async_remote_copy(
            src_ref=col_out.at[r, :, pl.ds(part * share, share)],
            dst_ref=landing(head, part, slot_here),
            send_sem=back_send.at[part, r],
            recv_sem=back_recv.at[head * PARTS + part, slot_here],
            device_id=(r, back_head),
            device_id_type=MESH,
        )

    def back_arrival(source_head, part, slot):
        return pltpu.make_async_remote_copy(
            src_ref=col_out.at[0, :, pl.ds(part * share, share)],
            dst_ref=landing(source_head, part, slot),
            send_sem=back_send.at[part, 0],
            recv_sem=back_recv.at[source_head * PARTS + part, slot],
            device_id=(me, other),
            device_id_type=MESH,
        )

    for part in range(PARTS):

        @pl.loop(1, n)
        def _(d):
            for t in range(3):
                col_arrival(t, part, d).wait_recv()

        @pl.loop(part * (share // HD), (part + 1) * (share // HD))
        def _(h):
            lanes = pl.ds(pl.multiple_of(h * HD, HD), HD)
            for start in range(0, cols, width):
                at = (slice(None), pl.ds(start, width), lanes)
                got = attend(*(ref[at].reshape(size, HD) for ref in cols_in), allowed)
                col_out[at] = got.reshape(n, width, HD)

        @pl.loop(1, n)
        def _(d):
            back_copy(part, lax.rem(me + d, n)).start()

        @pl.when(stays)
        def _():
            rows = pl.ds(pl.multiple_of(slot_here * cols, cols), cols)
            joined[head, rows, pl.ds(block + part * share, share)] = col_out[
                me, :, pl.ds(part * share, share)
            ]

        @pl.when(jnp.logical_not(stays))
        def _():
            back_copy(part, me).start()

        if part == 0:
            onward(SHARES // 2, SHARES)

    @pl.loop(0, SHARES)
    def _(s):
        index = index_of(member_beside, s)
        w_copy(w_other, index, 1, beside, head).wait_recv()
        w_copy(w_other, index, 3, sibling, head).start()

    row_copy.wait_recv()

    def back_wait(source_head):
        @pl.loop(0, n // 2)
        def _(slot):
            mine = (head * (n // 2) + slot == me) & (head == source_head)

            @pl.when(jnp.logical_not(mine))
            def _():
                for part in range(PARTS):
                    back_arrival(source_head, part, slot).wait_recv()

    back_wait(head)

    def own_col_part(lanes):
        summed[:, lanes] += jnp.dot(
            joined[head, :, pl.ds(block, block)],
            w_own[pl.ds(block, block), lanes],
            preferred_element_type=jnp.float32,
        )

    tiles(own_col_part)

    @pl.loop(0, SHARES)
    def _(s):
        w_copy(w_other, index_of(member_sibling, s), 2, sibling, head).wait_recv()
        w_copy(w_other, index_of(member_far, s), 3, sibling, head).wait_recv()

    back_wait(other)

    def other_part(lanes):
        total = summed[:, lanes] + jnp.dot(
            joined[other], w_other[:, lanes], preferred_element_type=jnp.float32
        )
        out_ref[:, lanes] = total.astype(jnp.bfloat16)

    tiles(other_part)

    for part in range(PARTS):

        @pl.loop(1, n)
        def _(d):
            for t in range(3):
                col_copy(t, part, d).wait_send()

    @pl.loop(0, SHARES)
    def _(s):
        w_copy(w_hbm, index_of(member, s), 0, me, other).wait_send()
        w_copy(w_other, index_of(member, s), 2, sibling, head).wait_send()
        w_copy(w_other, index_of(member_beside, s), 3, sibling, head).wait_send()

    @pl.loop(0, SHARES - STRAIGHT)
    def _(s):
        w_copy(w_other, index_of(member, s), 1, beside, head).wait_send()

    @pl.loop(SHARES - STRAIGHT, SHARES)
    def _(s):
        w_copy(w_hbm, index_of(member_beside, s), 0, me, other).wait_send()

    row_copy.wait_send()

    for part in range(PARTS):

        @pl.loop(1, n)
        def _(d):
            back_copy(part, lax.rem(me + d, n)).wait_send()

        @pl.when(jnp.logical_not(stays))
        def _():
            back_copy(part, me).wait_send()


def on_device(n, queries, keys, values, w_out):
    _, stride, local_feat = queries.shape
    depth, model_width = w_out.shape
    block = GROUP * HD
    assert queries.shape[0] == 1 and local_feat == 2 * block
    half = stride // lax.axis_size("head")
    cols = stride // n
    if n == LAYER * LAYER and stride % (LAYER * CHUNKS * WIDTH) == 0:
        out = call_layered(n, queries, keys, values, w_out, half)
        return out.reshape((1, half, model_width))
    bf16 = jnp.bfloat16
    dma = pltpu.SemaphoreType.DMA
    out = pl.pallas_call(
        functools.partial(body, n),
        out_shape=jax.ShapeDtypeStruct((half, model_width), bf16),
        in_specs=[pl.BlockSpec(memory_space=pltpu.HBM)] * 4,
        out_specs=pl.BlockSpec(memory_space=pltpu.VMEM),
        scratch_shapes=[pltpu.VMEM((stride, block), bf16)] * 3
        + [pltpu.VMEM((n, cols, block), bf16)] * 4
        + [
            pltpu.VMEM((stride, block), bf16),
            pltpu.VMEM((2, half, local_feat), bf16),
            pltpu.VMEM((half, model_width), jnp.float32),
            pltpu.VMEM((depth, model_width), bf16),
            pltpu.VMEM((depth, model_width), bf16),
            dma((7,)),
            dma((3 * PARTS, n)),
            dma((3 * PARTS, n)),
            dma((PARTS, n)),
            dma((2 * PARTS, n // 2)),
            dma((4, 4 * SHARES)),
            dma((4 * SHARES,)),
            dma,
            dma,
        ],
        compiler_params=pltpu.CompilerParams(has_side_effects=True, vmem_limit_bytes=60 * 2**20),
    )(queries, keys, values, w_out)
    return out.reshape((1, half, model_width))


def solution(mesh):
    return jax.shard_map(
        functools.partial(on_device, mesh.shape["ctx"]),
        mesh=mesh,
        in_specs=(
            P("ctx", None, "head"),
            P("ctx", None, "head"),
            P("ctx", None, "head"),
            P("head", None),
        ),
        out_specs=P("ctx", "head", None),
        check_vma=False,
    )
```
